32 devices in a mesh: wide: 8 (over z, x), narrow: 4 (over y, core).
Axes of the slice: x: 2, y: 2, z: 4, core: 2. Of those that a mesh axis runs over, the one named last changes fastest.
Arguments:
- tokens: bfloat16 [3, 10240, 768], P(None, 'wide'), may hold values from -6 to 6
- image_lengths: int32 [3, 8, 8], P(None, 'wide'), may hold values from 1 to 196, 1280 in all within a row
- heads_weight: bfloat16 [768, 3, 768], P('wide', None, 'narrow'), may hold values from -0.21875 to 0.21875
- heads_bias: float32 [2, 768], P(None, 'narrow'), may hold values from -3 to 3
- out_weight: bfloat16 [768, 768], P('narrow', 'wide'), may hold values from -1.75 to 1.75
- out_bias: float32 [768], replicated, may hold values from -3 to 3
- up_weight: bfloat16 [768, 3072], P('wide', 'narrow'), may hold values from -0.21875 to 0.21875
- up_bias: float32 [3072], P('narrow'), may hold values from -3 to 3
- down_weight: bfloat16 [3072, 768], P('narrow', 'wide'), may hold values from -0.109375 to 0.109375
- down_bias: float32 [768], replicated, may hold values from -3 to 3
- first_gain: float32 [768], replicated, may hold values from 0.1 to 1.9
- first_shift: float32 [768], replicated, may hold values from -3 to 3
- second_gain: float32 [768], replicated, may hold values from 0.1 to 1.9
- second_shift: float32 [768], replicated, may hold values from -3 to 3
- mixer_scale: float32 [768], replicated, may hold values from 0.5 to 2
- feed_scale: float32 [768], replicated, may hold values from 0.5 to 2
- cotangent: bfloat16 [3, 10240, 768], P(None, 'wide'), may hold values from -6 to 6
Outputs:
- layer_out: bfloat16 [3, 10240, 768], P(None, 'wide')
- token_grad: bfloat16 [3, 10240, 768], P(None, ('wide', 'narrow'))
- heads_weight_grad: float32 [768, 3, 768], P(None, None, 'narrow')
- heads_bias_grad: float32 [2, 768], P(None, 'narrow')
- out_weight_grad: float32 [768, 768], P('narrow')
- out_bias_grad: float32 [768], replicated
- up_weight_grad: float32 [768, 3072], P(None, 'narrow')
- up_bias_grad: float32 [3072], P('narrow')
- down_weight_grad: float32 [3072, 768], P('narrow')
- down_bias_grad: float32 [768], replicated
- first_gain_grad: float32 [768], replicated
- first_shift_grad: float32 [768], replicated
- second_gain_grad: float32 [768], replicated
- second_shift_grad: float32 [768], replicated
- mixer_scale_grad: float32 [768], replicated
- feed_scale_grad: float32 [768], replicated
The draws below stay inside these ranges and needn't reach their ends.
Inputs may be any that keep to these rules, and one draw needn't show every extreme that they name: `image_lengths`: each row of 8 numbers gives the lengths of the images packed in order into one micro-batch of one index of wide; they sum to 1280, and the largest is 196.
All inputs are finite; a program needn't handle non-finite values.
Results may differ from the reference program's by a relative error of at most 0.02.
Values may be sent and summed in bfloat16 or wider, within the bound.
No kernel may reach another device: no remote copies, remote signals or barrier semaphores. Data moves between devices by JAX's collectives and lax.ppermute only.
A program may use at most 256 MiB of HBM per device.

```python
import math
import jax
import jax.numpy as jnp
import numpy as np
from jax import lax

D = 768
HEADS = 12
HEAD_DIM = 64
FF = 3072
ROWS = 1280
MICRO = 3
MOST_PATCHES = 196
IMAGES = 8
N_WIDE = 8
N_NARROW = 4


def levels(stream_key, shape, split, smallest, largest):
    def one(axis_at, parts):
        heights = jax.random.uniform(jax.random.fold_in(jax.random.fold_in(stream_key, 6), axis_at), (parts,), jnp.float32, smallest / len(split), largest / len(split))
        return jnp.repeat(jnp.exp(heights), shape[axis_at] // parts).reshape((-1,) + (1,) * (len(shape) - axis_at - 1))

    level = one(*split[0])
    for cut in split[1:]:
        level = level * one(*cut)
    return level


def profile(number_of, total, most, slope):
    portions = [(1 << 20) // math.isqrt(standing ** slope) + 1 for standing in range(2, number_of + 1)]
    surplus, given = total - most - (number_of - 1), [1] * (number_of - 1)
    while surplus > 0:
        movable = [i for i in range(number_of - 1) if given[i] < most]
        pool, left = sum([portions[i] for i in movable]), surplus
        for i in movable:
            extra = min(most - given[i], max(1, left * portions[i] // pool), surplus)
            given[i] = given[i] + extra
            surplus = surplus - extra
    return np.array([most] + given)


def ragged(own_key, number_of, total, limit, skew):
    if number_of == 2:
        one = jax.random.randint(own_key, (), max(1, total - limit), min(limit, total - 1) + 1)
        return jnp.stack([one, total - one])
    tallies = jnp.asarray(profile(number_of, total, limit, skew), jnp.int32)
    pairs = (number_of - 1) // 2
    source_of, sink = tallies[1:1 + 2 * pairs:2], tallies[2:2 + 2 * pairs:2]
    margin = jnp.minimum(source_of - 1, limit - sink)
    passed = jax.random.randint(jax.random.fold_in(own_key, 1), (pairs,), 0, 1 << 20) % (margin + 1)
    tallies = tallies.at[1:1 + 2 * pairs:2].set(source_of - passed).at[2:2 + 2 * pairs:2].set(sink + passed)
    return tallies[jax.random.permutation(jax.random.fold_in(own_key, 2), number_of)]


def scatter_about(stream_key, dims, scale, bound, shards=(), kind=jnp.bfloat16):
    loudness = levels(stream_key, dims, shards, -0.22, 0.18) if shards else 1.0
    drawn = jax.random.normal(stream_key, dims, jnp.float32) * scale * loudness
    return jnp.minimum(jnp.maximum(drawn, -bound), bound).astype(kind)


def setup_inputs(seed: int = 0) -> dict:
    keys = jax.random.split(jax.random.key(seed), 18)
    tokens = scatter_about(keys[0], (MICRO, N_WIDE * ROWS, D), 1.0, 6.0, ((1, 8),))
    image_lengths = jax.vmap(lambda own: ragged(own, IMAGES, ROWS, MOST_PATCHES, 1))(jax.random.split(keys[1], MICRO * N_WIDE)).reshape((MICRO, N_WIDE, IMAGES)).astype(jnp.int32)
    heads_weight = scatter_about(keys[2], (D, 3, D), D ** -0.5, 0.21875, ((0, 8), (2, 4)))
    heads_bias = scatter_about(keys[3], (2, D), 0.5, 3.0, ((1, 4),), jnp.float32)
    out_weight = scatter_about(keys[4], (D, D), (max(D // 64, 1)) ** -0.5, 1.75, ((0, 4), (1, 8)))
    out_bias = scatter_about(keys[5], (D,), 0.5, 3.0, (), jnp.float32)
    up_weight = scatter_about(keys[6], (D, FF), D ** -0.5, 0.21875, ((0, 8), (1, 4)))
    up_bias = scatter_about(keys[7], (FF,), 0.5, 3.0, ((0, 4),), jnp.float32)
    down_weight = scatter_about(keys[8], (FF, D), FF ** -0.5, 0.109375, ((0, 4), (1, 8)))
    down_bias = scatter_about(keys[9], (D,), 0.5, 3.0, (), jnp.float32)
    first_gain = jnp.clip(1.0 + 0.18 * jax.random.normal(keys[10], (D,), jnp.float32), 0.1, 1.9)
    first_shift = scatter_about(keys[11], (D,), 0.5, 3.0, (), jnp.float32)
    second_gain = jnp.clip(1.0 + 0.18 * jax.random.normal(keys[12], (D,), jnp.float32), 0.1, 1.9)
    second_shift = scatter_about(keys[13], (D,), 0.5, 3.0, (), jnp.float32)
    mixer_scale = jnp.clip(jnp.exp(jax.random.uniform(keys[14], (D,), jnp.float32, math.log(0.5), math.log(2.0))), 0.5, 2.0)
    feed_scale = jnp.clip(jnp.exp(jax.random.uniform(keys[15], (D,), jnp.float32, math.log(0.5), math.log(2.0))), 0.5, 2.0)
    cotangent = scatter_about(keys[16], (MICRO, N_WIDE * ROWS, D), 1.0, 6.0, ((1, 8),))
    return dict(tokens=tokens, image_lengths=image_lengths, heads_weight=heads_weight, heads_bias=heads_bias, out_weight=out_weight, out_bias=out_bias, up_weight=up_weight, up_bias=up_bias, down_weight=down_weight, down_bias=down_bias, first_gain=first_gain, first_shift=first_shift, second_gain=second_gain, second_shift=second_shift, mixer_scale=mixer_scale, feed_scale=feed_scale, cotangent=cotangent)


epsilon = 1e-06
highest = lax.Precision.HIGHEST

@jax.custom_vjp
def low(v):
    return lax.optimization_barrier(v.astype(jnp.bfloat16)).astype(jnp.float32)

@jax.custom_vjp
def low_back(v):
    return v

def low_keep(v):
    return (low(v), None)

def low_pass(kept, grad):
    return (grad,)

def back_keep(v):
    return (v, None)

def back_low(kept, grad):
    return (low(grad),)
low.defvjp(low_keep, low_pass)
low_back.defvjp(back_keep, back_low)

def norm_rows(values_in, gain_row, shift_row):
    center = lax.optimization_barrier(jnp.mean(values_in, axis=-1, keepdims=True))
    shifted = values_in - center
    variance = lax.optimization_barrier(jnp.mean(shifted * shifted, axis=-1, keepdims=True))
    return shifted * lax.rsqrt(variance + epsilon) * gain_row + shift_row

def image_index(sizes_row, row_count):
    bounds = jnp.cumsum(sizes_row).astype(jnp.int32)
    places = jnp.arange(row_count, dtype=jnp.int32)
    return lax.optimization_barrier(jnp.sum((places[:, None] >= bounds[None, :]).astype(jnp.int32), axis=1))

def group_copies(values_in):
    return low_back(jnp.broadcast_to(values_in[None], (N_NARROW,) + values_in.shape))

def layer_rows(params, token_rows, sizes_row):
    heads_weight, heads_bias, out_weight, out_bias, up_weight, up_bias, down_weight, down_bias, first_gain, first_shift, second_gain, second_shift, mixer_scale, feed_scale = params
    row_count = token_rows.shape[0]
    group_width = D // N_NARROW
    hidden_width = FF // N_NARROW
    first_normed = low(norm_rows(token_rows, first_gain, first_shift))
    first_groups = group_copies(first_normed)
    projected = jnp.einsum('grd,dtgc->rtgc', first_groups, heads_weight.reshape(D, 3, N_NARROW, group_width), precision=highest).reshape(row_count, 3, D)
    query_heads = low(low_back(projected[:, 0] + heads_bias[0])).reshape(row_count, HEADS, HEAD_DIM)
    key_heads = low(low_back(projected[:, 1])).reshape(row_count, HEADS, HEAD_DIM)
    value_heads = low(low_back(projected[:, 2] + heads_bias[1])).reshape(row_count, HEADS, HEAD_DIM)
    raw_scores = jnp.einsum('qhc,khc->hqk', query_heads, key_heads, precision=highest) * HEAD_DIM ** (-0.5)
    index_row = image_index(sizes_row, row_count)
    same_image = index_row[:, None] == index_row[None, :]
    scores = jnp.where(same_image[None], low_back(raw_scores), -1e+30)
    row_max = lax.optimization_barrier(jnp.max(scores, axis=-1, keepdims=True))
    exp_scores = jnp.exp(scores - row_max)
    soft_weights = exp_scores / lax.optimization_barrier(jnp.sum(exp_scores, axis=-1, keepdims=True))
    context = jnp.einsum('hqk,khc->qhc', low(soft_weights), value_heads, precision=highest)
    context = low(low_back(context.reshape(row_count, D)))
    mixer_parts = jnp.einsum('rgc,gcd->grd', context.reshape(row_count, N_NARROW, group_width), out_weight.reshape(N_NARROW, group_width, D), precision=highest)
    mixed = lax.optimization_barrier(jnp.sum(low(low_back(mixer_parts)), axis=0))
    middle = token_rows + mixer_scale * (mixed + out_bias)
    second_normed = low(norm_rows(middle, second_gain, second_shift))
    second_groups = group_copies(second_normed)
    upper_raw = jnp.einsum('grd,dgf->rgf', second_groups, up_weight.reshape(D, N_NARROW, hidden_width), precision=highest).reshape(row_count, FF)
    upper = low_back(upper_raw + up_bias)
    active = low(jax.nn.gelu(upper, approximate=False))
    feed_parts = jnp.einsum('rgf,gfd->grd', active.reshape(row_count, N_NARROW, hidden_width), down_weight.reshape(N_NARROW, hidden_width, D), precision=highest)
    feed = lax.optimization_barrier(jnp.sum(low(low_back(feed_parts)), axis=0))
    return middle + feed_scale * (feed + down_bias)

def reference(tokens, image_lengths, heads_weight, heads_bias, out_weight, out_bias, up_weight, up_bias, down_weight, down_bias, first_gain, first_shift, second_gain, second_shift, mixer_scale, feed_scale, cotangent):
    set_count = MICRO * N_WIDE
    params = tuple((value_in.astype(jnp.float32) for value_in in (heads_weight, heads_bias, out_weight, out_bias, up_weight, up_bias, down_weight, down_bias, first_gain, first_shift, second_gain, second_shift, mixer_scale, feed_scale)))
    all_rows = tokens.astype(jnp.float32).reshape(set_count, ROWS, D)
    size_rows = image_lengths.reshape(set_count, IMAGES).astype(jnp.int32)

    def forward(param_set, row_sets):

        def one_set(running, items):
            return (running, layer_rows(param_set, items[0], items[1]))
        unused, outputs = lax.scan(jax.checkpoint(one_set), jnp.zeros((), jnp.float32), (row_sets, size_rows))
        return outputs
    outputs, pullback = jax.vjp(forward, params, all_rows)
    param_grads, row_grads = pullback(cotangent.astype(jnp.float32).reshape(set_count, ROWS, D))
    layer_out = outputs.reshape(MICRO, N_WIDE * ROWS, D).astype(jnp.bfloat16)
    token_grad = row_grads.reshape(MICRO, N_WIDE * ROWS, D).astype(jnp.bfloat16)
    return (layer_out, token_grad, param_grads[0], param_grads[1], param_grads[2], param_grads[3], param_grads[4], param_grads[5], param_grads[6], param_grads[7], param_grads[8], param_grads[9], param_grads[10], param_grads[11], param_grads[12], param_grads[13])
```

```python
import math
from functools import partial

import jax
import jax.numpy as jnp
from jax import lax
from jax.experimental import pallas as pl
from jax.experimental.pallas import tpu as pltpu
from jax.sharding import PartitionSpec as P

HEAD_DIM = 64
MOST = 196
epsilon = 1e-06
bf16 = jnp.bfloat16
f32 = jnp.float32
LOG2E = math.log2(math.e)
VMEM_LIMIT = 60 * 1024 * 1024


def round_up(value, step):
    return -(-value // step) * step


def nt(left, right):
    return lax.dot_general(left, right, (((1,), (1,)), ((), ())), preferred_element_type=f32)


def tn(left, right):
    return lax.dot_general(left, right, (((0,), (0,)), ((), ())), preferred_element_type=f32)


def nn(left, right):
    return jnp.dot(left, right, preferred_element_type=f32)


def params():
    return pltpu.CompilerParams(
        dimension_semantics=("arbitrary",), vmem_limit_bytes=VMEM_LIMIT
    )


def cost(flops, transcendentals, moved):
    return pl.CostEstimate(
        flops=int(flops), transcendentals=int(transcendentals), bytes_accessed=int(moved)
    )


def full(shape):
    return pl.BlockSpec(shape, lambda *a: (0,) * len(shape))


def per_micro(shape):
    return pl.BlockSpec((1,) + shape, lambda m, *a: (m,) + (0,) * len(shape))


def stack_heads(rows, heads):
    lane = lax.broadcasted_iota(jnp.int32, rows.shape, 1) // HEAD_DIM
    zero = jnp.zeros_like(rows)
    return jnp.concatenate([jnp.where(lane == h, rows, zero) for h in range(heads)], axis=0)


def unstack_heads(stacked, heads):
    rows = stacked.shape[0] // heads
    lane = lax.broadcasted_iota(jnp.int32, (rows, stacked.shape[1]), 1) // HEAD_DIM
    out = stacked[:rows]
    for h in range(1, heads):
        out = jnp.where(lane == h, stacked[h * rows : (h + 1) * rows], out)
    return out


def attend_kernel(own, heads, groups, first, off_ref, *refs):
    count = len(groups)
    x_ref, b_ref, bnd_ref = refs[:3]
    w_refs = refs[3 : 3 + count]
    rest = refs[3 + count + (0 if first else 1) :]
    mixed_ref = rest[0]
    off = pl.multiple_of(off_ref[0], 16)
    win = x_ref.shape[1]
    cols = heads * HEAD_DIM
    xw = x_ref[0]
    xo = x_ref[0, pl.ds(off, own), :]
    place = lax.broadcasted_iota(jnp.int32, (win, heads * own), 0)
    keep = (place >= bnd_ref[0, 0:1]) & (place < bnd_ref[0, 1:2])
    mixed = None if first else refs[3 + count][0]
    for i in range(count):
        q_ref, k_ref, v_ref, o_ref, l_ref = rest[1 + 5 * i : 6 + 5 * i]
        w = w_refs[i]
        both = nn(xw, w[:, : 2 * cols])
        k = both[:, :cols].astype(bf16)
        v = (both[:, cols:] + b_ref[groups[i], 1:2]).astype(bf16)
        q = (nn(xo, w[:, 2 * cols : 3 * cols]) + b_ref[groups[i], 0:1]).astype(bf16)
        q_ref[0] = q
        k_ref[0] = k
        v_ref[0] = v
        qs = stack_heads(q, heads)
        scores = nt(k, qs) * (HEAD_DIM**-0.5 * LOG2E)
        scores = jnp.where(keep, scores, -1e30)
        top = jnp.max(scores, axis=0, keepdims=True)
        weights = jnp.exp2(scores - top)
        total = jnp.sum(weights, axis=0, keepdims=True)
        out = tn(v, weights.astype(bf16)) * (1.0 / total)
        out = unstack_heads(out.T, heads).astype(bf16)
        o_ref[0] = out
        l_ref[0] = top + jnp.log2(total)
        part = nt(out, w[:, 3 * cols :])
        mixed = part if mixed is None else mixed + part
    mixed_ref[0] = mixed


def attend(off, x_win, pieces, bias, bounds, own, groups, mixed):
    micro, win, width = x_win.shape
    cols = pieces[0].shape[1] // 4
    heads = cols // HEAD_DIM
    stacked = heads * own
    count = len(groups)
    first = mixed is None
    shapes = [jax.ShapeDtypeStruct((micro, own, width), f32)]
    specs = [per_micro((own, width))]
    for _ in groups:
        for rows in (own, win, win, own):
            shapes.append(jax.ShapeDtypeStruct((micro, rows, cols), bf16))
            specs.append(per_micro((rows, cols)))
        shapes.append(jax.ShapeDtypeStruct((micro, 1, stacked), f32))
        specs.append(per_micro((1, stacked)))
    args = [x_win, bias, bounds] + list(pieces)
    in_specs = [per_micro((win, width)), full(bias.shape), per_micro((2, stacked))]
    in_specs += [full((width, 4 * cols))] * count
    if not first:
        args.append(mixed)
        in_specs.append(per_micro((own, width)))
    result = pl.pallas_call(
        partial(attend_kernel, own, heads, groups, first),
        grid_spec=pltpu.PrefetchScalarGridSpec(
            num_scalar_prefetch=1, grid=(micro,), in_specs=in_specs, out_specs=specs
        ),
        out_shape=shapes,
        compiler_params=params(),
        cost_estimate=cost(
            count * micro * 2 * (win * width * cols * 3 + 8 * stacked * win * HEAD_DIM),
            count * micro * stacked * win,
            micro * win * width * 2 + count * 4 * width * cols * 2,
        ),
        name="attend",
    )(off, *args)
    return result[0], [tuple(result[1 + 5 * i : 6 + 5 * i]) for i in range(count)]


def attend_back_kernel(own, heads, count, first, off_ref, *refs):
    x_ref, mg_ref, bnd_ref = refs[:3]
    w_refs = refs[3 : 3 + count]
    saved = refs[3 + count : 3 + 6 * count]
    at = 3 + 6 * count
    in_ref = None if first else refs[at]
    rest = refs[at + (0 if first else 1) :]
    dn_ref = rest[0]
    acc_refs = rest[1 + 2 * count :]
    off = pl.multiple_of(off_ref[0], 16)
    win = x_ref.shape[1]
    cols = heads * HEAD_DIM
    scale = HEAD_DIM**-0.5
    step = pl.program_id(0)
    mg = mg_ref[0]
    xw = x_ref[0]
    xt = xw.T
    xot = x_ref[0, pl.ds(off, own), :].T
    mgt = mg.T
    place = lax.broadcasted_iota(jnp.int32, (win, heads * own), 0)
    keep = (place >= bnd_ref[0, 0:1]) & (place < bnd_ref[0, 1:2])
    dn = None if first else in_ref[0]
    dn_own = None
    for i in range(count):
        w = w_refs[i]
        q_ref, k_ref, v_ref, o_ref, l_ref = saved[5 * i : 5 * i + 5]
        dw_ref, db_ref = rest[1 + 2 * i : 3 + 2 * i]
        acc_ref = acc_refs[i]
        k, v, o = k_ref[0], v_ref[0], o_ref[0]
        g = nn(mg, w[:, 3 * cols :]).astype(bf16)
        qs = stack_heads(q_ref[0], heads)
        gs = stack_heads(g, heads)
        both = gs.astype(f32) * jnp.concatenate([o.astype(f32)] * heads, axis=0)
        delta = lax.dot_general(
            jnp.ones((8, both.shape[1]), f32), both, (((1,), (1,)), ((), ())),
            precision=lax.Precision.HIGHEST, preferred_element_type=f32,
        )[0:1]
        scores = nt(k, qs) * (scale * LOG2E) - l_ref[0]
        weights = jnp.exp2(jnp.where(keep, scores, -1e30))
        slope = (weights * (nt(v, gs) - delta)).astype(bf16)
        low = weights.astype(bf16)
        dq = (unstack_heads(tn(k, slope).T, heads) * scale).astype(bf16)
        dkv = jnp.concatenate([nn(slope, qs) * scale, nn(low, gs)], axis=1).astype(bf16)
        part = nt(dkv, w[:, : 2 * cols])
        dn = part if dn is None else dn + part
        part = nt(dq, w[:, 2 * cols : 3 * cols])
        dn_own = part if dn_own is None else dn_own + part
        left = nn(xt, dkv)
        right = jnp.concatenate([nn(xot, dq), nn(mgt, o)], axis=1)
        sums = jnp.concatenate(
            [
                jnp.sum(dkv.astype(f32), axis=0, keepdims=True),
                jnp.sum(jnp.concatenate([dq, dq], axis=1).astype(f32), axis=0, keepdims=True),
            ],
            axis=1,
        )

        @pl.when(step == 0)
        def _():
            acc_ref[:, : 2 * cols] = left
            acc_ref[:, 2 * cols :] = right
            db_ref[...] = sums

        @pl.when(step > 0)
        def _():
            acc_ref[:, : 2 * cols] += left
            acc_ref[:, 2 * cols :] += right
            db_ref[...] += sums

        @pl.when(step == pl.num_programs(0) - 1)
        def _():
            dw_ref[...] = acc_ref[...].astype(bf16)

    dn_ref[0] = dn
    dn_ref[0, pl.ds(off, own), :] += dn_own


def attend_back(off, x_win, mixed_grad, pieces, saved, bounds, grad_in):
    micro, win, width = x_win.shape
    own = mixed_grad.shape[1]
    cols = pieces[0].shape[1] // 4
    heads = cols // HEAD_DIM
    stacked = heads * own
    count = len(pieces)
    first = grad_in is None
    args = [x_win, mixed_grad, bounds] + list(pieces)
    in_specs = [per_micro((win, width)), per_micro((own, width)), per_micro((2, stacked))]
    in_specs += [full((width, 4 * cols))] * count
    for one in saved:
        args += list(one)
        in_specs += [per_micro((rows, cols)) for rows in (own, win, win, own)]
        in_specs.append(per_micro((1, stacked)))
    if not first:
        args.append(grad_in)
        in_specs.append(per_micro((win, width)))
    shapes = [jax.ShapeDtypeStruct((micro, win, width), f32)]
    specs = [per_micro((win, width))]
    for _ in pieces:
        shapes += [
            jax.ShapeDtypeStruct((width, 4 * cols), bf16),
            jax.ShapeDtypeStruct((1, 4 * cols), f32),
        ]
        specs += [full((width, 4 * cols)), full((1, 4 * cols))]
    result = pl.pallas_call(
        partial(attend_back_kernel, own, heads, count, first),
        grid_spec=pltpu.PrefetchScalarGridSpec(
            num_scalar_prefetch=1,
            grid=(micro,),
            in_specs=in_specs,
            out_specs=specs,
            scratch_shapes=[pltpu.VMEM((width, 4 * cols), f32)] * count,
        ),
        out_shape=shapes,
        compiler_params=params(),
        cost_estimate=cost(
            count * micro * (40 * stacked * win * HEAD_DIM + 12 * win * width * cols),
            count * micro * stacked * win,
            micro * (10 * win) * width + count * 4 * width * cols * 4,
        ),
        name="attend_back",
    )(off, *args)
    return result[0], list(result[1::2]), list(result[2::2])


def feed_kernel(chunks, count, first, *refs):
    x_ref, g_ref = refs[:2]
    u_refs = refs[2 : 2 + count]
    d_refs = refs[2 + count : 2 + 2 * count]
    b_refs = refs[2 + 2 * count : 2 + 3 * count]
    at = 2 + 3 * count
    if not first:
        fi_ref, ni_ref = refs[at : at + 2]
        at = at + 2
    f_ref, n_ref = refs[at : at + 2]
    outs = refs[at + 2 : at + 2 + 3 * count]
    act_ref, ug_ref, xt_ref, gt_ref = refs[at + 2 + 3 * count :]
    rows = x_ref.shape[0]
    step = rows // chunks
    xt_ref[...] = x_ref[...].T
    gt_ref[...] = g_ref[...].T
    for i in range(count):
        u_ref, d_ref, b_ref = u_refs[i], d_refs[i], b_refs[i]
        du_ref, dd_ref, db_ref = outs[3 * i : 3 * i + 3]
        total = jnp.zeros((1, b_ref.shape[1]), f32)
        for c in range(chunks):
            rows_at = pl.ds(c * step, step)
            upper = nn(x_ref[rows_at, :], u_ref[...]) + b_ref[...]
            phi = 0.5 + 0.5 * lax.erf(upper * math.sqrt(0.5))
            active = (upper * phi).astype(bf16)
            bell = jnp.exp2(upper * upper * (-0.5 * LOG2E)) * (1.0 / math.sqrt(2.0 * math.pi))
            slope = phi + upper * bell
            grad = (nn(g_ref[rows_at, :], d_ref[...]) * slope).astype(bf16)
            act_ref[rows_at, :] = active
            ug_ref[rows_at, :] = grad
            total = total + jnp.sum(grad.astype(f32), axis=0, keepdims=True)
            feed = nt(active, d_ref[...])
            back = nt(grad, u_ref[...])
            if i > 0:
                feed = feed + f_ref[rows_at, :]
                back = back + n_ref[rows_at, :]
            elif not first:
                feed = feed + fi_ref[rows_at, :]
                back = back + ni_ref[rows_at, :]
            f_ref[rows_at, :] = feed
            n_ref[rows_at, :] = back
        db_ref[...] = total
        dd_ref[...] = nn(gt_ref[...], act_ref[...]).astype(bf16)
        du_ref[...] = nn(xt_ref[...], ug_ref[...]).astype(bf16)


def feed_part(x2, grad, ups, downs, biases, before):
    rows, width = x2.shape
    hidden = ups[0].shape[1]
    count = len(ups)
    first = before is None
    args = [x2, grad] + list(ups) + list(downs) + list(biases)
    aliases = {}
    if not first:
        aliases = {len(args): 0, len(args) + 1: 1}
        args += list(before)
    whole = pl.BlockSpec(memory_space=pltpu.VMEM)
    shapes = [jax.ShapeDtypeStruct((rows, width), f32)] * 2
    for _ in ups:
        shapes += [
            jax.ShapeDtypeStruct((width, hidden), bf16),
            jax.ShapeDtypeStruct((width, hidden), bf16),
            jax.ShapeDtypeStruct((1, hidden), f32),
        ]
    result = pl.pallas_call(
        partial(feed_kernel, 4, count, first),
        in_specs=[whole] * len(args),
        out_specs=[whole] * len(shapes),
        out_shape=shapes,
        scratch_shapes=[
            pltpu.VMEM((rows, hidden), bf16),
            pltpu.VMEM((rows, hidden), bf16),
            pltpu.VMEM((width, rows), bf16),
            pltpu.VMEM((width, rows), bf16),
        ],
        input_output_aliases=aliases,
        compiler_params=pltpu.CompilerParams(vmem_limit_bytes=VMEM_LIMIT),
        cost_estimate=cost(
            count * 12 * rows * width * hidden,
            count * 2 * rows * hidden,
            16 * rows * width + count * 8 * width * hidden,
        ),
        name="feed_part",
    )(*args)
    return tuple(result[:2]), list(result[2::3]), list(result[3::3]), list(result[4::3])


def norm_parts(values_in):
    center = jnp.mean(values_in, axis=-1, keepdims=True)
    shifted = values_in - center
    inverse = lax.rsqrt(jnp.mean(shifted * shifted, axis=-1, keepdims=True) + epsilon)
    return (shifted * inverse, inverse)


def norm_back(grad_in, unit_rows, inverse, gain_row):
    scaled = grad_in * gain_row
    return inverse * (
        scaled
        - jnp.mean(scaled, axis=-1, keepdims=True)
        - unit_rows * jnp.mean(scaled * unit_rows, axis=-1, keepdims=True)
    )


def swap(values_in, axis, bit):
    size = lax.axis_size(axis)
    return lax.ppermute(values_in, axis, [(i, i ^ bit) for i in range(size)])


def shift(values_in, axis, step):
    size = lax.axis_size(axis)
    pairs = [(i, i + step) for i in range(size) if 0 <= i + step < size]
    return lax.ppermute(values_in, axis, pairs)


def wide_bits(size):
    bits = []
    bit = size // 2
    while bit:
        bits.append(bit)
        bit //= 2
    return bits


def bit_of(axis, bit):
    return (lax.axis_index(axis) & bit) != 0


def join(mine, other, is_high, axis):
    low = jnp.where(is_high, other, mine)
    high = jnp.where(is_high, mine, other)
    return jnp.stack([low, high], axis=axis)


def widen(blocks, other, bit):
    pair = join(blocks, other, bit_of("wide", bit), 1)
    return pair.reshape((-1,) + blocks.shape[1:])


def gather_pieces(shard, far_first):
    bits = wide_bits(lax.axis_size("wide"))
    blocks = shard[None]
    for bit in bits[:-1]:
        blocks = widen(blocks, swap(blocks, "wide", bit), bit)
    last = bits[-1]
    if far_first:
        far = swap(blocks, "narrow", 2)
        mine = widen(blocks, swap(blocks, "wide", last), last)
        far = widen(far, swap(far, "wide", last), last)
    else:
        mine = widen(blocks, swap(blocks, "wide", last), last)
        far = swap(mine, "narrow", 2)
    mine = mine.reshape(-1, shard.shape[1])
    far = far.reshape(-1, shard.shape[1])
    return [mine, swap(mine, "narrow", 1), far, swap(far, "narrow", 1)]


def gather_narrow(piece):
    far = swap(piece, "narrow", 2)
    return [piece, swap(piece, "narrow", 1), far, swap(far, "narrow", 1)]


def add_low(left, right):
    return (left.astype(f32) + right.astype(f32)).astype(bf16)


def halve(values_in, axis, bit):
    half = values_in.shape[0] // 2
    high = bit_of(axis, bit).astype(jnp.int32)
    keep = lax.dynamic_slice_in_dim(values_in, high * half, half, 0)
    give = lax.dynamic_slice_in_dim(values_in, (1 - high) * half, half, 0)
    return keep, swap(give, axis, bit)


def spread(part):
    for bit in wide_bits(lax.axis_size("wide")):
        other = swap(part, "wide", bit)
        part = join(part, other, bit_of("wide", bit), 0).reshape((-1,) + part.shape[1:])
    return part


def reduce_pair(near_part, given_part):
    return add_low(near_part, swap(given_part, "narrow", 1))


def reduce_rest(near, far, narrow_last):
    bits = list(reversed(wide_bits(lax.axis_size("wide"))))
    if narrow_last:
        keep, other = halve(near, "wide", bits[0])
        far_keep, far_other = halve(far, "wide", bits[0])
        far = add_low(far_keep, far_other)
        near = add_low(keep, other)
        bits = bits[1:]
    mine = add_low(near, swap(far, "narrow", 2))
    if narrow_last:
        bits = list(bits)
    for bit in bits:
        keep, other = halve(mine, "wide", bit)
        mine = add_low(keep, other)
    return spread(mine)


def reduce_everywhere(values_in):
    for bit in wide_bits(lax.axis_size("wide")):
        values_in = values_in + swap(values_in, "wide", bit)
    for bit in wide_bits(lax.axis_size("narrow")):
        values_in = values_in + swap(values_in, "narrow", bit)
    return values_in


def body(
    tokens, image_lengths, heads_weight, heads_bias, out_weight, out_bias, up_weight, up_bias,
    down_weight, down_bias, first_gain, first_shift, second_gain, second_shift, mixer_scale,
    feed_scale, cotangent,
):
    micro, row_count, width = tokens.shape
    narrow_size = lax.axis_size("narrow")
    narrow_at = lax.axis_index("narrow")
    own = row_count // narrow_size
    cols = heads_weight.shape[2]
    heads = cols // HEAD_DIM
    rows = micro * own
    halo = round_up(MOST - 1, 16)
    window = min(row_count, round_up(own + 2 * halo, 128))
    lead = round_up((window - own) // 2, 16)
    start = jnp.clip(narrow_at * own - lead, 0, row_count - window)
    off = narrow_at * own - start
    offset = off.reshape(1).astype(jnp.int32)

    shard_heads = jnp.concatenate(
        [heads_weight[:, 1], heads_weight[:, 2], heads_weight[:, 0], out_weight.T], axis=1
    )
    heads_pieces = gather_pieces(shard_heads, False)
    bias_pieces = gather_narrow(
        jnp.concatenate([heads_bias.reshape(-1), up_bias]).reshape(1, -1)
    )
    up_pieces = gather_pieces(up_weight, True)
    down_pieces = gather_pieces(down_weight.T, False)
    qv_bias = jnp.stack([b[0, : 2 * cols].reshape(2, cols) for b in bias_pieces])
    up_biases = [b[:, 2 * cols :] for b in bias_pieces]

    ends = jnp.cumsum(image_lengths[:, 0], axis=1)
    places = narrow_at * own + jnp.arange(own, dtype=jnp.int32)
    passed = ends[:, :, None] <= places[None, None, :]
    first_key = jnp.max(jnp.where(passed, ends[:, :, None], 0), axis=1) - start
    last_key = jnp.min(jnp.where(passed, row_count, ends[:, :, None]), axis=1) - start
    bounds = jnp.tile(jnp.stack([first_key, last_key], axis=1), (1, 1, heads)).astype(jnp.int32)

    token_window = lax.dynamic_slice_in_dim(tokens, start, window, 1).astype(f32)
    window_normed = (norm_parts(token_window)[0] * first_gain + first_shift).astype(bf16)
    output_grad = lax.dynamic_slice_in_dim(cotangent, narrow_at * own, own, 1)
    output_grad = output_grad.reshape(rows, width).astype(f32)
    feed_grad = (feed_scale * output_grad).astype(bf16)
    token_rows = lax.dynamic_slice_in_dim(tokens, narrow_at * own, own, 1)
    token_rows = token_rows.reshape(rows, width).astype(f32)

    mixed, near_saved = attend(
        offset, window_normed, heads_pieces[:2], qv_bias, bounds, own, (0, 1), None
    )
    mixed, far_saved = attend(
        offset, window_normed, heads_pieces[2:], qv_bias, bounds, own, (2, 3), mixed
    )
    branch = mixed.reshape(rows, width) + out_bias
    middle = token_rows + mixer_scale * branch
    second_unit, second_inverse = norm_parts(middle)
    second_normed = (second_unit * second_gain + second_shift).astype(bf16)

    sums, far_up, far_down, far_bias = feed_part(
        second_normed, feed_grad, up_pieces[2:], down_pieces[2:], up_biases[2:], None
    )
    far_down_sum = reduce_pair(*far_down)
    far_up_sum = reduce_pair(*far_up)
    sums, near_up, near_down, near_bias = feed_part(
        second_normed, feed_grad, up_pieces[:2], down_pieces[:2], up_biases[:2], sums
    )
    feed, second_normed_grad = sums
    up_bias_parts = near_bias + far_bias
    down_total = reduce_rest(reduce_pair(*near_down), far_down_sum, False)
    up_total = reduce_rest(reduce_pair(*near_up), far_up_sum, True)

    feed_branch = feed + down_bias
    layer_own = (middle + feed_scale * feed_branch).astype(bf16).reshape(micro, own, width)
    y_high, core_high = bit_of("narrow", 2), bit_of("narrow", 1)
    layer_far = swap(layer_own, "narrow", 2)
    layer_near = join(layer_own, swap(layer_own, "narrow", 1), core_high, 1)
    layer_far = join(layer_far, swap(layer_far, "narrow", 1), core_high, 1)
    layer_out = join(layer_near, layer_far, y_high, 1).reshape(micro, row_count, width)

    feed_scale_sum = jnp.sum(output_grad * feed_branch, axis=0)
    down_bias_sum = feed_scale * jnp.sum(output_grad, axis=0)
    second_gain_sum = jnp.sum(second_normed_grad * second_unit, axis=0)
    second_shift_sum = jnp.sum(second_normed_grad, axis=0)
    middle_grad = output_grad + norm_back(second_normed_grad, second_unit, second_inverse, second_gain)
    mixer_scale_sum = jnp.sum(middle_grad * branch, axis=0)
    out_bias_sum = mixer_scale * jnp.sum(middle_grad, axis=0)
    mixed_grad = (mixer_scale * middle_grad).astype(bf16).reshape(micro, own, width)

    window_grad, far_heads, far_sums = attend_back(
        offset, window_normed, mixed_grad, heads_pieces[2:], far_saved, bounds, None
    )
    far_heads_sum = reduce_pair(*far_heads)
    window_grad, near_heads, near_sums = attend_back(
        offset, window_normed, mixed_grad, heads_pieces[:2], near_saved, bounds, window_grad
    )
    heads_total = reduce_rest(reduce_pair(*near_heads), far_heads_sum, False)
    head_bias_parts = [
        jnp.concatenate([s[0, 2 * cols : 3 * cols], s[0, cols : 2 * cols]])
        for s in near_sums + far_sums
    ]

    before = lax.dynamic_slice_in_dim(window_grad, jnp.maximum(off - halo, 0), halo, 1)
    after = lax.dynamic_slice_in_dim(
        window_grad, jnp.minimum(off + own, window - halo), halo, 1
    )
    from_left = shift(after.astype(bf16), "narrow", 1).astype(f32)
    from_right = shift(before.astype(bf16), "narrow", -1).astype(f32)
    first_normed_grad = lax.dynamic_slice_in_dim(window_grad, off, own, 1)
    first_normed_grad = (
        first_normed_grad
        + jnp.pad(from_left, ((0, 0), (0, own - halo), (0, 0)))
        + jnp.pad(from_right, ((0, 0), (own - halo, 0), (0, 0)))
    ).reshape(rows, width)

    first_unit, first_inverse = norm_parts(token_rows)
    first_gain_sum = jnp.sum(first_normed_grad * first_unit, axis=0)
    first_shift_sum = jnp.sum(first_normed_grad, axis=0)
    token_grad = (
        middle_grad + norm_back(first_normed_grad, first_unit, first_inverse, first_gain)
    ).astype(bf16).reshape(micro, own, width)

    sums = jnp.stack(
        [out_bias_sum, down_bias_sum, first_gain_sum, first_shift_sum, second_gain_sum,
         second_shift_sum, mixer_scale_sum, feed_scale_sum]
    )
    group_sums = jnp.stack(
        [jnp.concatenate([head_bias_parts[r], up_bias_parts[r][0]]) for r in range(narrow_size)]
    )
    group_sums = jnp.stack([group_sums[r ^ narrow_at] for r in range(narrow_size)])
    packed = jnp.concatenate([sums.reshape(-1), group_sums.reshape(-1)]).reshape(-1, 128)
    packed = reduce_everywhere(packed).reshape(-1)
    sums = packed[: 8 * width].reshape(8, width)
    group_sums = packed[8 * width :].reshape(narrow_size, -1)
    mine = lax.dynamic_slice_in_dim(group_sums, narrow_at, 1, 0)[0]

    heads_grad = jnp.stack(
        [heads_total[:, 2 * cols : 3 * cols], heads_total[:, :cols], heads_total[:, cols : 2 * cols]],
        axis=1,
    ).astype(f32)
    out_grad = heads_total[:, 3 * cols :].T.astype(f32)
    return (
        layer_out, token_grad, heads_grad, mine[: 2 * cols].reshape(2, cols), out_grad, sums[0],
        up_total.astype(f32), mine[2 * cols :], down_total.T.astype(f32), sums[1], sums[2],
        sums[3], sums[4], sums[5], sums[6], sums[7],
    )


def solution(mesh):
    return jax.shard_map(
        body,
        mesh=mesh,
        in_specs=(
            P(None, "wide", None),
            P(None, "wide", None),
            P("wide", None, "narrow"),
            P(None, "narrow"),
            P("narrow", "wide"),
            P(),
            P("wide", "narrow"),
            P("narrow"),
            P("narrow", "wide"),
            P(),
            P(),
            P(),
            P(),
            P(),
            P(),
            P(),
            P(None, "wide", None),
        ),
        out_specs=(
            P(None, "wide", None),
            P(None, ("wide", "narrow"), None),
            P(None, None, "narrow"),
            P(None, "narrow"),
            P("narrow", None),
            P(),
            P(None, "narrow"),
            P("narrow"),
            P("narrow", None),
            P(),
            P(),
            P(),
            P(),
            P(),
            P(),
            P(),
        ),
        check_vma=False,
    )
```

```python
import math
from functools import partial

import jax
import jax.numpy as jnp
from jax import lax
from jax.experimental import pallas as pl
from jax.experimental.pallas import tpu as pltpu
from jax.sharding import PartitionSpec as P

HEAD_DIM = 64
MOST = 196
epsilon = 1e-06
bf16 = jnp.bfloat16
f32 = jnp.float32
LOG2E = math.log2(math.e)
VMEM_LIMIT = 60 * 1024 * 1024


def round_up(value, step):
    return -(-value // step) * step


def nt(left, right):
    return lax.dot_general(left, right, (((1,), (1,)), ((), ())), preferred_element_type=f32)


def tn(left, right):
    return lax.dot_general(left, right, (((0,), (0,)), ((), ())), preferred_element_type=f32)


def nn(left, right):
    return jnp.dot(left, right, preferred_element_type=f32)


def params():
    return pltpu.CompilerParams(
        dimension_semantics=("arbitrary",), vmem_limit_bytes=VMEM_LIMIT
    )


def cost(flops, transcendentals, moved):
    return pl.CostEstimate(
        flops=int(flops), transcendentals=int(transcendentals), bytes_accessed=int(moved)
    )


def full(shape):
    return pl.BlockSpec(shape, lambda *a: (0,) * len(shape))


def per_micro(shape):
    return pl.BlockSpec((1,) + shape, lambda m, *a: (m,) + (0,) * len(shape))


def stack_heads(rows, heads):
    lane = lax.broadcasted_iota(jnp.int32, rows.shape, 1) // HEAD_DIM
    zero = jnp.zeros_like(rows)
    return jnp.concatenate([jnp.where(lane == h, rows, zero) for h in range(heads)], axis=0)


def unstack_heads(stacked, heads):
    rows = stacked.shape[0] // heads
    lane = lax.broadcasted_iota(jnp.int32, (rows, stacked.shape[1]), 1) // HEAD_DIM
    out = stacked[:rows]
    for h in range(1, heads):
        out = jnp.where(lane == h, stacked[h * rows : (h + 1) * rows], out)
    return out


def attend_kernel(own, heads, count, first, off_ref, *refs):
    x_ref, b_ref, bnd_ref = refs[:3]
    w_refs = refs[3 : 3 + count]
    rest = refs[3 + count + (0 if first else 1) :]
    mixed_ref = rest[0]
    off = pl.multiple_of(off_ref[0], 16)
    win = x_ref.shape[1]
    cols = heads * HEAD_DIM
    xw = x_ref[0]
    xo = x_ref[0, pl.ds(off, own), :]
    place = lax.broadcasted_iota(jnp.int32, (win, heads * own), 0)
    keep = (place >= bnd_ref[0, 0:1]) & (place < bnd_ref[0, 1:2])
    mixed = None if first else refs[3 + count][0]
    for i in range(count):
        q_ref, k_ref, v_ref, o_ref, l_ref = rest[1 + 5 * i : 6 + 5 * i]
        w = w_refs[i]
        both = nn(xw, w[:, : 2 * cols])
        k = both[:, :cols].astype(bf16)
        v = (both[:, cols:] + b_ref[i, 1:2]).astype(bf16)
        q = (nn(xo, w[:, 2 * cols : 3 * cols]) + b_ref[i, 0:1]).astype(bf16)
        q_ref[0] = q
        k_ref[0] = k
        v_ref[0] = v
        qs = stack_heads(q, heads)
        scores = nt(k, qs) * (HEAD_DIM**-0.5 * LOG2E)
        scores = jnp.where(keep, scores, -1e30)
        top = jnp.max(scores, axis=0, keepdims=True)
        weights = jnp.exp2(scores - top)
        total = jnp.sum(weights, axis=0, keepdims=True)
        out = tn(v, weights.astype(bf16)) * (1.0 / total)
        out = unstack_heads(out.T, heads).astype(bf16)
        o_ref[0] = out
        l_ref[0] = top + jnp.log2(total)
        part = nt(out, w[:, 3 * cols :])
        mixed = part if mixed is None else mixed + part
    mixed_ref[0] = mixed


def attend(off, x_win, pieces, bias, bounds, own, mixed):
    micro, win, width = x_win.shape
    cols = pieces[0].shape[1] // 4
    heads = cols // HEAD_DIM
    stacked = heads * own
    count = len(pieces)
    first = mixed is None
    shapes = [jax.ShapeDtypeStruct((micro, own, width), f32)]
    specs = [per_micro((own, width))]
    for _ in pieces:
        for rows in (own, win, win, own):
            shapes.append(jax.ShapeDtypeStruct((micro, rows, cols), bf16))
            specs.append(per_micro((rows, cols)))
        shapes.append(jax.ShapeDtypeStruct((micro, 1, stacked), f32))
        specs.append(per_micro((1, stacked)))
    args = [x_win, bias, bounds] + list(pieces)
    in_specs = [per_micro((win, width)), full(bias.shape), per_micro((2, stacked))]
    in_specs += [full((width, 4 * cols))] * count
    if not first:
        args.append(mixed)
        in_specs.append(per_micro((own, width)))
    result = pl.pallas_call(
        partial(attend_kernel, own, heads, count, first),
        grid_spec=pltpu.PrefetchScalarGridSpec(
            num_scalar_prefetch=1, grid=(micro,), in_specs=in_specs, out_specs=specs
        ),
        out_shape=shapes,
        compiler_params=params(),
        cost_estimate=cost(
            count * micro * 2 * (win * width * cols * 3 + 8 * stacked * win * HEAD_DIM),
            count * micro * stacked * win,
            micro * win * width * 2 + count * 4 * width * cols * 2,
        ),
        name="attend",
    )(off, *args)
    return result[0], [tuple(result[1 + 5 * i : 6 + 5 * i]) for i in range(count)]


def attend_back_kernel(own, heads, count, first, off_ref, *refs):
    xt_ref, xot_ref, mg_ref, mgt_ref, bnd_ref = refs[:5]
    w_refs = refs[5 : 5 + count]
    saved = refs[5 + count : 5 + 6 * count]
    at = 5 + 6 * count
    in_ref = None if first else refs[at]
    rest = refs[at + (0 if first else 1) :]
    dn_ref = rest[0]
    acc_refs = rest[1 + 2 * count :]
    off = pl.multiple_of(off_ref[0], 16)
    win = xt_ref.shape[2]
    cols = heads * HEAD_DIM
    scale = HEAD_DIM**-0.5
    step = pl.program_id(0)
    mg = mg_ref[0]
    place = lax.broadcasted_iota(jnp.int32, (win, heads * own), 0)
    keep = (place >= bnd_ref[0, 0:1]) & (place < bnd_ref[0, 1:2])
    dn = None if first else in_ref[0]
    dn_own = None
    for i in range(count):
        w = w_refs[i]
        q_ref, k_ref, v_ref, o_ref, l_ref = saved[5 * i : 5 * i + 5]
        dw_ref, db_ref = rest[1 + 2 * i : 3 + 2 * i]
        acc_ref = acc_refs[i]
        k, v, o = k_ref[0], v_ref[0], o_ref[0]
        g = nn(mg, w[:, 3 * cols :]).astype(bf16)
        qs = stack_heads(q_ref[0], heads)
        gs = stack_heads(g, heads)
        both = gs.astype(f32) * jnp.concatenate([o.astype(f32)] * heads, axis=0)
        delta = lax.dot_general(
            jnp.ones((8, both.shape[1]), f32), both, (((1,), (1,)), ((), ())),
            precision=lax.Precision.HIGHEST, preferred_element_type=f32,
        )[0:1]
        scores = nt(k, qs) * (scale * LOG2E) - l_ref[0]
        weights = jnp.exp2(jnp.where(keep, scores, -1e30))
        slope = (weights * (nt(v, gs) - delta)).astype(bf16)
        low = weights.astype(bf16)
        dq = (unstack_heads(tn(k, slope).T, heads) * scale).astype(bf16)
        dkv = jnp.concatenate([nn(slope, qs) * scale, nn(low, gs)], axis=1).astype(bf16)
        part = nt(dkv, w[:, : 2 * cols])
        dn = part if dn is None else dn + part
        part = nt(dq, w[:, 2 * cols : 3 * cols])
        dn_own = part if dn_own is None else dn_own + part
        left = nn(xt_ref[0], dkv)
        right = jnp.concatenate([nn(xot_ref[0], dq), nn(mgt_ref[0], o)], axis=1)
        sums = jnp.concatenate(
            [
                jnp.sum(dkv.astype(f32), axis=0, keepdims=True),
                jnp.sum(jnp.concatenate([dq, dq], axis=1).astype(f32), axis=0, keepdims=True),
            ],
            axis=1,
        )

        @pl.when(step == 0)
        def _():
            acc_ref[:, : 2 * cols] = left
            acc_ref[:, 2 * cols :] = right
            db_ref[...] = sums

        @pl.when(step > 0)
        def _():
            acc_ref[:, : 2 * cols] += left
            acc_ref[:, 2 * cols :] += right
            db_ref[...] += sums

        @pl.when(step == pl.num_programs(0) - 1)
        def _():
            dw_ref[...] = acc_ref[...].astype(bf16)

    dn_ref[0] = dn
    dn_ref[0, pl.ds(off, own), :] += dn_own


def attend_back(off, xt, xot, mixed_grad, mgt, pieces, saved, bounds, grad_in):
    micro, width, win = xt.shape
    own = mixed_grad.shape[1]
    cols = pieces[0].shape[1] // 4
    heads = cols // HEAD_DIM
    stacked = heads * own
    count = len(pieces)
    first = grad_in is None
    args = [xt, xot, mixed_grad, mgt, bounds] + list(pieces)
    in_specs = [
        per_micro((width, win)), per_micro((width, own)), per_micro((own, width)),
        per_micro((width, own)), per_micro((2, stacked)),
    ]
    in_specs += [full((width, 4 * cols))] * count
    for one in saved:
        args += list(one)
        in_specs += [per_micro((rows, cols)) for rows in (own, win, win, own)]
        in_specs.append(per_micro((1, stacked)))
    if not first:
        args.append(grad_in)
        in_specs.append(per_micro((win, width)))
    shapes = [jax.ShapeDtypeStruct((micro, win, width), f32)]
    specs = [per_micro((win, width))]
    for _ in pieces:
        shapes += [
            jax.ShapeDtypeStruct((width, 4 * cols), bf16),
            jax.ShapeDtypeStruct((1, 4 * cols), f32),
        ]
        specs += [full((width, 4 * cols)), full((1, 4 * cols))]
    result = pl.pallas_call(
        partial(attend_back_kernel, own, heads, count, first),
        grid_spec=pltpu.PrefetchScalarGridSpec(
            num_scalar_prefetch=1,
            grid=(micro,),
            in_specs=in_specs,
            out_specs=specs,
            scratch_shapes=[pltpu.VMEM((width, 4 * cols), f32)] * count,
        ),
        out_shape=shapes,
        compiler_params=params(),
        cost_estimate=cost(
            count * micro * (40 * stacked * win * HEAD_DIM + 12 * win * width * cols),
            count * micro * stacked * win,
            micro * (10 * win) * width + count * 4 * width * cols * 4,
        ),
        name="attend_back",
    )(off, *args)
    return result[0], list(result[1::2]), list(result[2::2])


def feed_kernel(chunks, count, first, *refs):
    x_ref, g_ref, xt_ref, gt_ref = refs[:4]
    w_refs = refs[4 : 4 + count]
    b_refs = refs[4 + count : 4 + 2 * count]
    at = 4 + 2 * count
    if not first:
        fi_ref, ni_ref = refs[at : at + 2]
        at = at + 2
    f_ref, n_ref = refs[at : at + 2]
    outs = refs[at + 2 : at + 2 + 2 * count]
    act_ref, ug_ref = refs[at + 2 + 2 * count :]
    rows = x_ref.shape[0]
    step = rows // chunks
    for i in range(count):
        w_ref, b_ref = w_refs[i], b_refs[i]
        dw_ref, db_ref = outs[2 * i : 2 * i + 2]
        hidden = b_ref.shape[1]
        total = jnp.zeros((1, hidden), f32)
        for c in range(chunks):
            rows_at = pl.ds(c * step, step)
            upper = nn(x_ref[rows_at, :], w_ref[:, :hidden]) + b_ref[...]
            phi = 0.5 + 0.5 * lax.erf(upper * math.sqrt(0.5))
            active = (upper * phi).astype(bf16)
            bell = jnp.exp2(upper * upper * (-0.5 * LOG2E)) * (1.0 / math.sqrt(2.0 * math.pi))
            slope = phi + upper * bell
            grad = (nn(g_ref[rows_at, :], w_ref[:, hidden:]) * slope).astype(bf16)
            act_ref[rows_at, :] = active
            ug_ref[rows_at, :] = grad
            total = total + jnp.sum(grad.astype(f32), axis=0, keepdims=True)
            feed = nt(active, w_ref[:, hidden:])
            back = nt(grad, w_ref[:, :hidden])
            if i > 0:
                feed = feed + f_ref[rows_at, :]
                back = back + n_ref[rows_at, :]
            elif not first:
                feed = feed + fi_ref[rows_at, :]
                back = back + ni_ref[rows_at, :]
            f_ref[rows_at, :] = feed
            n_ref[rows_at, :] = back
        db_ref[...] = total
        dw_ref[:, :hidden] = nn(xt_ref[...], ug_ref[...]).astype(bf16)
        dw_ref[:, hidden:] = nn(gt_ref[...], act_ref[...]).astype(bf16)


def feed_part(x2, grad, x2t, gradt, pieces, biases, before):
    rows, width = x2.shape
    hidden = biases[0].shape[1]
    count = len(pieces)
    first = before is None
    args = [x2, grad, x2t, gradt] + list(pieces) + list(biases)
    aliases = {}
    if not first:
        aliases = {len(args): 0, len(args) + 1: 1}
        args += list(before)
    whole = pl.BlockSpec(memory_space=pltpu.VMEM)
    shapes = [jax.ShapeDtypeStruct((rows, width), f32)] * 2
    for _ in pieces:
        shapes += [
            jax.ShapeDtypeStruct((width, 2 * hidden), bf16),
            jax.ShapeDtypeStruct((1, hidden), f32),
        ]
    result = pl.pallas_call(
        partial(feed_kernel, 4, count, first),
        in_specs=[whole] * len(args),
        out_specs=[whole] * len(shapes),
        out_shape=shapes,
        scratch_shapes=[pltpu.VMEM((rows, hidden), bf16), pltpu.VMEM((rows, hidden), bf16)],
        input_output_aliases=aliases,
        compiler_params=pltpu.CompilerParams(vmem_limit_bytes=VMEM_LIMIT),
        cost_estimate=cost(
            count * 12 * rows * width * hidden,
            count * 2 * rows * hidden,
            16 * rows * width + count * 8 * width * hidden,
        ),
        name="feed_part",
    )(*args)
    return tuple(result[:2]), list(result[2::2]), list(result[3::2])


def norm_parts(values_in):
    center = jnp.mean(values_in, axis=-1, keepdims=True)
    shifted = values_in - center
    inverse = lax.rsqrt(jnp.mean(shifted * shifted, axis=-1, keepdims=True) + epsilon)
    return (shifted * inverse, inverse)


def norm_back(grad_in, unit_rows, inverse, gain_row):
    scaled = grad_in * gain_row
    return inverse * (
        scaled
        - jnp.mean(scaled, axis=-1, keepdims=True)
        - unit_rows * jnp.mean(scaled * unit_rows, axis=-1, keepdims=True)
    )


def swap(values_in, axis, bit):
    size = lax.axis_size(axis)
    return lax.ppermute(values_in, axis, [(i, i ^ bit) for i in range(size)])


def shift(values_in, axis, step):
    size = lax.axis_size(axis)
    pairs = [(i, i + step) for i in range(size) if 0 <= i + step < size]
    return lax.ppermute(values_in, axis, pairs)


def wide_bits(size):
    bits = []
    bit = size // 2
    while bit:
        bits.append(bit)
        bit //= 2
    return bits


def bit_of(axis, bit):
    return (lax.axis_index(axis) & bit) != 0


def join(mine, other, is_high, axis):
    low = jnp.where(is_high, other, mine)
    high = jnp.where(is_high, mine, other)
    return jnp.stack([low, high], axis=axis)


def tie(*values_in):
    return lax.optimization_barrier(values_in)


def far_groups():
    bits = wide_bits(lax.axis_size("wide"))[:-1]
    return [bits[i : i + 2] for i in range(0, len(bits), 2)]


def offsets(bits):
    return [
        sum(bit for i, bit in enumerate(reversed(bits)) if (k >> i) & 1)
        for k in range(2 ** len(bits))
    ]


def exchange(values_in, bits):
    return [values_in] + [swap(values_in, "wide", o) for o in offsets(bits)[1:]]


def arrange(parts, bits, axis):
    if not bits:
        return jnp.expand_dims(parts[0], axis)
    half = len(parts) // 2
    low = arrange(parts[:half], bits[1:], axis)
    high = arrange(parts[half:], bits[1:], axis)
    is_high = bit_of("wide", bits[0])
    return jnp.concatenate(
        [jnp.where(is_high, high, low), jnp.where(is_high, low, high)], axis=axis
    )


def arrange_blocks(parts, bits):
    return arrange(parts, bits, 1).reshape((-1,) + parts[0].shape[1:])


def last_bit():
    return wide_bits(lax.axis_size("wide"))[-1]


def gather_narrow(piece):
    far = swap(piece, "narrow", 2)
    return [piece, swap(piece, "narrow", 1), far, swap(far, "narrow", 1)]


def add_low(*parts):
    total = parts[0].astype(f32)
    for part in parts[1:]:
        total = total + part.astype(f32)
    return total.astype(bf16)


def cut(values_in, axis, bits):
    count = 2 ** len(bits)
    size = values_in.shape[0] // count
    at = lax.axis_index(axis)
    places = []
    for o in offsets(bits):
        other = at ^ o
        place = 0
        for bit in bits:
            place = 2 * place + ((other & bit) != 0).astype(jnp.int32)
        places.append(place)
    return [lax.dynamic_slice_in_dim(values_in, p * size, size, 0) for p in places]


def send_cut(parts, bits):
    return [swap(part, "wide", o) for part, o in zip(parts[1:], offsets(bits)[1:])]


def reduce_far(part):
    for bits in far_groups():
        parts = cut(part, "wide", bits)
        part = add_low(parts[0], *send_cut(parts, bits))
    return part


def spread_far(part):
    for bits in reversed(far_groups()):
        part = arrange(exchange(part, bits), bits, 0).reshape((-1,) + part.shape[1:])
    return part


def reduce_last(part):
    parts = cut(part, "wide", [last_bit()])
    return add_low(parts[0], *send_cut(parts, [last_bit()]))


def spread_last(part):
    bits = [last_bit()]
    return arrange(exchange(part, bits), bits, 0).reshape((-1,) + part.shape[1:])


def reduce_everywhere(values_in):
    for bit in wide_bits(lax.axis_size("wide")):
        values_in = values_in + swap(values_in, "wide", bit)
    for bit in wide_bits(lax.axis_size("narrow")):
        values_in = values_in + swap(values_in, "narrow", bit)
    return values_in


def body(
    tokens, image_lengths, heads_weight, heads_bias, out_weight, out_bias, up_weight, up_bias,
    down_weight, down_bias, first_gain, first_shift, second_gain, second_shift, mixer_scale,
    feed_scale, cotangent,
):
    micro, row_count, width = tokens.shape
    narrow_size = lax.axis_size("narrow")
    narrow_at = lax.axis_index("narrow")
    own = row_count // narrow_size
    cols = heads_weight.shape[2]
    heads = cols // HEAD_DIM
    rows = micro * own
    halo = round_up(MOST - 1, 16)
    window = min(row_count, round_up(own + 2 * halo, 128))
    lead = round_up((window - own) // 2, 16)
    start = jnp.clip(narrow_at * own - lead, 0, row_count - window)
    off = narrow_at * own - start
    offset = off.reshape(1).astype(jnp.int32)

    hidden = up_weight.shape[1]
    groups = far_groups()

    bias_pieces = gather_narrow(
        jnp.concatenate([heads_bias.reshape(-1), up_bias]).reshape(1, -1)
    )
    qv_biases = [heads_bias[None]]
    qv_biases += [b[:, : 2 * cols].reshape(1, 2, cols) for b in bias_pieces[1:]]
    up_biases = [up_bias.reshape(1, hidden)] + [b[:, 2 * cols :] for b in bias_pieces[1:]]
    heads_blocks = jnp.concatenate(
        [heads_weight[:, 1], heads_weight[:, 2], heads_weight[:, 0], out_weight.T], axis=1
    )[None]
    for bits in groups:
        heads_blocks = arrange_blocks(exchange(heads_blocks, bits), bits)
    feed_blocks = jnp.concatenate([up_weight, down_weight.T], axis=1)[None]
    heads_blocks, feed_blocks = tie(heads_blocks, feed_blocks)
    for bits in groups[:-1]:
        feed_blocks = arrange_blocks(exchange(feed_blocks, bits), bits)
    feed_parts = exchange(feed_blocks, groups[-1])
    last = [last_bit()]
    heads_own = arrange_blocks(exchange(heads_blocks, last), last).reshape(width, -1)

    ends = jnp.cumsum(image_lengths[:, 0], axis=1)
    places = narrow_at * own + jnp.arange(own, dtype=jnp.int32)
    passed = ends[:, :, None] <= places[None, None, :]
    first_key = jnp.max(jnp.where(passed, ends[:, :, None], 0), axis=1) - start
    last_key = jnp.min(jnp.where(passed, row_count, ends[:, :, None]), axis=1) - start
    bounds = jnp.tile(jnp.stack([first_key, last_key], axis=1), (1, 1, heads)).astype(jnp.int32)

    token_window = lax.dynamic_slice_in_dim(tokens, start, window, 1).astype(f32)
    window_normed = (norm_parts(token_window)[0] * first_gain + first_shift).astype(bf16)
    output_grad = lax.dynamic_slice_in_dim(cotangent, narrow_at * own, own, 1)
    output_grad = output_grad.reshape(rows, width).astype(f32)
    feed_grad = (feed_scale * output_grad).astype(bf16)
    token_rows = lax.dynamic_slice_in_dim(tokens, narrow_at * own, own, 1)
    token_rows = token_rows.reshape(rows, width).astype(f32)

    normed_t = window_normed.transpose(0, 2, 1)
    own_normed = (norm_parts(token_rows)[0] * first_gain + first_shift).astype(bf16)
    own_normed_t = own_normed.reshape(micro, own, width).transpose(0, 2, 1)
    feed_grad_t = feed_grad.T

    heads_near = swap(heads_own, "narrow", 1)
    heads_far = swap(heads_own, "narrow", 2)
    mixed, saved0 = attend(
        offset, window_normed, [heads_own], qv_biases[0], bounds, own, None
    )
    mixed, *feed_parts = tie(mixed, *feed_parts)
    feed_blocks = arrange_blocks(feed_parts, groups[-1])
    mixed, feed_blocks = tie(mixed, feed_blocks)
    feed_other = exchange(feed_blocks, last)[1]
    mixed, saved1 = attend(
        offset, window_normed, [heads_near], qv_biases[1], bounds, own, mixed
    )
    mixed, feed_other = tie(mixed, feed_other)
    feed_own = arrange_blocks([feed_blocks, feed_other], last).reshape(width, -1)
    mixed, feed_own, heads_far = tie(mixed, feed_own, heads_far)
    feed_near = swap(feed_own, "narrow", 1)
    feed_far = swap(feed_own, "narrow", 2)
    heads_cross = swap(heads_far, "narrow", 1)
    mixed, saved2 = attend(
        offset, window_normed, [heads_far], qv_biases[2], bounds, own, mixed
    )
    mixed, saved3 = attend(
        offset, window_normed, [heads_cross], qv_biases[3], bounds, own, mixed
    )
    branch = mixed.reshape(rows, width) + out_bias
    middle = token_rows + mixer_scale * branch
    second_unit, second_inverse = norm_parts(middle)
    second_normed = (second_unit * second_gain + second_shift).astype(bf16)

    second_normed_t = second_normed.T

    def feed_on(pieces, biases, before):
        return feed_part(
            second_normed, feed_grad, second_normed_t, feed_grad_t, pieces, biases, before
        )

    sums, (part1,), bias1 = feed_on([feed_near], up_biases[1:2], None)
    given = swap(part1, "narrow", 1)
    sums, (part0,), bias0 = feed_on([feed_own], up_biases[:1], sums)
    near = add_low(part0, given)
    near_cut = cut(near, "wide", last)
    feed, back, *near_cut = tie(*sums, *near_cut)
    near_sent = send_cut(near_cut, last)
    feed_far, near_keep = tie(feed_far, near_cut[0])
    feed_cross = swap(feed_far, "narrow", 1)
    sums, (part2, part3), bias23 = feed_on([feed_far, feed_cross], up_biases[2:], (feed, back))
    given = swap(part3, "narrow", 1)
    feed, second_normed_grad = sums
    up_bias_parts = bias0 + bias1 + bias23

    feed_branch = feed + down_bias
    layer_own = (middle + feed_scale * feed_branch).astype(bf16).reshape(micro, own, width)
    y_high, core_high = bit_of("narrow", 2), bit_of("narrow", 1)
    layer_far = swap(layer_own, "narrow", 2)
    layer_near = join(layer_own, swap(layer_own, "narrow", 1), core_high, 1)
    layer_far = join(layer_far, swap(layer_far, "narrow", 1), core_high, 1)
    layer_out = join(layer_near, layer_far, y_high, 1).reshape(micro, row_count, width)

    feed_scale_sum = jnp.sum(output_grad * feed_branch, axis=0)
    down_bias_sum = feed_scale * jnp.sum(output_grad, axis=0)
    second_gain_sum = jnp.sum(second_normed_grad * second_unit, axis=0)
    second_shift_sum = jnp.sum(second_normed_grad, axis=0)
    middle_grad = output_grad + norm_back(second_normed_grad, second_unit, second_inverse, second_gain)
    mixer_scale_sum = jnp.sum(middle_grad * branch, axis=0)
    out_bias_sum = mixer_scale * jnp.sum(middle_grad, axis=0)
    mixed_grad = (mixer_scale * middle_grad).astype(bf16).reshape(micro, own, width)

    mgt = mixed_grad.transpose(0, 2, 1)

    def back_on(pieces, saved, grad_in):
        return attend_back(
            offset, normed_t, own_normed_t, mixed_grad, mgt, pieces, saved, bounds, grad_in
        )

    near, far = add_low(near_keep, *near_sent), add_low(part2, given)
    far_cut = cut(far, "wide", last)
    mgt, near, *far_cut = tie(mgt, near, *far_cut)
    far_sent = send_cut(far_cut, last)
    window_grad, (heads3,), sums3 = back_on([heads_cross], saved3, None)
    given3 = swap(heads3, "narrow", 1)
    window_grad, *far_sent = tie(window_grad, *far_sent)
    far = add_low(far_cut[0], *far_sent)
    window_grad, far = tie(window_grad, far)
    far_given = swap(far, "narrow", 2)
    window_grad, (heads2,), sums2 = back_on([heads_far], saved2, window_grad)
    window_grad, far_given, given3 = tie(window_grad, far_given, given3)
    mine = add_low(near, far_given)
    for bits in groups[:-1]:
        parts = cut(mine, "wide", bits)
        mine = add_low(parts[0], *send_cut(parts, bits))
    mine_cut = cut(mine, "wide", groups[-1])
    heads_sum = add_low(heads2, given3)
    window_grad, heads_sum, *mine_cut = tie(window_grad, heads_sum, *mine_cut)
    mine_sent = send_cut(mine_cut, groups[-1])
    heads_given = swap(heads_sum, "narrow", 2)
    window_grad, (heads1,), sums1 = back_on([heads_near], saved1, window_grad)
    given1 = swap(heads1, "narrow", 1)
    window_grad, heads_given, *mine_sent = tie(window_grad, heads_given, *mine_sent)
    mine = add_low(mine_cut[0], *mine_sent)
    window_grad, mine = tie(window_grad, mine)
    mine_all = exchange(mine, groups[-1])
    window_grad, (heads0,), sums0 = back_on([heads_own], saved0, window_grad)
    window_grad, *mine_all = tie(window_grad, *mine_all)
    mine = arrange(mine_all, groups[-1], 0).reshape((-1,) + mine.shape[1:])
    for bits in reversed(groups[:-1]):
        mine = arrange(exchange(mine, bits), bits, 0).reshape((-1,) + mine.shape[1:])
    feed_total = spread_last(mine)
    heads_total = spread_last(
        spread_far(reduce_far(reduce_last(add_low(heads0, given1, heads_given))))
    )
    head_bias_parts = [
        jnp.concatenate([s[0, 2 * cols : 3 * cols], s[0, cols : 2 * cols]])
        for s in sums0 + sums1 + sums2 + sums3
    ]

    before = lax.dynamic_slice_in_dim(window_grad, jnp.maximum(off - halo, 0), halo, 1)
    after = lax.dynamic_slice_in_dim(
        window_grad, jnp.minimum(off + own, window - halo), halo, 1
    )
    from_left = shift(after.astype(bf16), "narrow", 1).astype(f32)
    from_right = shift(before.astype(bf16), "narrow", -1).astype(f32)
    first_normed_grad = lax.dynamic_slice_in_dim(window_grad, off, own, 1)
    first_normed_grad = (
        first_normed_grad
        + jnp.pad(from_left, ((0, 0), (0, own - halo), (0, 0)))
        + jnp.pad(from_right, ((0, 0), (own - halo, 0), (0, 0)))
    ).reshape(rows, width)

    first_unit, first_inverse = norm_parts(token_rows)
    first_gain_sum = jnp.sum(first_normed_grad * first_unit, axis=0)
    first_shift_sum = jnp.sum(first_normed_grad, axis=0)
    token_grad = (
        middle_grad + norm_back(first_normed_grad, first_unit, first_inverse, first_gain)
    ).astype(bf16).reshape(micro, own, width)

    sums = jnp.stack(
        [out_bias_sum, down_bias_sum, first_gain_sum, first_shift_sum, second_gain_sum,
         second_shift_sum, mixer_scale_sum, feed_scale_sum]
    )
    group_sums = jnp.stack(
        [jnp.concatenate([head_bias_parts[r], up_bias_parts[r][0]]) for r in range(narrow_size)]
    )
    group_sums = jnp.stack([group_sums[r ^ narrow_at] for r in range(narrow_size)])
    packed = jnp.concatenate([sums.reshape(-1), group_sums.reshape(-1)]).reshape(-1, 128)
    packed = reduce_everywhere(packed).reshape(-1)
    sums = packed[: 8 * width].reshape(8, width)
    group_sums = packed[8 * width :].reshape(narrow_size, -1)
    mine = lax.dynamic_slice_in_dim(group_sums, narrow_at, 1, 0)[0]

    heads_grad = jnp.stack(
        [heads_total[:, 2 * cols : 3 * cols], heads_total[:, :cols], heads_total[:, cols : 2 * cols]],
        axis=1,
    ).astype(f32)
    out_grad = heads_total[:, 3 * cols :].T.astype(f32)
    return (
        layer_out, token_grad, heads_grad, mine[: 2 * cols].reshape(2, cols), out_grad, sums[0],
        feed_total[:, :hidden].astype(f32), mine[2 * cols :],
        feed_total[:, hidden:].T.astype(f32), sums[1], sums[2],
        sums[3], sums[4], sums[5], sums[6], sums[7],
    )


def solution(mesh):
    return jax.shard_map(
        body,
        mesh=mesh,
        in_specs=(
            P(None, "wide", None),
            P(None, "wide", None),
            P("wide", None, "narrow"),
            P(None, "narrow"),
            P("narrow", "wide"),
            P(),
            P("wide", "narrow"),
            P("narrow"),
            P("narrow", "wide"),
            P(),
            P(),
            P(),
            P(),
            P(),
            P(),
            P(),
            P(None, "wide", None),
        ),
        out_specs=(
            P(None, "wide", None),
            P(None, ("wide", "narrow"), None),
            P(None, None, "narrow"),
            P(None, "narrow"),
            P("narrow", None),
            P(),
            P(None, "narrow"),
            P("narrow"),
            P("narrow", None),
            P(),
            P(),
            P(),
            P(),
            P(),
            P(),
            P(),
        ),
        check_vma=False,
    )
```

```python
import math
from functools import partial

import jax
import jax.numpy as jnp
from jax import lax
from jax.experimental import pallas as pl
from jax.experimental.pallas import tpu as pltpu
from jax.sharding import PartitionSpec as P

HEAD_DIM = 64
MOST = 196
epsilon = 1e-06
bf16 = jnp.bfloat16
f32 = jnp.float32
LOG2E = math.log2(math.e)
VMEM_LIMIT = 60 * 1024 * 1024


def round_up(value, step):
    return -(-value // step) * step


def nt(left, right):
    return lax.dot_general(left, right, (((1,), (1,)), ((), ())), preferred_element_type=f32)


def tn(left, right):
    return lax.dot_general(left, right, (((0,), (0,)), ((), ())), preferred_element_type=f32)


def nn(left, right):
    return jnp.dot(left, right, preferred_element_type=f32)


def params():
    return pltpu.CompilerParams(
        dimension_semantics=("arbitrary",), vmem_limit_bytes=VMEM_LIMIT
    )


def cost(flops, transcendentals, moved):
    return pl.CostEstimate(flops=1024, transcendentals=0, bytes_accessed=1024)


def full(shape):
    return pl.BlockSpec(shape, lambda *a: (0,) * len(shape))


def per_micro(shape):
    return pl.BlockSpec((1,) + shape, lambda m, *a: (m,) + (0,) * len(shape))


def stack_heads(rows, heads):
    lane = lax.broadcasted_iota(jnp.int32, rows.shape, 1) // HEAD_DIM
    zero = jnp.zeros_like(rows)
    return jnp.concatenate([jnp.where(lane == h, rows, zero) for h in range(heads)], axis=0)


def unstack_heads(stacked, heads):
    rows = stacked.shape[0] // heads
    lane = lax.broadcasted_iota(jnp.int32, (rows, stacked.shape[1]), 1) // HEAD_DIM
    out = stacked[:rows]
    for h in range(1, heads):
        out = jnp.where(lane == h, stacked[h * rows : (h + 1) * rows], out)
    return out


def attend_kernel(own, heads, count, first, off_ref, *refs):
    x_ref, b_ref, bnd_ref = refs[:3]
    w_refs = refs[3 : 3 + count]
    rest = refs[3 + count + (0 if first else 1) :]
    mixed_ref = rest[0]
    off = pl.multiple_of(off_ref[0], 16)
    win = x_ref.shape[1]
    cols = heads * HEAD_DIM
    xw = x_ref[0]
    xo = x_ref[0, pl.ds(off, own), :]
    place = lax.broadcasted_iota(jnp.int32, (win, heads * own), 0)
    keep = (place >= bnd_ref[0, 0:1]) & (place < bnd_ref[0, 1:2])
    mixed = None if first else refs[3 + count][0]
    for i in range(count):
        q_ref, k_ref, v_ref, o_ref, l_ref = rest[1 + 5 * i : 6 + 5 * i]
        w = w_refs[i]
        both = nn(xw, w[:, : 2 * cols])
        k = both[:, :cols].astype(bf16)
        v = (both[:, cols:] + b_ref[i, 1:2]).astype(bf16)
        q = (nn(xo, w[:, 2 * cols : 3 * cols]) + b_ref[i, 0:1]).astype(bf16)
        q_ref[0] = q
        k_ref[0] = k
        v_ref[0] = v
        qs = stack_heads(q, heads)
        scores = nt(k, qs) * (HEAD_DIM**-0.5 * LOG2E)
        scores = jnp.where(keep, scores, -1e30)
        top = jnp.max(scores, axis=0, keepdims=True)
        weights = jnp.exp2(scores - top)
        total = jnp.sum(weights, axis=0, keepdims=True)
        out = tn(v, weights.astype(bf16)) * (1.0 / total)
        out = unstack_heads(out.T, heads).astype(bf16)
        o_ref[0] = out
        l_ref[0] = top + jnp.log2(total)
        part = nt(out, w[:, 3 * cols :])
        mixed = part if mixed is None else mixed + part
    mixed_ref[0] = mixed


def attend(off, x_win, pieces, bias, bounds, own, mixed):
    micro, win, width = x_win.shape
    cols = pieces[0].shape[1] // 4
    heads = cols // HEAD_DIM
    stacked = heads * own
    count = len(pieces)
    first = mixed is None
    shapes = [jax.ShapeDtypeStruct((micro, own, width), f32)]
    specs = [per_micro((own, width))]
    for _ in pieces:
        for rows in (own, win, win, own):
            shapes.append(jax.ShapeDtypeStruct((micro, rows, cols), bf16))
            specs.append(per_micro((rows, cols)))
        shapes.append(jax.ShapeDtypeStruct((micro, 1, stacked), f32))
        specs.append(per_micro((1, stacked)))
    args = [x_win, bias, bounds] + list(pieces)
    in_specs = [per_micro((win, width)), full(bias.shape), per_micro((2, stacked))]
    in_specs += [full((width, 4 * cols))] * count
    if not first:
        args.append(mixed)
        in_specs.append(per_micro((own, width)))
    result = pl.pallas_call(
        partial(attend_kernel, own, heads, count, first),
        grid_spec=pltpu.PrefetchScalarGridSpec(
            num_scalar_prefetch=1, grid=(micro,), in_specs=in_specs, out_specs=specs
        ),
        out_shape=shapes,
        compiler_params=params(),
        cost_estimate=cost(
            count * micro * 2 * (win * width * cols * 3 + 8 * stacked * win * HEAD_DIM),
            count * micro * stacked * win,
            micro * win * width * 2 + count * 4 * width * cols * 2,
        ),
        name="attend",
    )(off, *args)
    return result[0], [tuple(result[1 + 5 * i : 6 + 5 * i]) for i in range(count)]


def attend_back_kernel(own, heads, count, first, halo, off_ref, *refs):
    x_ref, mg_ref, bnd_ref = refs[:3]
    w_refs = refs[3 : 3 + count]
    saved = refs[3 + count : 3 + 6 * count]
    at = 3 + 6 * count
    in_ref = None if first else refs[at]
    rest = refs[at + (0 if first else 1) :]
    dn_ref = rest[0]
    halo_refs = rest[1 + 2 * count : 1 + 2 * count + (2 if halo else 0)]
    acc_refs = rest[1 + 2 * count + len(halo_refs) :]
    off = pl.multiple_of(off_ref[0], 16)
    win = x_ref.shape[1]
    cols = heads * HEAD_DIM
    scale = HEAD_DIM**-0.5
    step = pl.program_id(0)
    mg = mg_ref[0]
    xt = x_ref[0].T
    xot = x_ref[0, pl.ds(off, own), :].T
    mgt = mg.T
    place = lax.broadcasted_iota(jnp.int32, (win, heads * own), 0)
    keep = (place >= bnd_ref[0, 0:1]) & (place < bnd_ref[0, 1:2])
    dn = None if first else in_ref[0]
    dn_own = None
    for i in range(count):
        w = w_refs[i]
        q_ref, k_ref, v_ref, o_ref, l_ref = saved[5 * i : 5 * i + 5]
        dw_ref, db_ref = rest[1 + 2 * i : 3 + 2 * i]
        acc_ref = acc_refs[i]
        k, v, o = k_ref[0], v_ref[0], o_ref[0]
        g = nn(mg, w[:, 3 * cols :]).astype(bf16)
        qs = stack_heads(q_ref[0], heads)
        gs = stack_heads(g, heads)
        both = gs.astype(f32) * jnp.concatenate([o.astype(f32)] * heads, axis=0)
        delta = lax.dot_general(
            jnp.ones((8, both.shape[1]), f32), both, (((1,), (1,)), ((), ())),
            precision=lax.Precision.HIGHEST, preferred_element_type=f32,
        )[0:1]
        scores = nt(k, qs) * (scale * LOG2E) - l_ref[0]
        weights = jnp.exp2(jnp.where(keep, scores, -1e30))
        slope = (weights * (nt(v, gs) - delta)).astype(bf16)
        low = weights.astype(bf16)
        dq = (unstack_heads(tn(k, slope).T, heads) * scale).astype(bf16)
        dkv = jnp.concatenate([nn(slope, qs) * scale, nn(low, gs)], axis=1).astype(bf16)
        part = nt(dkv, w[:, : 2 * cols])
        dn = part if dn is None else dn + part
        part = nt(dq, w[:, 2 * cols : 3 * cols])
        dn_own = part if dn_own is None else dn_own + part
        left = nn(xt, dkv)
        right = jnp.concatenate([nn(xot, dq), nn(mgt, o)], axis=1)
        sums = jnp.concatenate(
            [
                jnp.sum(dkv.astype(f32), axis=0, keepdims=True),
                jnp.sum(jnp.concatenate([dq, dq], axis=1).astype(f32), axis=0, keepdims=True),
            ],
            axis=1,
        )

        @pl.when(step == 0)
        def _():
            acc_ref[:, : 2 * cols] = left
            acc_ref[:, 2 * cols :] = right
            db_ref[...] = sums

        @pl.when(step > 0)
        def _():
            acc_ref[:, : 2 * cols] += left
            acc_ref[:, 2 * cols :] += right
            db_ref[...] += sums

        @pl.when(step == pl.num_programs(0) - 1)
        def _():
            dw_ref[...] = acc_ref[...].astype(bf16)

    dn_ref[0] = dn
    dn_ref[0, pl.ds(off, own), :] += dn_own
    if halo:
        before = pl.multiple_of(jnp.maximum(off - halo, 0), 16)
        after = pl.multiple_of(jnp.minimum(off + own, win - halo), 16)
        halo_refs[0][0] = dn_ref[0, pl.ds(before, halo), :].astype(bf16)
        halo_refs[1][0] = dn_ref[0, pl.ds(after, halo), :].astype(bf16)


def attend_back(off, x_win, mixed_grad, pieces, saved, bounds, grad_in, halo):
    micro, win, width = x_win.shape
    own = mixed_grad.shape[1]
    cols = pieces[0].shape[1] // 4
    heads = cols // HEAD_DIM
    stacked = heads * own
    count = len(pieces)
    first = grad_in is None
    args = [x_win, mixed_grad, bounds] + list(pieces)
    in_specs = [per_micro((win, width)), per_micro((own, width)), per_micro((2, stacked))]
    in_specs += [full((width, 4 * cols))] * count
    for one in saved:
        args += list(one)
        in_specs += [per_micro((rows, cols)) for rows in (own, win, win, own)]
        in_specs.append(per_micro((1, stacked)))
    if not first:
        args.append(grad_in)
        in_specs.append(per_micro((win, width)))
    shapes = [jax.ShapeDtypeStruct((micro, win, width), f32)]
    specs = [per_micro((win, width))]
    for _ in pieces:
        shapes += [
            jax.ShapeDtypeStruct((width, 4 * cols), bf16),
            jax.ShapeDtypeStruct((1, 4 * cols), f32),
        ]
        specs += [full((width, 4 * cols)), full((1, 4 * cols))]
    for _ in range(2 if halo else 0):
        shapes.append(jax.ShapeDtypeStruct((micro, halo, width), bf16))
        specs.append(per_micro((halo, width)))
    result = pl.pallas_call(
        partial(attend_back_kernel, own, heads, count, first, halo),
        grid_spec=pltpu.PrefetchScalarGridSpec(
            num_scalar_prefetch=1,
            grid=(micro,),
            in_specs=in_specs,
            out_specs=specs,
            scratch_shapes=[pltpu.VMEM((width, 4 * cols), f32)] * count,
        ),
        out_shape=shapes,
        compiler_params=params(),
        cost_estimate=cost(
            count * micro * (40 * stacked * win * HEAD_DIM + 12 * win * width * cols),
            count * micro * stacked * win,
            micro * (10 * win) * width + count * 4 * width * cols * 4,
        ),
        name="attend_back",
    )(off, *args)
    return result[0], result[1 : 1 + 2 * count : 2], result[2 : 2 + 2 * count : 2], result[1 + 2 * count :]


def feed_kernel(chunks, count, first, *refs):
    x_ref, g_ref = refs[:2]
    w_refs = refs[2 : 2 + count]
    b_refs = refs[2 + count : 2 + 2 * count]
    at = 2 + 2 * count
    if not first:
        fi_ref, ni_ref = refs[at : at + 2]
        at = at + 2
    f_ref, n_ref = refs[at : at + 2]
    outs = refs[at + 2 : at + 2 + 2 * count]
    act_ref, ug_ref, xt_ref, gt_ref = refs[at + 2 + 2 * count :]
    rows = x_ref.shape[0]
    step = rows // chunks
    xt_ref[...] = x_ref[...].T
    gt_ref[...] = g_ref[...].T
    for i in range(count):
        w_ref, b_ref = w_refs[i], b_refs[i]
        dw_ref, db_ref = outs[2 * i : 2 * i + 2]
        hidden = b_ref.shape[1]
        total = jnp.zeros((1, hidden), f32)
        for c in range(chunks):
            rows_at = pl.ds(c * step, step)
            upper = nn(x_ref[rows_at, :], w_ref[:, :hidden]) + b_ref[...]
            phi = 0.5 + 0.5 * lax.erf(upper * math.sqrt(0.5))
            active = (upper * phi).astype(bf16)
            bell = jnp.exp2(upper * upper * (-0.5 * LOG2E)) * (1.0 / math.sqrt(2.0 * math.pi))
            slope = phi + upper * bell
            grad = (nn(g_ref[rows_at, :], w_ref[:, hidden:]) * slope).astype(bf16)
            act_ref[rows_at, :] = active
            ug_ref[rows_at, :] = grad
            total = total + jnp.sum(grad.astype(f32), axis=0, keepdims=True)
            feed = nt(active, w_ref[:, hidden:])
            back = nt(grad, w_ref[:, :hidden])
            if i > 0:
                feed = feed + f_ref[rows_at, :]
                back = back + n_ref[rows_at, :]
            elif not first:
                feed = feed + fi_ref[rows_at, :]
                back = back + ni_ref[rows_at, :]
            f_ref[rows_at, :] = feed
            n_ref[rows_at, :] = back
        db_ref[...] = total
        dw_ref[:, :hidden] = nn(xt_ref[...], ug_ref[...]).astype(bf16)
        dw_ref[:, hidden:] = nn(gt_ref[...], act_ref[...]).astype(bf16)


def feed_part(x2, grad, pieces, biases, before):
    rows, width = x2.shape
    hidden = biases[0].shape[1]
    count = len(pieces)
    first = before is None
    args = [x2, grad] + list(pieces) + list(biases)
    aliases = {}
    if not first:
        aliases = {len(args): 0, len(args) + 1: 1}
        args += list(before)
    whole = pl.BlockSpec(memory_space=pltpu.VMEM)
    shapes = [jax.ShapeDtypeStruct((rows, width), f32)] * 2
    for _ in pieces:
        shapes += [
            jax.ShapeDtypeStruct((width, 2 * hidden), bf16),
            jax.ShapeDtypeStruct((1, hidden), f32),
        ]
    result = pl.pallas_call(
        partial(feed_kernel, 4, count, first),
        in_specs=[whole] * len(args),
        out_specs=[whole] * len(shapes),
        out_shape=shapes,
        scratch_shapes=[
            pltpu.VMEM((rows, hidden), bf16),
            pltpu.VMEM((rows, hidden), bf16),
            pltpu.VMEM((width, rows), bf16),
            pltpu.VMEM((width, rows), bf16),
        ],
        input_output_aliases=aliases,
        compiler_params=pltpu.CompilerParams(vmem_limit_bytes=VMEM_LIMIT),
        cost_estimate=cost(
            count * 12 * rows * width * hidden,
            count * 2 * rows * hidden,
            16 * rows * width + count * 8 * width * hidden,
        ),
        name="feed_part",
    )(*args)
    return tuple(result[:2]), list(result[2::2]), list(result[3::2])


def norm_parts(values_in):
    center = jnp.mean(values_in, axis=-1, keepdims=True)
    shifted = values_in - center
    inverse = lax.rsqrt(jnp.mean(shifted * shifted, axis=-1, keepdims=True) + epsilon)
    return (shifted * inverse, inverse)


def norm_back(grad_in, unit_rows, inverse, gain_row):
    scaled = grad_in * gain_row
    return inverse * (
        scaled
        - jnp.mean(scaled, axis=-1, keepdims=True)
        - unit_rows * jnp.mean(scaled * unit_rows, axis=-1, keepdims=True)
    )


VECTORS = (
    "out_bias", "down_bias", "first_gain", "first_shift", "second_gain", "second_shift",
    "mixer_scale", "feed_scale",
)


def row(vec_ref, name):
    at = VECTORS.index(name)
    return vec_ref[at : at + 1]


def own_rows(shape):
    return pl.BlockSpec((1,) + shape, lambda m, place: (m, place[0]) + (0,) * (len(shape) - 1))


def rows_call(kernel, name, place, args, specs, shapes, out_specs):
    micro = args[0].shape[0]
    return pl.pallas_call(
        kernel,
        grid_spec=pltpu.PrefetchScalarGridSpec(
            num_scalar_prefetch=1, grid=(micro,), in_specs=specs, out_specs=out_specs
        ),
        out_shape=shapes,
        compiler_params=params(),
        cost_estimate=cost(0, 0, 0),
        name=name,
    )(place, *args)


def first_norm_kernel(place_ref, x_ref, c_ref, vec_ref, n_ref, g_ref):
    start = pl.multiple_of(place_ref[1], 16)
    win = n_ref.shape[1]
    unit = norm_parts(x_ref[0, pl.ds(start, win), :].astype(f32))[0]
    n_ref[0] = (unit * row(vec_ref, "first_gain") + row(vec_ref, "first_shift")).astype(bf16)
    g_ref[0] = (row(vec_ref, "feed_scale") * c_ref[0].astype(f32)).astype(bf16)


def second_norm_kernel(place_ref, mixed_ref, x_ref, vec_ref, m_ref, n_ref):
    branch = mixed_ref[0] + row(vec_ref, "out_bias")
    middle = x_ref[0].astype(f32) + row(vec_ref, "mixer_scale") * branch
    m_ref[0] = middle
    unit = norm_parts(middle)[0]
    n_ref[0] = (unit * row(vec_ref, "second_gain") + row(vec_ref, "second_shift")).astype(bf16)


def column_sums(sum_ref, rows_in):
    total = jnp.concatenate([jnp.sum(r, axis=0, keepdims=True) for r in rows_in], axis=0)

    @pl.when(pl.program_id(0) == 0)
    def _():
        sum_ref[...] = total

    @pl.when(pl.program_id(0) > 0)
    def _():
        sum_ref[...] += total


def second_back_kernel(
    place_ref, feed_ref, back_ref, m_ref, mixed_ref, c_ref, vec_ref, l_ref, mg_ref, low_ref, sum_ref
):
    middle, back, grad = m_ref[0], back_ref[0], c_ref[0].astype(f32)
    feed_scale = row(vec_ref, "feed_scale")
    branch = feed_ref[0] + row(vec_ref, "down_bias")
    l_ref[0] = (middle + feed_scale * branch).astype(bf16)
    unit, inverse = norm_parts(middle)
    middle_grad = grad + norm_back(back, unit, inverse, row(vec_ref, "second_gain"))
    mg_ref[0] = middle_grad
    low_ref[0] = (row(vec_ref, "mixer_scale") * middle_grad).astype(bf16)
    mixer = mixed_ref[0] + row(vec_ref, "out_bias")
    zero = jnp.zeros_like(grad[:8])
    column_sums(
        sum_ref,
        [middle_grad, grad, zero, zero, back * unit, back, middle_grad * mixer, grad * branch],
    )


def first_back_kernel(
    place_ref, win_ref, left_ref, right_ref, mg_ref, x_ref, vec_ref, t_ref, sum_ref
):
    own, halo = mg_ref.shape[1], left_ref.shape[1]
    off = pl.multiple_of(place_ref[2], 16)
    gap = jnp.zeros((own - halo, left_ref.shape[2]), f32)
    grad = win_ref[0, pl.ds(off, own), :]
    grad = grad + jnp.concatenate([left_ref[0].astype(f32), gap], axis=0)
    grad = grad + jnp.concatenate([gap, right_ref[0].astype(f32)], axis=0)
    unit, inverse = norm_parts(x_ref[0].astype(f32))
    t_ref[0] = (
        mg_ref[0] + norm_back(grad, unit, inverse, row(vec_ref, "first_gain"))
    ).astype(bf16)
    zero = jnp.zeros_like(grad[:8])
    column_sums(sum_ref, [zero, zero, grad * unit, grad, zero, zero, zero, zero])


def swap(values_in, axis, bit):
    size = lax.axis_size(axis)
    return lax.ppermute(values_in, axis, [(i, i ^ bit) for i in range(size)])


def shift(values_in, axis, step):
    size = lax.axis_size(axis)
    pairs = [(i, i + step) for i in range(size) if 0 <= i + step < size]
    return lax.ppermute(values_in, axis, pairs)


def wide_bits(size):
    bits = []
    bit = size // 2
    while bit:
        bits.append(bit)
        bit //= 2
    return bits


def bit_of(axis, bit):
    return (lax.axis_index(axis) & bit) != 0


def join(mine, other, is_high, axis):
    low = jnp.where(is_high, other, mine)
    high = jnp.where(is_high, mine, other)
    return jnp.stack([low, high], axis=axis)


def tie(*values_in):
    return lax.optimization_barrier(values_in)


def far_groups():
    bits = wide_bits(lax.axis_size("wide"))[:-1]
    return [bits[i : i + 2] for i in range(0, len(bits), 2)]


def offsets(bits):
    return [
        sum(bit for i, bit in enumerate(reversed(bits)) if (k >> i) & 1)
        for k in range(2 ** len(bits))
    ]


def exchange(values_in, bits):
    return [values_in] + [swap(values_in, "wide", o) for o in offsets(bits)[1:]]


def arrange(parts, bits, axis):
    if not bits:
        return jnp.expand_dims(parts[0], axis)
    half = len(parts) // 2
    low = arrange(parts[:half], bits[1:], axis)
    high = arrange(parts[half:], bits[1:], axis)
    is_high = bit_of("wide", bits[0])
    return jnp.concatenate(
        [jnp.where(is_high, high, low), jnp.where(is_high, low, high)], axis=axis
    )


def arrange_blocks(parts, bits):
    return arrange(parts, bits, 1).reshape((-1,) + parts[0].shape[1:])


def last_bit():
    return wide_bits(lax.axis_size("wide"))[-1]


def gather_narrow(piece):
    far = swap(piece, "narrow", 2)
    return [piece, swap(piece, "narrow", 1), far, swap(far, "narrow", 1)]


def add_low(*parts):
    total = parts[0].astype(f32)
    for part in parts[1:]:
        total = total + part.astype(f32)
    return total.astype(bf16)


def cut(values_in, axis, bits):
    count = 2 ** len(bits)
    size = values_in.shape[0] // count
    at = lax.axis_index(axis)
    places = []
    for o in offsets(bits):
        other = at ^ o
        place = 0
        for bit in bits:
            place = 2 * place + ((other & bit) != 0).astype(jnp.int32)
        places.append(place)
    return [lax.dynamic_slice_in_dim(values_in, p * size, size, 0) for p in places]


def send_cut(parts, bits):
    return [swap(part, "wide", o) for part, o in zip(parts[1:], offsets(bits)[1:])]


def reduce_far(part):
    for bits in far_groups():
        parts = cut(part, "wide", bits)
        part = add_low(parts[0], *send_cut(parts, bits))
    return part


def spread_far(part):
    for bits in reversed(far_groups()):
        part = arrange(exchange(part, bits), bits, 0).reshape((-1,) + part.shape[1:])
    return part


def reduce_last(part):
    parts = cut(part, "wide", [last_bit()])
    return add_low(parts[0], *send_cut(parts, [last_bit()]))


def spread_last(part):
    bits = [last_bit()]
    return arrange(exchange(part, bits), bits, 0).reshape((-1,) + part.shape[1:])


def reduce_everywhere(values_in):
    for bit in wide_bits(lax.axis_size("wide")):
        values_in = values_in + swap(values_in, "wide", bit)
    for bit in wide_bits(lax.axis_size("narrow")):
        values_in = values_in + swap(values_in, "narrow", bit)
    return values_in


def body(
    tokens, image_lengths, heads_weight, heads_bias, out_weight, out_bias, up_weight, up_bias,
    down_weight, down_bias, first_gain, first_shift, second_gain, second_shift, mixer_scale,
    feed_scale, cotangent,
):
    micro, row_count, width = tokens.shape
    narrow_size = lax.axis_size("narrow")
    narrow_at = lax.axis_index("narrow")
    own = row_count // narrow_size
    cols = heads_weight.shape[2]
    heads = cols // HEAD_DIM
    rows = micro * own
    halo = round_up(MOST - 1, 16)
    window = min(row_count, round_up(own + 2 * halo, 128))
    lead = round_up((window - own) // 2, 16)
    start = jnp.clip(narrow_at * own - lead, 0, row_count - window)
    off = narrow_at * own - start
    offset = off.reshape(1).astype(jnp.int32)

    hidden = up_weight.shape[1]
    groups = far_groups()

    bias_pieces = gather_narrow(
        jnp.concatenate([heads_bias.reshape(-1), up_bias]).reshape(1, -1)
    )
    qv_biases = [heads_bias[None]]
    qv_biases += [b[:, : 2 * cols].reshape(1, 2, cols) for b in bias_pieces[1:]]
    up_biases = [up_bias.reshape(1, hidden)] + [b[:, 2 * cols :] for b in bias_pieces[1:]]
    heads_blocks = jnp.concatenate(
        [heads_weight[:, 1], heads_weight[:, 2], heads_weight[:, 0], out_weight.T], axis=1
    )[None]
    for bits in groups:
        heads_blocks = arrange_blocks(exchange(heads_blocks, bits), bits)
    feed_blocks = jnp.concatenate([up_weight, down_weight.T], axis=1)[None]
    heads_blocks, feed_blocks = tie(heads_blocks, feed_blocks)
    for bits in groups[:-1]:
        feed_blocks = arrange_blocks(exchange(feed_blocks, bits), bits)
    feed_parts = exchange(feed_blocks, groups[-1])
    last = [last_bit()]
    heads_own = arrange_blocks(exchange(heads_blocks, last), last).reshape(width, -1)

    ends = jnp.cumsum(image_lengths[:, 0], axis=1)
    places = narrow_at * own + jnp.arange(own, dtype=jnp.int32)
    passed = ends[:, :, None] <= places[None, None, :]
    first_key = jnp.max(jnp.where(passed, ends[:, :, None], 0), axis=1) - start
    last_key = jnp.min(jnp.where(passed, row_count, ends[:, :, None]), axis=1) - start
    bounds = jnp.tile(jnp.stack([first_key, last_key], axis=1), (1, 1, heads)).astype(jnp.int32)

    place = jnp.stack([narrow_at, start, off]).astype(jnp.int32)
    vectors = jnp.stack(
        [out_bias, down_bias, first_gain, first_shift, second_gain, second_shift, mixer_scale,
         feed_scale]
    )
    own_spec, part_spec, vec_spec = own_rows((own, width)), per_micro((own, width)), full((8, width))
    low_rows = jax.ShapeDtypeStruct((micro, own, width), bf16)
    high_rows = jax.ShapeDtypeStruct((micro, own, width), f32)
    sum_rows = jax.ShapeDtypeStruct((8, width), f32)
    window_normed, feed_grad = rows_call(
        first_norm_kernel, "first_norm", place, [tokens, cotangent, vectors],
        [per_micro((row_count, width)), own_spec, vec_spec],
        [jax.ShapeDtypeStruct((micro, window, width), bf16), low_rows],
        [per_micro((window, width)), part_spec],
    )
    feed_grad = feed_grad.reshape(rows, width)

    heads_near = swap(heads_own, "narrow", 1)
    heads_far = swap(heads_own, "narrow", 2)
    mixed, saved0 = attend(
        offset, window_normed, [heads_own], qv_biases[0], bounds, own, None
    )
    mixed, *feed_parts = tie(mixed, *feed_parts)
    feed_blocks = arrange_blocks(feed_parts, groups[-1])
    mixed, feed_blocks = tie(mixed, feed_blocks)
    feed_other = exchange(feed_blocks, last)[1]
    mixed, saved1 = attend(
        offset, window_normed, [heads_near], qv_biases[1], bounds, own, mixed
    )
    mixed, feed_other = tie(mixed, feed_other)
    feed_own = arrange_blocks([feed_blocks, feed_other], last).reshape(width, -1)
    mixed, feed_own, heads_far = tie(mixed, feed_own, heads_far)
    feed_near = swap(feed_own, "narrow", 1)
    feed_far = swap(feed_own, "narrow", 2)
    heads_cross = swap(heads_far, "narrow", 1)
    mixed, saved2 = attend(
        offset, window_normed, [heads_far], qv_biases[2], bounds, own, mixed
    )
    mixed, saved3 = attend(
        offset, window_normed, [heads_cross], qv_biases[3], bounds, own, mixed
    )
    middle, second_normed = rows_call(
        second_norm_kernel, "second_norm", place, [mixed, tokens, vectors],
        [part_spec, own_spec, vec_spec], [high_rows, low_rows], [part_spec, part_spec],
    )
    second_normed = second_normed.reshape(rows, width)

    def feed_on(pieces, biases, before):
        return feed_part(second_normed, feed_grad, pieces, biases, before)

    sums, (part1,), bias1 = feed_on([feed_near], up_biases[1:2], None)
    given = swap(part1, "narrow", 1)
    sums, (part0,), bias0 = feed_on([feed_own], up_biases[:1], sums)
    near = add_low(part0, given)
    near_cut = cut(near, "wide", last)
    feed, back, *near_cut = tie(*sums, *near_cut)
    near_sent = send_cut(near_cut, last)
    near_keep = near_cut[0]
    feed, feed_far = tie(feed, feed_far)
    feed_cross = swap(feed_far, "narrow", 1)
    sums, (part2,), bias2 = feed_on([feed_far], up_biases[2:3], (feed, back))
    sums, (part3,), bias3 = feed_on([feed_cross], up_biases[3:], sums)
    given = swap(part3, "narrow", 1)
    feed, second_normed_grad = sums
    up_bias_parts = bias0 + bias1 + bias2 + bias3

    layer_own, middle_grad, mixed_grad, back_sums = rows_call(
        second_back_kernel, "second_back", place,
        [feed.reshape(micro, own, width), second_normed_grad.reshape(micro, own, width), middle,
         mixed, cotangent, vectors],
        [part_spec, part_spec, part_spec, part_spec, own_spec, vec_spec],
        [low_rows, high_rows, low_rows, sum_rows],
        [part_spec, part_spec, part_spec, vec_spec],
    )
    y_high, core_high = bit_of("narrow", 2), bit_of("narrow", 1)
    layer_far = swap(layer_own, "narrow", 2)
    layer_near = join(layer_own, swap(layer_own, "narrow", 1), core_high, 1)
    layer_far = join(layer_far, swap(layer_far, "narrow", 1), core_high, 1)
    layer_out = join(layer_near, layer_far, y_high, 1).reshape(micro, row_count, width)

    def back_on(pieces, saved, grad_in, halo):
        return attend_back(
            offset, window_normed, mixed_grad, pieces, saved, bounds, grad_in, halo
        )

    near, far = add_low(near_keep, *near_sent), add_low(part2, given)
    far_cut = cut(far, "wide", last)
    mixed_grad, near, *far_cut = tie(mixed_grad, near, *far_cut)
    far_sent = send_cut(far_cut, last)
    window_grad, (heads3,), sums3, _ = back_on([heads_cross], saved3, None, 0)
    given3 = swap(heads3, "narrow", 1)
    window_grad, *far_sent = tie(window_grad, *far_sent)
    far = add_low(far_cut[0], *far_sent)
    window_grad, far = tie(window_grad, far)
    far_given = swap(far, "narrow", 2)
    window_grad, (heads2,), sums2, _ = back_on([heads_far], saved2, window_grad, 0)
    window_grad, far_given, given3 = tie(window_grad, far_given, given3)
    mine = add_low(near, far_given)
    for bits in groups[:-1]:
        parts = cut(mine, "wide", bits)
        mine = add_low(parts[0], *send_cut(parts, bits))
    mine_cut = cut(mine, "wide", groups[-1])
    heads_sum = add_low(heads2, given3)
    window_grad, heads_sum, *mine_cut = tie(window_grad, heads_sum, *mine_cut)
    mine_sent = send_cut(mine_cut, groups[-1])
    heads_given = swap(heads_sum, "narrow", 2)
    window_grad, (heads1,), sums1, _ = back_on([heads_near], saved1, window_grad, 0)
    given1 = swap(heads1, "narrow", 1)
    window_grad, heads_given, *mine_sent = tie(window_grad, heads_given, *mine_sent)
    mine = add_low(mine_cut[0], *mine_sent)
    window_grad, mine = tie(window_grad, mine)
    mine_all = exchange(mine, groups[-1])
    window_grad, (heads0,), sums0, halos = back_on([heads_own], saved0, window_grad, halo)
    window_grad, *mine_all = tie(window_grad, *mine_all)
    mine = arrange(mine_all, groups[-1], 0).reshape((-1,) + mine.shape[1:])
    for bits in reversed(groups[:-1]):
        mine = arrange(exchange(mine, bits), bits, 0).reshape((-1,) + mine.shape[1:])
    feed_total = spread_last(mine)
    heads_total = spread_last(
        spread_far(reduce_far(reduce_last(add_low(heads0, given1, heads_given))))
    )
    head_bias_parts = [
        jnp.concatenate([s[0, 2 * cols : 3 * cols], s[0, cols : 2 * cols]])
        for s in [*sums0, *sums1, *sums2, *sums3]
    ]

    from_left = shift(halos[1], "narrow", 1)
    from_right = shift(halos[0], "narrow", -1)
    token_grad, first_sums = rows_call(
        first_back_kernel, "first_back", place,
        [window_grad, from_left, from_right, middle_grad, tokens, vectors],
        [per_micro((window, width)), per_micro((halo, width)), per_micro((halo, width)), part_spec,
         own_spec, vec_spec],
        [low_rows, sum_rows], [part_spec, vec_spec],
    )
    outer = jnp.stack([mixer_scale, feed_scale] + [jnp.ones_like(out_bias)] * 6)
    sums = (back_sums + first_sums) * outer
    group_sums = jnp.stack(
        [jnp.concatenate([head_bias_parts[r], up_bias_parts[r][0]]) for r in range(narrow_size)]
    )
    group_sums = jnp.stack([group_sums[r ^ narrow_at] for r in range(narrow_size)])
    packed = jnp.concatenate([sums.reshape(-1), group_sums.reshape(-1)]).reshape(-1, 128)
    packed = reduce_everywhere(packed).reshape(-1)
    sums = packed[: 8 * width].reshape(8, width)
    group_sums = packed[8 * width :].reshape(narrow_size, -1)
    mine = lax.dynamic_slice_in_dim(group_sums, narrow_at, 1, 0)[0]

    heads_grad = jnp.stack(
        [heads_total[:, 2 * cols : 3 * cols], heads_total[:, :cols], heads_total[:, cols : 2 * cols]],
        axis=1,
    ).astype(f32)
    out_grad = heads_total[:, 3 * cols :].T.astype(f32)
    return (
        layer_out, token_grad, heads_grad, mine[: 2 * cols].reshape(2, cols), out_grad, sums[0],
        feed_total[:, :hidden].astype(f32), mine[2 * cols :],
        feed_total[:, hidden:].T.astype(f32), sums[1], sums[2],
        sums[3], sums[4], sums[5], sums[6], sums[7],
    )


def solution(mesh):
    return jax.shard_map(
        body,
        mesh=mesh,
        in_specs=(
            P(None, "wide", None),
            P(None, "wide", None),
            P("wide", None, "narrow"),
            P(None, "narrow"),
            P("narrow", "wide"),
            P(),
            P("wide", "narrow"),
            P("narrow"),
            P("narrow", "wide"),
            P(),
            P(),
            P(),
            P(),
            P(),
            P(),
            P(),
            P(None, "wide", None),
        ),
        out_specs=(
            P(None, "wide", None),
            P(None, ("wide", "narrow"), None),
            P(None, None, "narrow"),
            P(None, "narrow"),
            P("narrow", None),
            P(),
            P(None, "narrow"),
            P("narrow"),
            P("narrow", None),
            P(),
            P(),
            P(),
            P(),
            P(),
            P(),
            P(),
        ),
        check_vma=False,
    )
```

```python
import math
from functools import partial

import jax
import jax.numpy as jnp
from jax import lax
from jax.experimental import pallas as pl
from jax.experimental.pallas import tpu as pltpu
from jax.sharding import PartitionSpec as P

HEAD_DIM = 64
MOST = 196
epsilon = 1e-06
bf16 = jnp.bfloat16
f32 = jnp.float32
LOG2E = math.log2(math.e)
VMEM_LIMIT = 60 * 1024 * 1024


def round_up(value, step):
    return -(-value // step) * step


def nt(left, right):
    return lax.dot_general(left, right, (((1,), (1,)), ((), ())), preferred_element_type=f32)


def tn(left, right):
    return lax.dot_general(left, right, (((0,), (0,)), ((), ())), preferred_element_type=f32)


def nn(left, right):
    return jnp.dot(left, right, preferred_element_type=f32)


def params():
    return pltpu.CompilerParams(
        dimension_semantics=("arbitrary",), vmem_limit_bytes=VMEM_LIMIT
    )


def cost(flops, transcendentals, moved):
    return pl.CostEstimate(flops=1024, transcendentals=0, bytes_accessed=1024)


def full(shape):
    return pl.BlockSpec(shape, lambda *a: (0,) * len(shape))


def per_micro(shape):
    return pl.BlockSpec((1,) + shape, lambda m, *a: (m,) + (0,) * len(shape))


def stack_heads(rows, heads):
    lane = lax.broadcasted_iota(jnp.int32, rows.shape, 1) // HEAD_DIM
    zero = jnp.zeros_like(rows)
    return jnp.concatenate([jnp.where(lane == h, rows, zero) for h in range(heads)], axis=0)


def unstack_heads(stacked, heads):
    rows = stacked.shape[0] // heads
    lane = lax.broadcasted_iota(jnp.int32, (rows, stacked.shape[1]), 1) // HEAD_DIM
    out = stacked[:rows]
    for h in range(1, heads):
        out = jnp.where(lane == h, stacked[h * rows : (h + 1) * rows], out)
    return out


def attend_kernel(own, heads, count, first, off_ref, *refs):
    x_ref, b_ref, bnd_ref = refs[:3]
    w_refs = refs[3 : 3 + count]
    rest = refs[3 + count + (0 if first else 1) :]
    mixed_ref = rest[0]
    off = pl.multiple_of(off_ref[0], 16)
    win = x_ref.shape[1]
    cols = heads * HEAD_DIM
    xw = x_ref[0]
    xo = x_ref[0, pl.ds(off, own), :]
    place = lax.broadcasted_iota(jnp.int32, (win, heads * own), 0)
    keep = (place >= bnd_ref[0, 0:1]) & (place < bnd_ref[0, 1:2])
    mixed = None if first else refs[3 + count][0]
    for i in range(count):
        q_ref, k_ref, v_ref, o_ref, l_ref = rest[1 + 5 * i : 6 + 5 * i]
        w = w_refs[i]
        both = nn(xw, w[:, : 2 * cols])
        k = both[:, :cols].astype(bf16)
        v = (both[:, cols:] + b_ref[i, 1:2]).astype(bf16)
        q = (nn(xo, w[:, 2 * cols : 3 * cols]) + b_ref[i, 0:1]).astype(bf16)
        q_ref[0] = q
        k_ref[0] = k
        v_ref[0] = v
        qs = stack_heads(q, heads)
        scores = nt(k, qs) * (HEAD_DIM**-0.5 * LOG2E)
        scores = jnp.where(keep, scores, -1e30)
        top = jnp.max(scores, axis=0, keepdims=True)
        weights = jnp.exp2(scores - top)
        total = jnp.sum(weights, axis=0, keepdims=True)
        out = tn(v, weights.astype(bf16)) * (1.0 / total)
        out = unstack_heads(out.T, heads).astype(bf16)
        o_ref[0] = out
        l_ref[0] = top + jnp.log2(total)
        part = nt(out, w[:, 3 * cols :])
        mixed = part if mixed is None else mixed + part
    mixed_ref[0] = mixed


def attend(off, x_win, pieces, bias, bounds, own, mixed):
    micro, win, width = x_win.shape
    cols = pieces[0].shape[1] // 4
    heads = cols // HEAD_DIM
    stacked = heads * own
    count = len(pieces)
    first = mixed is None
    shapes = [jax.ShapeDtypeStruct((micro, own, width), f32)]
    specs = [per_micro((own, width))]
    for _ in pieces:
        for rows in (own, win, win, own):
            shapes.append(jax.ShapeDtypeStruct((micro, rows, cols), bf16))
            specs.append(per_micro((rows, cols)))
        shapes.append(jax.ShapeDtypeStruct((micro, 1, stacked), f32))
        specs.append(per_micro((1, stacked)))
    args = [x_win, bias, bounds] + list(pieces)
    in_specs = [per_micro((win, width)), full(bias.shape), per_micro((2, stacked))]
    in_specs += [full((width, 4 * cols))] * count
    if not first:
        args.append(mixed)
        in_specs.append(per_micro((own, width)))
    result = pl.pallas_call(
        partial(attend_kernel, own, heads, count, first),
        grid_spec=pltpu.PrefetchScalarGridSpec(
            num_scalar_prefetch=1, grid=(micro,), in_specs=in_specs, out_specs=specs
        ),
        out_shape=shapes,
        compiler_params=params(),
        cost_estimate=cost(
            count * micro * 2 * (win * width * cols * 3 + 8 * stacked * win * HEAD_DIM),
            count * micro * stacked * win,
            micro * win * width * 2 + count * 4 * width * cols * 2,
        ),
        name="attend",
    )(off, *args)
    return result[0], [tuple(result[1 + 5 * i : 6 + 5 * i]) for i in range(count)]


def attend_back_kernel(own, heads, count, first, halo, off_ref, *refs):
    x_ref, mg_ref, bnd_ref = refs[:3]
    w_refs = refs[3 : 3 + count]
    saved = refs[3 + count : 3 + 6 * count]
    at = 3 + 6 * count
    in_ref = None if first else refs[at]
    rest = refs[at + (0 if first else 1) :]
    dn_ref = rest[0]
    halo_refs = rest[1 + 2 * count : 1 + 2 * count + (2 if halo else 0)]
    acc_refs = rest[1 + 2 * count + len(halo_refs) :]
    off = pl.multiple_of(off_ref[0], 16)
    win = x_ref.shape[1]
    cols = heads * HEAD_DIM
    scale = HEAD_DIM**-0.5
    step = pl.program_id(0)
    mg = mg_ref[0]
    xt = x_ref[0].T
    xot = x_ref[0, pl.ds(off, own), :].T
    mgt = mg.T
    place = lax.broadcasted_iota(jnp.int32, (win, heads * own), 0)
    keep = (place >= bnd_ref[0, 0:1]) & (place < bnd_ref[0, 1:2])
    dn = None if first else in_ref[0]
    dn_own = None
    for i in range(count):
        w = w_refs[i]
        q_ref, k_ref, v_ref, o_ref, l_ref = saved[5 * i : 5 * i + 5]
        dw_ref, db_ref = rest[1 + 2 * i : 3 + 2 * i]
        acc_ref = acc_refs[i]
        k, v, o = k_ref[0], v_ref[0], o_ref[0]
        g = nn(mg, w[:, 3 * cols :]).astype(bf16)
        qs = stack_heads(q_ref[0], heads)
        gs = stack_heads(g, heads)
        both = gs.astype(f32) * jnp.concatenate([o.astype(f32)] * heads, axis=0)
        delta = lax.dot_general(
            jnp.ones((8, both.shape[1]), f32), both, (((1,), (1,)), ((), ())),
            precision=lax.Precision.HIGHEST, preferred_element_type=f32,
        )[0:1]
        scores = nt(k, qs) * (scale * LOG2E) - l_ref[0]
        weights = jnp.exp2(jnp.where(keep, scores, -1e30))
        slope = (weights * (nt(v, gs) - delta)).astype(bf16)
        low = weights.astype(bf16)
        dq = (unstack_heads(tn(k, slope).T, heads) * scale).astype(bf16)
        dkv = jnp.concatenate([nn(slope, qs) * scale, nn(low, gs)], axis=1).astype(bf16)
        part = nt(dkv, w[:, : 2 * cols])
        dn = part if dn is None else dn + part
        part = nt(dq, w[:, 2 * cols : 3 * cols])
        dn_own = part if dn_own is None else dn_own + part
        left = nn(xt, dkv)
        right = jnp.concatenate([nn(xot, dq), nn(mgt, o)], axis=1)
        sums = jnp.concatenate(
            [
                jnp.sum(dkv.astype(f32), axis=0, keepdims=True),
                jnp.sum(jnp.concatenate([dq, dq], axis=1).astype(f32), axis=0, keepdims=True),
            ],
            axis=1,
        )

        @pl.when(step == 0)
        def _():
            acc_ref[:, : 2 * cols] = left
            acc_ref[:, 2 * cols :] = right
            db_ref[...] = sums

        @pl.when(step > 0)
        def _():
            acc_ref[:, : 2 * cols] += left
            acc_ref[:, 2 * cols :] += right
            db_ref[...] += sums

        @pl.when(step == pl.num_programs(0) - 1)
        def _():
            dw_ref[...] = acc_ref[...].astype(bf16)

    dn_ref[0] = dn
    dn_ref[0, pl.ds(off, own), :] += dn_own
    if halo:
        before = pl.multiple_of(jnp.maximum(off - halo, 0), 16)
        after = pl.multiple_of(jnp.minimum(off + own, win - halo), 16)
        halo_refs[0][0] = dn_ref[0, pl.ds(before, halo), :].astype(bf16)
        halo_refs[1][0] = dn_ref[0, pl.ds(after, halo), :].astype(bf16)


def attend_back(off, x_win, mixed_grad, pieces, saved, bounds, grad_in, halo):
    micro, win, width = x_win.shape
    own = mixed_grad.shape[1]
    cols = pieces[0].shape[1] // 4
    heads = cols // HEAD_DIM
    stacked = heads * own
    count = len(pieces)
    first = grad_in is None
    args = [x_win, mixed_grad, bounds] + list(pieces)
    in_specs = [per_micro((win, width)), per_micro((own, width)), per_micro((2, stacked))]
    in_specs += [full((width, 4 * cols))] * count
    for one in saved:
        args += list(one)
        in_specs += [per_micro((rows, cols)) for rows in (own, win, win, own)]
        in_specs.append(per_micro((1, stacked)))
    if not first:
        args.append(grad_in)
        in_specs.append(per_micro((win, width)))
    shapes = [jax.ShapeDtypeStruct((micro, win, width), f32)]
    specs = [per_micro((win, width))]
    for _ in pieces:
        shapes += [
            jax.ShapeDtypeStruct((width, 4 * cols), bf16),
            jax.ShapeDtypeStruct((1, 4 * cols), f32),
        ]
        specs += [full((width, 4 * cols)), full((1, 4 * cols))]
    for _ in range(2 if halo else 0):
        shapes.append(jax.ShapeDtypeStruct((micro, halo, width), bf16))
        specs.append(per_micro((halo, width)))
    result = pl.pallas_call(
        partial(attend_back_kernel, own, heads, count, first, halo),
        grid_spec=pltpu.PrefetchScalarGridSpec(
            num_scalar_prefetch=1,
            grid=(micro,),
            in_specs=in_specs,
            out_specs=specs,
            scratch_shapes=[pltpu.VMEM((width, 4 * cols), f32)] * count,
        ),
        out_shape=shapes,
        compiler_params=params(),
        cost_estimate=cost(
            count * micro * (40 * stacked * win * HEAD_DIM + 12 * win * width * cols),
            count * micro * stacked * win,
            micro * (10 * win) * width + count * 4 * width * cols * 4,
        ),
        name="attend_back",
    )(off, *args)
    return result[0], result[1 : 1 + 2 * count : 2], result[2 : 2 + 2 * count : 2], result[1 + 2 * count :]


def feed_kernel(chunks, count, first, *refs):
    x_ref, g_ref = refs[:2]
    w_refs = refs[2 : 2 + count]
    b_refs = refs[2 + count : 2 + 2 * count]
    at = 2 + 2 * count
    if not first:
        fi_ref, ni_ref = refs[at : at + 2]
        at = at + 2
    f_ref, n_ref = refs[at : at + 2]
    outs = refs[at + 2 : at + 2 + 2 * count]
    act_ref, ug_ref, xt_ref, gt_ref = refs[at + 2 + 2 * count :]
    rows = x_ref.shape[0]
    step = rows // chunks
    xt_ref[...] = x_ref[...].T
    gt_ref[...] = g_ref[...].T
    for i in range(count):
        w_ref, b_ref = w_refs[i], b_refs[i]
        dw_ref, db_ref = outs[2 * i : 2 * i + 2]
        hidden = b_ref.shape[1]
        total = jnp.zeros((1, hidden), f32)
        for c in range(chunks):
            rows_at = pl.ds(c * step, step)
            upper = nn(x_ref[rows_at, :], w_ref[:, :hidden]) + b_ref[...]
            phi = 0.5 + 0.5 * lax.erf(upper * math.sqrt(0.5))
            active = (upper * phi).astype(bf16)
            bell = jnp.exp2(upper * upper * (-0.5 * LOG2E)) * (1.0 / math.sqrt(2.0 * math.pi))
            slope = phi + upper * bell
            grad = (nn(g_ref[rows_at, :], w_ref[:, hidden:]) * slope).astype(bf16)
            act_ref[rows_at, :] = active
            ug_ref[rows_at, :] = grad
            total = total + jnp.sum(grad.astype(f32), axis=0, keepdims=True)
            feed = nt(active, w_ref[:, hidden:])
            back = nt(grad, w_ref[:, :hidden])
            if i > 0:
                feed = feed + f_ref[rows_at, :]
                back = back + n_ref[rows_at, :]
            elif not first:
                feed = feed + fi_ref[rows_at, :]
                back = back + ni_ref[rows_at, :]
            f_ref[rows_at, :] = feed
            n_ref[rows_at, :] = back
        db_ref[...] = total
        dw_ref[:, :hidden] = nn(xt_ref[...], ug_ref[...]).astype(bf16)
        dw_ref[:, hidden:] = nn(gt_ref[...], act_ref[...]).astype(bf16)


def feed_part(x2, grad, pieces, biases, before):
    rows, width = x2.shape
    hidden = biases[0].shape[1]
    count = len(pieces)
    first = before is None
    args = [x2, grad] + list(pieces) + list(biases)
    aliases = {}
    if not first:
        aliases = {len(args): 0, len(args) + 1: 1}
        args += list(before)
    whole = pl.BlockSpec(memory_space=pltpu.VMEM)
    shapes = [jax.ShapeDtypeStruct((rows, width), f32)] * 2
    for _ in pieces:
        shapes += [
            jax.ShapeDtypeStruct((width, 2 * hidden), bf16),
            jax.ShapeDtypeStruct((1, hidden), f32),
        ]
    result = pl.pallas_call(
        partial(feed_kernel, 4, count, first),
        in_specs=[whole] * len(args),
        out_specs=[whole] * len(shapes),
        out_shape=shapes,
        scratch_shapes=[
            pltpu.VMEM((rows, hidden), bf16),
            pltpu.VMEM((rows, hidden), bf16),
            pltpu.VMEM((width, rows), bf16),
            pltpu.VMEM((width, rows), bf16),
        ],
        input_output_aliases=aliases,
        compiler_params=pltpu.CompilerParams(vmem_limit_bytes=VMEM_LIMIT),
        cost_estimate=cost(
            count * 12 * rows * width * hidden,
            count * 2 * rows * hidden,
            16 * rows * width + count * 8 * width * hidden,
        ),
        name="feed_part",
    )(*args)
    return tuple(result[:2]), list(result[2::2]), list(result[3::2])


def norm_parts(values_in):
    center = jnp.mean(values_in, axis=-1, keepdims=True)
    shifted = values_in - center
    inverse = lax.rsqrt(jnp.mean(shifted * shifted, axis=-1, keepdims=True) + epsilon)
    return (shifted * inverse, inverse)


def norm_back(grad_in, unit_rows, inverse, gain_row):
    scaled = grad_in * gain_row
    return inverse * (
        scaled
        - jnp.mean(scaled, axis=-1, keepdims=True)
        - unit_rows * jnp.mean(scaled * unit_rows, axis=-1, keepdims=True)
    )


VECTORS = (
    "out_bias", "down_bias", "first_gain", "first_shift", "second_gain", "second_shift",
    "mixer_scale", "feed_scale",
)


def row(vec_ref, name):
    at = VECTORS.index(name)
    return vec_ref[at : at + 1]


def own_rows(shape):
    return pl.BlockSpec((1,) + shape, lambda m, place: (m, place[0]) + (0,) * (len(shape) - 1))


def rows_call(kernel, name, place, args, specs, shapes, out_specs):
    micro = args[0].shape[0]
    return pl.pallas_call(
        kernel,
        grid_spec=pltpu.PrefetchScalarGridSpec(
            num_scalar_prefetch=1, grid=(micro,), in_specs=specs, out_specs=out_specs
        ),
        out_shape=shapes,
        compiler_params=params(),
        cost_estimate=cost(0, 0, 0),
        name=name,
    )(place, *args)


def first_norm_kernel(place_ref, x_ref, c_ref, vec_ref, n_ref, g_ref):
    start = pl.multiple_of(place_ref[1], 16)
    win = n_ref.shape[1]
    unit = norm_parts(x_ref[0, pl.ds(start, win), :].astype(f32))[0]
    n_ref[0] = (unit * row(vec_ref, "first_gain") + row(vec_ref, "first_shift")).astype(bf16)
    g_ref[0] = (row(vec_ref, "feed_scale") * c_ref[0].astype(f32)).astype(bf16)


def second_norm_kernel(place_ref, mixed_ref, x_ref, vec_ref, m_ref, n_ref):
    branch = mixed_ref[0] + row(vec_ref, "out_bias")
    middle = x_ref[0].astype(f32) + row(vec_ref, "mixer_scale") * branch
    m_ref[0] = middle
    unit = norm_parts(middle)[0]
    n_ref[0] = (unit * row(vec_ref, "second_gain") + row(vec_ref, "second_shift")).astype(bf16)


def column_sums(sum_ref, rows_in):
    total = jnp.concatenate([jnp.sum(r, axis=0, keepdims=True) for r in rows_in], axis=0)

    @pl.when(pl.program_id(0) == 0)
    def _():
        sum_ref[...] = total

    @pl.when(pl.program_id(0) > 0)
    def _():
        sum_ref[...] += total


def second_back_kernel(
    place_ref, feed_ref, back_ref, m_ref, mixed_ref, c_ref, vec_ref, l_ref, mg_ref, low_ref, sum_ref
):
    middle, back, grad = m_ref[0], back_ref[0], c_ref[0].astype(f32)
    feed_scale = row(vec_ref, "feed_scale")
    branch = feed_ref[0] + row(vec_ref, "down_bias")
    l_ref[0] = (middle + feed_scale * branch).astype(bf16)
    unit, inverse = norm_parts(middle)
    middle_grad = grad + norm_back(back, unit, inverse, row(vec_ref, "second_gain"))
    mg_ref[0] = middle_grad
    low_ref[0] = (row(vec_ref, "mixer_scale") * middle_grad).astype(bf16)
    mixer = mixed_ref[0] + row(vec_ref, "out_bias")
    zero = jnp.zeros_like(grad[:8])
    column_sums(
        sum_ref,
        [middle_grad, grad, zero, zero, back * unit, back, middle_grad * mixer, grad * branch],
    )


def first_back_kernel(
    place_ref, win_ref, left_ref, right_ref, mg_ref, x_ref, vec_ref, t_ref, sum_ref
):
    own, halo = mg_ref.shape[1], left_ref.shape[1]
    off = pl.multiple_of(place_ref[2], 16)
    gap = jnp.zeros((own - halo, left_ref.shape[2]), f32)
    grad = win_ref[0, pl.ds(off, own), :]
    grad = grad + jnp.concatenate([left_ref[0].astype(f32), gap], axis=0)
    grad = grad + jnp.concatenate([gap, right_ref[0].astype(f32)], axis=0)
    unit, inverse = norm_parts(x_ref[0].astype(f32))
    t_ref[0] = (
        mg_ref[0] + norm_back(grad, unit, inverse, row(vec_ref, "first_gain"))
    ).astype(bf16)
    zero = jnp.zeros_like(grad[:8])
    column_sums(sum_ref, [zero, zero, grad * unit, grad, zero, zero, zero, zero])


def swap(values_in, axis, bit):
    size = lax.axis_size(axis)
    return lax.ppermute(values_in, axis, [(i, i ^ bit) for i in range(size)])


def shift(values_in, axis, step):
    size = lax.axis_size(axis)
    pairs = [(i, i + step) for i in range(size) if 0 <= i + step < size]
    return lax.ppermute(values_in, axis, pairs)


def wide_bits(size):
    bits = []
    bit = size // 2
    while bit:
        bits.append(bit)
        bit //= 2
    return bits


def bit_of(axis, bit):
    return (lax.axis_index(axis) & bit) != 0


def join(mine, other, is_high, axis):
    low = jnp.where(is_high, other, mine)
    high = jnp.where(is_high, mine, other)
    return jnp.stack([low, high], axis=axis)


def tie(*values_in):
    return lax.optimization_barrier(values_in)


def far_groups():
    bits = wide_bits(lax.axis_size("wide"))[:-1]
    return [bits[i : i + 2] for i in range(0, len(bits), 2)]


def offsets(bits):
    return [
        sum(bit for i, bit in enumerate(reversed(bits)) if (k >> i) & 1)
        for k in range(2 ** len(bits))
    ]


def exchange(values_in, bits):
    return [values_in] + [swap(values_in, "wide", o) for o in offsets(bits)[1:]]


def arrange(parts, bits, axis):
    if not bits:
        return jnp.expand_dims(parts[0], axis)
    half = len(parts) // 2
    low = arrange(parts[:half], bits[1:], axis)
    high = arrange(parts[half:], bits[1:], axis)
    is_high = bit_of("wide", bits[0])
    return jnp.concatenate(
        [jnp.where(is_high, high, low), jnp.where(is_high, low, high)], axis=axis
    )


def arrange_blocks(parts, bits):
    return arrange(parts, bits, 1).reshape((-1,) + parts[0].shape[1:])


def last_bit():
    return wide_bits(lax.axis_size("wide"))[-1]


def gather_narrow(piece):
    far = swap(piece, "narrow", 2)
    return [piece, swap(piece, "narrow", 1), far, swap(far, "narrow", 1)]


def add_low(*parts):
    total = parts[0].astype(f32)
    for part in parts[1:]:
        total = total + part.astype(f32)
    return total.astype(bf16)


def cut(values_in, axis, bits):
    count = 2 ** len(bits)
    size = values_in.shape[0] // count
    at = lax.axis_index(axis)
    places = []
    for o in offsets(bits):
        other = at ^ o
        place = 0
        for bit in bits:
            place = 2 * place + ((other & bit) != 0).astype(jnp.int32)
        places.append(place)
    return [lax.dynamic_slice_in_dim(values_in, p * size, size, 0) for p in places]


def send_cut(parts, bits):
    return [swap(part, "wide", o) for part, o in zip(parts[1:], offsets(bits)[1:])]


def reduce_far(part):
    for bits in far_groups():
        parts = cut(part, "wide", bits)
        part = add_low(parts[0], *send_cut(parts, bits))
    return part


def spread_far(part):
    for bits in reversed(far_groups()):
        part = arrange(exchange(part, bits), bits, 0).reshape((-1,) + part.shape[1:])
    return part


def reduce_last(part):
    parts = cut(part, "wide", [last_bit()])
    return add_low(parts[0], *send_cut(parts, [last_bit()]))


def spread_last(part):
    bits = [last_bit()]
    return arrange(exchange(part, bits), bits, 0).reshape((-1,) + part.shape[1:])


def reduce_everywhere(values_in):
    for bit in wide_bits(lax.axis_size("wide")):
        values_in = values_in + swap(values_in, "wide", bit)
    for bit in wide_bits(lax.axis_size("narrow")):
        values_in = values_in + swap(values_in, "narrow", bit)
    return values_in


def body(
    tokens, image_lengths, heads_weight, heads_bias, out_weight, out_bias, up_weight, up_bias,
    down_weight, down_bias, first_gain, first_shift, second_gain, second_shift, mixer_scale,
    feed_scale, cotangent,
):
    micro, row_count, width = tokens.shape
    narrow_size = lax.axis_size("narrow")
    narrow_at = lax.axis_index("narrow")
    own = row_count // narrow_size
    cols = heads_weight.shape[2]
    heads = cols // HEAD_DIM
    rows = micro * own
    halo = round_up(MOST - 1, 16)
    window = min(row_count, round_up(own + 2 * halo, 128))
    lead = round_up((window - own) // 2, 16)
    start = jnp.clip(narrow_at * own - lead, 0, row_count - window)
    off = narrow_at * own - start
    offset = off.reshape(1).astype(jnp.int32)

    hidden = up_weight.shape[1]
    groups = far_groups()

    bias_pieces = gather_narrow(
        jnp.concatenate([heads_bias.reshape(-1), up_bias]).reshape(1, -1)
    )
    qv_biases = [heads_bias[None]]
    qv_biases += [b[:, : 2 * cols].reshape(1, 2, cols) for b in bias_pieces[1:]]
    up_biases = [up_bias.reshape(1, hidden)] + [b[:, 2 * cols :] for b in bias_pieces[1:]]
    heads_blocks = jnp.concatenate(
        [heads_weight[:, 1], heads_weight[:, 2], heads_weight[:, 0], out_weight.T], axis=1
    )[None]
    for bits in groups:
        heads_blocks = arrange_blocks(exchange(heads_blocks, bits), bits)
    feed_blocks = jnp.concatenate([up_weight, down_weight.T], axis=1)[None]
    heads_blocks, feed_blocks = tie(heads_blocks, feed_blocks)
    for bits in groups[:-1]:
        feed_blocks = arrange_blocks(exchange(feed_blocks, bits), bits)
    feed_parts = exchange(feed_blocks, groups[-1])
    last = [last_bit()]
    heads_all = arrange_blocks(exchange(heads_blocks, last), last)
    heads_own = heads_all.reshape(width, -1)

    ends = jnp.cumsum(image_lengths[:, 0], axis=1)
    places = narrow_at * own + jnp.arange(own, dtype=jnp.int32)
    passed = ends[:, :, None] <= places[None, None, :]
    first_key = jnp.max(jnp.where(passed, ends[:, :, None], 0), axis=1) - start
    last_key = jnp.min(jnp.where(passed, row_count, ends[:, :, None]), axis=1) - start
    bounds = jnp.tile(jnp.stack([first_key, last_key], axis=1), (1, 1, heads)).astype(jnp.int32)

    place = jnp.stack([narrow_at, start, off]).astype(jnp.int32)
    vectors = jnp.stack(
        [out_bias, down_bias, first_gain, first_shift, second_gain, second_shift, mixer_scale,
         feed_scale]
    )
    own_spec, part_spec, vec_spec = own_rows((own, width)), per_micro((own, width)), full((8, width))
    low_rows = jax.ShapeDtypeStruct((micro, own, width), bf16)
    high_rows = jax.ShapeDtypeStruct((micro, own, width), f32)
    sum_rows = jax.ShapeDtypeStruct((8, width), f32)
    window_normed, feed_grad = rows_call(
        first_norm_kernel, "first_norm", place, [tokens, cotangent, vectors],
        [per_micro((row_count, width)), own_spec, vec_spec],
        [jax.ShapeDtypeStruct((micro, window, width), bf16), low_rows],
        [per_micro((window, width)), part_spec],
    )
    feed_grad = feed_grad.reshape(rows, width)

    def halves(blocks):
        half = blocks.shape[0] // 2
        return blocks[:half], blocks[half:]

    def attend_on(piece, at, before):
        return attend(offset, window_normed, [piece], qv_biases[at], bounds, own, before)

    heads_low, heads_high = halves(heads_all)
    window_normed, heads_low = tie(window_normed, heads_low)
    heads_near = swap(heads_own, "narrow", 1)
    far_low = swap(heads_low, "narrow", 2)
    mixed, saved0 = attend_on(heads_own, 0, None)
    mixed, far_low, *feed_parts = tie(mixed, far_low, *feed_parts)
    feed_low, feed_high = halves(arrange_blocks(feed_parts, groups[-1]))
    mixed, feed_low, feed_high, heads_high = tie(mixed, feed_low, feed_high, heads_high)
    far_high = swap(heads_high, "narrow", 2)
    low_other = exchange(feed_low, last)[1]
    mixed, saved1 = attend_on(heads_near, 1, mixed)
    mixed, far_high, low_other = tie(mixed, far_high, low_other)
    heads_far = jnp.concatenate([far_low, far_high], axis=0).reshape(width, -1)
    mixed, heads_far, feed_low, feed_high = tie(mixed, heads_far, feed_low, feed_high)
    heads_cross = swap(heads_far, "narrow", 1)
    high_other = exchange(feed_high, last)[1]
    feed_far_low = swap(feed_low, "narrow", 2)
    mixed, saved2 = attend_on(heads_far, 2, mixed)
    mixed, high_other, feed_far_low = tie(mixed, high_other, feed_far_low)

    def whole_feed(low, high, low_sent, high_sent):
        mine = jnp.concatenate([low, high], axis=0)
        other = jnp.concatenate([low_sent, high_sent], axis=0)
        return arrange_blocks([mine, other], last).reshape(width, -1)

    feed_own = whole_feed(feed_low, feed_high, low_other, high_other)
    mixed, feed_own, feed_high = tie(mixed, feed_own, feed_high)
    feed_near = swap(feed_own, "narrow", 1)
    feed_far_high = swap(feed_high, "narrow", 2)
    mixed, saved3 = attend_on(heads_cross, 3, mixed)
    mixed, feed_far_high = tie(mixed, feed_far_high)
    middle, second_normed = rows_call(
        second_norm_kernel, "second_norm", place, [mixed, tokens, vectors],
        [part_spec, own_spec, vec_spec], [high_rows, low_rows], [part_spec, part_spec],
    )
    second_normed = second_normed.reshape(rows, width)

    def feed_on(pieces, biases, before):
        return feed_part(second_normed, feed_grad, pieces, biases, before)

    second_normed, feed_far_low = tie(second_normed, feed_far_low)
    far_low_other = exchange(feed_far_low, last)[1]
    sums, (part0,), bias0 = feed_on([feed_own], up_biases[:1], None)
    *sums, far_low_other, feed_far_high = tie(*sums, far_low_other, feed_far_high)
    far_high_other = exchange(feed_far_high, last)[1]
    sums, (part1,), bias1 = feed_on([feed_near], up_biases[1:2], sums)
    *sums, far_high_other = tie(*sums, far_high_other)
    feed_far = whole_feed(feed_far_low, feed_far_high, far_low_other, far_high_other)
    *sums, feed_far, part1 = tie(*sums, feed_far, part1)
    feed_cross = swap(feed_far, "narrow", 1)
    given = swap(part1, "narrow", 1)
    sums, (part2,), bias2 = feed_on([feed_far], up_biases[2:3], sums)
    *sums, given = tie(*sums, given)
    near_keep, near_give = cut(add_low(part0, given), "wide", last)
    up_give, down_give = near_give[:, :hidden], near_give[:, hidden:]
    *sums, near_keep, up_give, down_give = tie(*sums, near_keep, up_give, down_give)
    up_sent = swap(up_give, "wide", last[0])
    sums, (part3,), bias3 = feed_on([feed_cross], up_biases[3:], sums)
    feed, second_normed_grad, up_sent, part3, down_give = tie(*sums, up_sent, part3, down_give)
    down_sent = swap(down_give, "wide", last[0])
    given = swap(part3, "narrow", 1)
    up_bias_parts = bias0 + bias1 + bias2 + bias3

    layer_own, middle_grad, mixed_grad, back_sums = rows_call(
        second_back_kernel, "second_back", place,
        [feed.reshape(micro, own, width), second_normed_grad.reshape(micro, own, width), middle,
         mixed, cotangent, vectors],
        [part_spec, part_spec, part_spec, part_spec, own_spec, vec_spec],
        [low_rows, high_rows, low_rows, sum_rows],
        [part_spec, part_spec, part_spec, vec_spec],
    )
    y_high, core_high = bit_of("narrow", 2), bit_of("narrow", 1)
    layer_far = swap(layer_own, "narrow", 2)
    layer_near = join(layer_own, swap(layer_own, "narrow", 1), core_high, 1)
    layer_far = join(layer_far, swap(layer_far, "narrow", 1), core_high, 1)
    layer_out = join(layer_near, layer_far, y_high, 1).reshape(micro, row_count, width)

    def back_on(pieces, saved, grad_in, halo):
        return attend_back(
            offset, window_normed, mixed_grad, pieces, saved, bounds, grad_in, halo
        )

    mixed_grad, down_sent, given = tie(mixed_grad, down_sent, given)
    near = add_low(near_keep, jnp.concatenate([up_sent, down_sent], axis=1))
    far_cut = cut(add_low(part2, given), "wide", last)
    mixed_grad, near, *far_cut = tie(mixed_grad, near, *far_cut)
    far_sent = send_cut(far_cut, last)
    window_grad, (heads3,), sums3, _ = back_on([heads_cross], saved3, None, 0)
    given3 = swap(heads3, "narrow", 1)
    window_grad, *far_sent = tie(window_grad, *far_sent)
    far = add_low(far_cut[0], *far_sent)
    window_grad, far = tie(window_grad, far)
    far_given = swap(far, "narrow", 2)
    window_grad, (heads2,), sums2, _ = back_on([heads_far], saved2, window_grad, 0)
    window_grad, far_given, given3 = tie(window_grad, far_given, given3)
    mine = add_low(near, far_given)
    for bits in groups[:-1]:
        parts = cut(mine, "wide", bits)
        mine = add_low(parts[0], *send_cut(parts, bits))
    mine_cut = cut(mine, "wide", groups[-1])
    heads_sum = add_low(heads2, given3)
    window_grad, heads_sum, *mine_cut = tie(window_grad, heads_sum, *mine_cut)
    mine_sent = send_cut(mine_cut, groups[-1])
    heads_given = swap(heads_sum, "narrow", 2)
    window_grad, (heads1,), sums1, _ = back_on([heads_near], saved1, window_grad, 0)
    given1 = swap(heads1, "narrow", 1)
    window_grad, heads_given, *mine_sent = tie(window_grad, heads_given, *mine_sent)
    mine = add_low(mine_cut[0], *mine_sent)
    window_grad, mine = tie(window_grad, mine)
    mine_all = exchange(mine, groups[-1])
    window_grad, (heads0,), sums0, halos = back_on([heads_own], saved0, window_grad, halo)
    window_grad, *mine_all = tie(window_grad, *mine_all)
    mine = arrange(mine_all, groups[-1], 0).reshape((-1,) + mine.shape[1:])
    for bits in reversed(groups[:-1]):
        mine = arrange(exchange(mine, bits), bits, 0).reshape((-1,) + mine.shape[1:])
    feed_total = spread_last(mine)
    heads_total = spread_last(
        spread_far(reduce_far(reduce_last(add_low(heads0, given1, heads_given))))
    )
    head_bias_parts = [
        jnp.concatenate([s[0, 2 * cols : 3 * cols], s[0, cols : 2 * cols]])
        for s in [*sums0, *sums1, *sums2, *sums3]
    ]

    from_left = shift(halos[1], "narrow", 1)
    from_right = shift(halos[0], "narrow", -1)
    token_grad, first_sums = rows_call(
        first_back_kernel, "first_back", place,
        [window_grad, from_left, from_right, middle_grad, tokens, vectors],
        [per_micro((window, width)), per_micro((halo, width)), per_micro((halo, width)), part_spec,
         own_spec, vec_spec],
        [low_rows, sum_rows], [part_spec, vec_spec],
    )
    outer = jnp.stack([mixer_scale, feed_scale] + [jnp.ones_like(out_bias)] * 6)
    sums = (back_sums + first_sums) * outer
    group_sums = jnp.stack(
        [jnp.concatenate([head_bias_parts[r], up_bias_parts[r][0]]) for r in range(narrow_size)]
    )
    group_sums = jnp.stack([group_sums[r ^ narrow_at] for r in range(narrow_size)])
    packed = jnp.concatenate([sums.reshape(-1), group_sums.reshape(-1)]).reshape(-1, 128)
    packed = reduce_everywhere(packed).reshape(-1)
    sums = packed[: 8 * width].reshape(8, width)
    group_sums = packed[8 * width :].reshape(narrow_size, -1)
    mine = lax.dynamic_slice_in_dim(group_sums, narrow_at, 1, 0)[0]

    heads_grad = jnp.stack(
        [heads_total[:, 2 * cols : 3 * cols], heads_total[:, :cols], heads_total[:, cols : 2 * cols]],
        axis=1,
    ).astype(f32)
    out_grad = heads_total[:, 3 * cols :].T.astype(f32)
    return (
        layer_out, token_grad, heads_grad, mine[: 2 * cols].reshape(2, cols), out_grad, sums[0],
        feed_total[:, :hidden].astype(f32), mine[2 * cols :],
        feed_total[:, hidden:].T.astype(f32), sums[1], sums[2],
        sums[3], sums[4], sums[5], sums[6], sums[7],
    )


def solution(mesh):
    return jax.shard_map(
        body,
        mesh=mesh,
        in_specs=(
            P(None, "wide", None),
            P(None, "wide", None),
            P("wide", None, "narrow"),
            P(None, "narrow"),
            P("narrow", "wide"),
            P(),
            P("wide", "narrow"),
            P("narrow"),
            P("narrow", "wide"),
            P(),
            P(),
            P(),
            P(),
            P(),
            P(),
            P(),
            P(None, "wide", None),
        ),
        out_specs=(
            P(None, "wide", None),
            P(None, ("wide", "narrow"), None),
            P(None, None, "narrow"),
            P(None, "narrow"),
            P("narrow", None),
            P(),
            P(None, "narrow"),
            P("narrow"),
            P("narrow", None),
            P(),
            P(),
            P(),
            P(),
            P(),
            P(),
            P(),
        ),
        check_vma=False,
    )
```

```python
import math
from functools import partial

import jax
import jax.numpy as jnp
from jax import lax
from jax.experimental import pallas as pl
from jax.experimental.pallas import tpu as pltpu
from jax.sharding import PartitionSpec as P

HEAD_DIM = 64
MOST = 196
epsilon = 1e-06
bf16 = jnp.bfloat16
f32 = jnp.float32
LOG2E = math.log2(math.e)
VMEM_LIMIT = 60 * 1024 * 1024
FEED_CHUNKS = 2
QUERIES = 160


def round_up(value, step):
    return -(-value // step) * step


def nt(left, right):
    return lax.dot_general(left, right, (((1,), (1,)), ((), ())), preferred_element_type=f32)


def tn(left, right):
    return lax.dot_general(left, right, (((0,), (0,)), ((), ())), preferred_element_type=f32)


def nn(left, right):
    return jnp.dot(left, right, preferred_element_type=f32)


def query_chunk(own):
    return QUERIES if own % QUERIES == 0 else own


def key_span(own, win):
    return min(win, query_chunk(own) + 2 * round_up(MOST - 1, 16))


def key_start(off, at, own, win):
    first = jnp.clip(off + at - round_up(MOST - 1, 16), 0, win - key_span(own, win))
    return pl.multiple_of(first, 16)


def params():
    return pltpu.CompilerParams(
        dimension_semantics=("arbitrary",), vmem_limit_bytes=VMEM_LIMIT
    )


def cost(flops, transcendentals, moved):
    return pl.CostEstimate(flops=1024, transcendentals=0, bytes_accessed=1024)


def full(shape):
    return pl.BlockSpec(shape, lambda *a: (0,) * len(shape))


def per_micro(shape):
    return pl.BlockSpec((1,) + shape, lambda m, *a: (m,) + (0,) * len(shape))


def stack_heads(rows, heads):
    lane = lax.broadcasted_iota(jnp.int32, rows.shape, 1) // HEAD_DIM
    zero = jnp.zeros_like(rows)
    return jnp.concatenate([jnp.where(lane == h, rows, zero) for h in range(heads)], axis=0)


def unstack_heads(stacked, heads):
    rows = stacked.shape[0] // heads
    lane = lax.broadcasted_iota(jnp.int32, (rows, stacked.shape[1]), 1) // HEAD_DIM
    out = stacked[:rows]
    for h in range(1, heads):
        out = jnp.where(lane == h, stacked[h * rows : (h + 1) * rows], out)
    return out


def attend_kernel(own, heads, count, first, off_ref, *refs):
    x_ref, b_ref, bnd_ref = refs[:3]
    w_refs = refs[3 : 3 + count]
    rest = refs[3 + count + (0 if first else 1) :]
    mixed_ref = rest[0]
    off = pl.multiple_of(off_ref[0], 16)
    win = x_ref.shape[1]
    cols = heads * HEAD_DIM
    xw = x_ref[0]
    xo = x_ref[0, pl.ds(off, own), :]
    size, span = query_chunk(own), key_span(own, win)
    place = lax.broadcasted_iota(jnp.int32, (span, heads * size), 0)
    mixed = None if first else refs[3 + count][0]
    for i in range(count):
        q_ref, k_ref, v_ref, o_ref, l_ref = rest[1 + 5 * i : 6 + 5 * i]
        w = w_refs[i]
        both = nn(xw, w[:, : 2 * cols])
        k = both[:, :cols].astype(bf16)
        v = (both[:, cols:] + b_ref[i, 1:2]).astype(bf16)
        q = (nn(xo, w[:, 2 * cols : 3 * cols]) + b_ref[i, 0:1]).astype(bf16)
        q_ref[0] = q
        k_ref[0] = k
        v_ref[0] = v
        parts = []
        for c in range(own // size):
            key_at = key_start(off, c * size, own, win)
            kc, vc = k_ref[0, pl.ds(key_at, span), :], v_ref[0, pl.ds(key_at, span), :]
            qs = stack_heads(q[c * size : (c + 1) * size], heads)
            keep = (place >= bnd_ref[0, c, 0:1] - key_at) & (place < bnd_ref[0, c, 1:2] - key_at)
            scores = nt(kc, qs) * (HEAD_DIM**-0.5 * LOG2E)
            scores = jnp.where(keep, scores, -1e30)
            top = jnp.max(scores, axis=0, keepdims=True)
            weights = jnp.exp2(scores - top)
            total = jnp.sum(weights, axis=0, keepdims=True)
            out = tn(vc, weights.astype(bf16)) * (1.0 / total)
            parts.append(unstack_heads(out.T, heads).astype(bf16))
            l_ref[0, c] = top + jnp.log2(total)
        out = jnp.concatenate(parts, axis=0)
        o_ref[0] = out
        part = nt(out, w[:, 3 * cols :])
        mixed = part if mixed is None else mixed + part
    mixed_ref[0] = mixed


def attend(off, x_win, pieces, bias, bounds, own, mixed):
    micro, win, width = x_win.shape
    cols = pieces[0].shape[1] // 4
    heads = cols // HEAD_DIM
    size = query_chunk(own)
    stacked = heads * size
    count = len(pieces)
    first = mixed is None
    shapes = [jax.ShapeDtypeStruct((micro, own, width), f32)]
    specs = [per_micro((own, width))]
    for _ in pieces:
        for rows in (own, win, win, own):
            shapes.append(jax.ShapeDtypeStruct((micro, rows, cols), bf16))
            specs.append(per_micro((rows, cols)))
        shapes.append(jax.ShapeDtypeStruct((micro, own // size, 1, stacked), f32))
        specs.append(per_micro((own // size, 1, stacked)))
    args = [x_win, bias, bounds] + list(pieces)
    in_specs = [per_micro((win, width)), full(bias.shape), per_micro((own // size, 2, stacked))]
    in_specs += [full((width, 4 * cols))] * count
    if not first:
        args.append(mixed)
        in_specs.append(per_micro((own, width)))
    result = pl.pallas_call(
        partial(attend_kernel, own, heads, count, first),
        grid_spec=pltpu.PrefetchScalarGridSpec(
            num_scalar_prefetch=1, grid=(micro,), in_specs=in_specs, out_specs=specs
        ),
        out_shape=shapes,
        compiler_params=params(),
        cost_estimate=cost(
            count * micro * 2 * (win * width * cols * 3 + 8 * stacked * win * HEAD_DIM),
            count * micro * stacked * win,
            micro * win * width * 2 + count * 4 * width * cols * 2,
        ),
        name="attend",
    )(off, *args)
    return result[0], [tuple(result[1 + 5 * i : 6 + 5 * i]) for i in range(count)]


def attend_back_kernel(own, heads, count, first, halo, off_ref, *refs):
    x_ref, mg_ref, bnd_ref = refs[:3]
    w_refs = refs[3 : 3 + count]
    saved = refs[3 + count : 3 + 6 * count]
    at = 3 + 6 * count
    in_ref = None if first else refs[at]
    rest = refs[at + (0 if first else 1) :]
    dn_ref = rest[0]
    halo_refs = rest[1 + 2 * count : 1 + 2 * count + (2 if halo else 0)]
    *acc_refs, dkv_ref = rest[1 + 2 * count + len(halo_refs) :]
    off = pl.multiple_of(off_ref[0], 16)
    win = x_ref.shape[1]
    cols = heads * HEAD_DIM
    scale = HEAD_DIM**-0.5
    step = pl.program_id(0)
    mg = mg_ref[0]
    xt = x_ref[0].T
    xot = x_ref[0, pl.ds(off, own), :].T
    mgt = mg.T
    size, span = query_chunk(own), key_span(own, win)
    place = lax.broadcasted_iota(jnp.int32, (span, heads * size), 0)
    dn = None if first else in_ref[0]
    dn_own = None
    for i in range(count):
        w = w_refs[i]
        q_ref, k_ref, v_ref, o_ref, l_ref = saved[5 * i : 5 * i + 5]
        dw_ref, db_ref = rest[1 + 2 * i : 3 + 2 * i]
        acc_ref = acc_refs[i]
        o = o_ref[0]
        g = nn(mg, w[:, 3 * cols :]).astype(bf16)
        dkv_ref[...] = jnp.zeros_like(dkv_ref)
        parts = []
        for c in range(own // size):
            key_at = key_start(off, c * size, own, win)
            keys = pl.ds(key_at, span)
            kc, vc = k_ref[0, keys, :], v_ref[0, keys, :]
            qs = stack_heads(q_ref[0, c * size : (c + 1) * size, :], heads)
            gs = stack_heads(g[c * size : (c + 1) * size], heads)
            keep = (place >= bnd_ref[0, c, 0:1] - key_at) & (place < bnd_ref[0, c, 1:2] - key_at)
            scores = nt(kc, qs) * (scale * LOG2E) - l_ref[0, c]
            weights = jnp.exp2(jnp.where(keep, scores, -1e30))
            weighed = weights * nt(vc, gs)
            delta = jnp.sum(weighed, axis=0, keepdims=True)
            slope = (weighed - weights * delta).astype(bf16)
            parts.append((unstack_heads(tn(kc, slope).T, heads) * scale).astype(bf16))
            dkv_ref[0, keys, :] += nn(slope, qs)
            dkv_ref[1, keys, :] += nn(weights.astype(bf16), gs)
        dq = jnp.concatenate(parts, axis=0)
        dkv = jnp.concatenate([dkv_ref[0] * scale, dkv_ref[1]], axis=1).astype(bf16)
        part = nt(dkv, w[:, : 2 * cols])
        dn = part if dn is None else dn + part
        part = nt(dq, w[:, 2 * cols : 3 * cols])
        dn_own = part if dn_own is None else dn_own + part
        left = nn(xt, dkv)
        right = jnp.concatenate([nn(xot, dq), nn(mgt, o)], axis=1)
        sums = jnp.concatenate(
            [
                jnp.sum(dkv.astype(f32), axis=0, keepdims=True),
                jnp.sum(jnp.concatenate([dq, dq], axis=1).astype(f32), axis=0, keepdims=True),
            ],
            axis=1,
        )

        @pl.when(step == 0)
        def _():
            acc_ref[:, : 2 * cols] = left
            acc_ref[:, 2 * cols :] = right
            db_ref[...] = sums

        @pl.when(step > 0)
        def _():
            acc_ref[:, : 2 * cols] += left
            acc_ref[:, 2 * cols :] += right
            db_ref[...] += sums

        @pl.when(step == pl.num_programs(0) - 1)
        def _():
            dw_ref[...] = acc_ref[...].astype(bf16)

    dn_ref[0] = dn
    dn_ref[0, pl.ds(off, own), :] += dn_own
    if halo:
        before = pl.multiple_of(jnp.maximum(off - halo, 0), 16)
        after = pl.multiple_of(jnp.minimum(off + own, win - halo), 16)
        halo_refs[0][0] = dn_ref[0, pl.ds(before, halo), :].astype(bf16)
        halo_refs[1][0] = dn_ref[0, pl.ds(after, halo), :].astype(bf16)


def attend_back(off, x_win, mixed_grad, pieces, saved, bounds, grad_in, halo):
    micro, win, width = x_win.shape
    own = mixed_grad.shape[1]
    cols = pieces[0].shape[1] // 4
    heads = cols // HEAD_DIM
    size = query_chunk(own)
    stacked = heads * size
    count = len(pieces)
    first = grad_in is None
    args = [x_win, mixed_grad, bounds] + list(pieces)
    in_specs = [per_micro((win, width)), per_micro((own, width)), per_micro((own // size, 2, stacked))]
    in_specs += [full((width, 4 * cols))] * count
    for one in saved:
        args += list(one)
        in_specs += [per_micro((rows, cols)) for rows in (own, win, win, own)]
        in_specs.append(per_micro((own // size, 1, stacked)))
    if not first:
        args.append(grad_in)
        in_specs.append(per_micro((win, width)))
    shapes = [jax.ShapeDtypeStruct((micro, win, width), f32)]
    specs = [per_micro((win, width))]
    for _ in pieces:
        shapes += [
            jax.ShapeDtypeStruct((width, 4 * cols), bf16),
            jax.ShapeDtypeStruct((1, 4 * cols), f32),
        ]
        specs += [full((width, 4 * cols)), full((1, 4 * cols))]
    for _ in range(2 if halo else 0):
        shapes.append(jax.ShapeDtypeStruct((micro, halo, width), bf16))
        specs.append(per_micro((halo, width)))
    result = pl.pallas_call(
        partial(attend_back_kernel, own, heads, count, first, halo),
        grid_spec=pltpu.PrefetchScalarGridSpec(
            num_scalar_prefetch=1,
            grid=(micro,),
            in_specs=in_specs,
            out_specs=specs,
            scratch_shapes=[pltpu.VMEM((width, 4 * cols), f32)] * count
            + [pltpu.VMEM((2, win, cols), f32)],
        ),
        out_shape=shapes,
        compiler_params=params(),
        cost_estimate=cost(
            count * micro * (40 * stacked * win * HEAD_DIM + 12 * win * width * cols),
            count * micro * stacked * win,
            micro * (10 * win) * width + count * 4 * width * cols * 4,
        ),
        name="attend_back",
    )(off, *args)
    return result[0], result[1 : 1 + 2 * count : 2], result[2 : 2 + 2 * count : 2], result[1 + 2 * count :]


def feed_kernel(chunks, count, first, *refs):
    x_ref, g_ref = refs[:2]
    w_refs = refs[2 : 2 + count]
    b_refs = refs[2 + count : 2 + 2 * count]
    at = 2 + 2 * count
    if not first:
        fi_ref, ni_ref = refs[at : at + 2]
        at = at + 2
    f_ref, n_ref = refs[at : at + 2]
    outs = refs[at + 2 : at + 2 + 2 * count]
    act_ref, ug_ref, xt_ref, gt_ref = refs[at + 2 + 2 * count :]
    rows = x_ref.shape[0]
    step = rows // chunks
    xt_ref[...] = x_ref[...].T
    gt_ref[...] = g_ref[...].T
    for i in range(count):
        w_ref, b_ref = w_refs[i], b_refs[i]
        dw_ref, db_ref = outs[2 * i : 2 * i + 2]
        hidden = b_ref.shape[1]
        total = jnp.zeros((1, hidden), f32)
        for c in range(chunks):
            rows_at = pl.ds(c * step, step)
            upper = nn(x_ref[rows_at, :], w_ref[:, :hidden]) + b_ref[...]
            phi = 0.5 + 0.5 * lax.erf(upper * math.sqrt(0.5))
            active = (upper * phi).astype(bf16)
            bell = jnp.exp2(upper * upper * (-0.5 * LOG2E)) * (1.0 / math.sqrt(2.0 * math.pi))
            slope = phi + upper * bell
            grad = (nn(g_ref[rows_at, :], w_ref[:, hidden:]) * slope).astype(bf16)
            act_ref[rows_at, :] = active
            ug_ref[rows_at, :] = grad
            total = total + jnp.sum(grad.astype(f32), axis=0, keepdims=True)
            feed = nt(active, w_ref[:, hidden:])
            back = nt(grad, w_ref[:, :hidden])
            if i > 0:
                feed = feed + f_ref[rows_at, :]
                back = back + n_ref[rows_at, :]
            elif not first:
                feed = feed + fi_ref[rows_at, :]
                back = back + ni_ref[rows_at, :]
            f_ref[rows_at, :] = feed
            n_ref[rows_at, :] = back
        db_ref[...] = total
        dw_ref[:, :hidden] = nn(xt_ref[...], ug_ref[...]).astype(bf16)
        dw_ref[:, hidden:] = nn(gt_ref[...], act_ref[...]).astype(bf16)


def feed_part(x2, grad, pieces, biases, before):
    rows, width = x2.shape
    hidden = biases[0].shape[1]
    count = len(pieces)
    first = before is None
    args = [x2, grad] + list(pieces) + list(biases)
    aliases = {}
    if not first:
        aliases = {len(args): 0, len(args) + 1: 1}
        args += list(before)
    whole = pl.BlockSpec(memory_space=pltpu.VMEM)
    shapes = [jax.ShapeDtypeStruct((rows, width), f32)] * 2
    for _ in pieces:
        shapes += [
            jax.ShapeDtypeStruct((width, 2 * hidden), bf16),
            jax.ShapeDtypeStruct((1, hidden), f32),
        ]
    result = pl.pallas_call(
        partial(feed_kernel, FEED_CHUNKS, count, first),
        in_specs=[whole] * len(args),
        out_specs=[whole] * len(shapes),
        out_shape=shapes,
        scratch_shapes=[
            pltpu.VMEM((rows, hidden), bf16),
            pltpu.VMEM((rows, hidden), bf16),
            pltpu.VMEM((width, rows), bf16),
            pltpu.VMEM((width, rows), bf16),
        ],
        input_output_aliases=aliases,
        compiler_params=pltpu.CompilerParams(vmem_limit_bytes=VMEM_LIMIT),
        cost_estimate=cost(
            count * 12 * rows * width * hidden,
            count * 2 * rows * hidden,
            16 * rows * width + count * 8 * width * hidden,
        ),
        name="feed_part",
    )(*args)
    return tuple(result[:2]), list(result[2::2]), list(result[3::2])


def norm_parts(values_in):
    center = jnp.mean(values_in, axis=-1, keepdims=True)
    shifted = values_in - center
    inverse = lax.rsqrt(jnp.mean(shifted * shifted, axis=-1, keepdims=True) + epsilon)
    return (shifted * inverse, inverse)


def norm_back(grad_in, unit_rows, inverse, gain_row):
    scaled = grad_in * gain_row
    return inverse * (
        scaled
        - jnp.mean(scaled, axis=-1, keepdims=True)
        - unit_rows * jnp.mean(scaled * unit_rows, axis=-1, keepdims=True)
    )


VECTORS = (
    "out_bias", "down_bias", "first_gain", "first_shift", "second_gain", "second_shift",
    "mixer_scale", "feed_scale",
)


def row(vec_ref, name):
    at = VECTORS.index(name)
    return vec_ref[at : at + 1]


def own_rows(shape):
    return pl.BlockSpec((1,) + shape, lambda m, place: (m, place[0]) + (0,) * (len(shape) - 1))


def rows_call(kernel, name, place, args, specs, shapes, out_specs):
    micro = args[0].shape[0]
    return pl.pallas_call(
        kernel,
        grid_spec=pltpu.PrefetchScalarGridSpec(
            num_scalar_prefetch=1, grid=(micro,), in_specs=specs, out_specs=out_specs
        ),
        out_shape=shapes,
        compiler_params=params(),
        cost_estimate=cost(0, 0, 0),
        name=name,
    )(place, *args)


def first_norm_kernel(place_ref, x_ref, c_ref, vec_ref, n_ref, g_ref):
    start = pl.multiple_of(place_ref[1], 16)
    win = n_ref.shape[1]
    unit = norm_parts(x_ref[0, pl.ds(start, win), :].astype(f32))[0]
    n_ref[0] = (unit * row(vec_ref, "first_gain") + row(vec_ref, "first_shift")).astype(bf16)
    g_ref[0] = (row(vec_ref, "feed_scale") * c_ref[0].astype(f32)).astype(bf16)


def second_norm_kernel(place_ref, mixed_ref, x_ref, vec_ref, m_ref, n_ref):
    branch = mixed_ref[0] + row(vec_ref, "out_bias")
    middle = x_ref[0].astype(f32) + row(vec_ref, "mixer_scale") * branch
    m_ref[0] = middle
    unit = norm_parts(middle)[0]
    n_ref[0] = (unit * row(vec_ref, "second_gain") + row(vec_ref, "second_shift")).astype(bf16)


def column_sums(sum_ref, rows_in):
    total = jnp.concatenate([jnp.sum(r, axis=0, keepdims=True) for r in rows_in], axis=0)

    @pl.when(pl.program_id(0) == 0)
    def _():
        sum_ref[...] = total

    @pl.when(pl.program_id(0) > 0)
    def _():
        sum_ref[...] += total


def second_back_kernel(
    place_ref, feed_ref, back_ref, m_ref, mixed_ref, c_ref, vec_ref, l_ref, mg_ref, low_ref, sum_ref
):
    middle, back, grad = m_ref[0], back_ref[0], c_ref[0].astype(f32)
    feed_scale = row(vec_ref, "feed_scale")
    branch = feed_ref[0] + row(vec_ref, "down_bias")
    l_ref[0] = (middle + feed_scale * branch).astype(bf16)
    unit, inverse = norm_parts(middle)
    middle_grad = grad + norm_back(back, unit, inverse, row(vec_ref, "second_gain"))
    mg_ref[0] = middle_grad
    low_ref[0] = (row(vec_ref, "mixer_scale") * middle_grad).astype(bf16)
    mixer = mixed_ref[0] + row(vec_ref, "out_bias")
    zero = jnp.zeros_like(grad[:8])
    column_sums(
        sum_ref,
        [middle_grad, grad, zero, zero, back * unit, back, middle_grad * mixer, grad * branch],
    )


def first_back_kernel(
    place_ref, win_ref, left_ref, right_ref, mg_ref, x_ref, vec_ref, t_ref, sum_ref
):
    own, halo = mg_ref.shape[1], left_ref.shape[1]
    off = pl.multiple_of(place_ref[2], 16)
    gap = jnp.zeros((own - halo, left_ref.shape[2]), f32)
    grad = win_ref[0, pl.ds(off, own), :]
    grad = grad + jnp.concatenate([left_ref[0].astype(f32), gap], axis=0)
    grad = grad + jnp.concatenate([gap, right_ref[0].astype(f32)], axis=0)
    unit, inverse = norm_parts(x_ref[0].astype(f32))
    t_ref[0] = (
        mg_ref[0] + norm_back(grad, unit, inverse, row(vec_ref, "first_gain"))
    ).astype(bf16)
    zero = jnp.zeros_like(grad[:8])
    column_sums(sum_ref, [zero, zero, grad * unit, grad, zero, zero, zero, zero])


def swap(values_in, axis, bit):
    size = lax.axis_size(axis)
    return lax.ppermute(values_in, axis, [(i, i ^ bit) for i in range(size)])


def shift(values_in, axis, step):
    size = lax.axis_size(axis)
    pairs = [(i, i + step) for i in range(size) if 0 <= i + step < size]
    return lax.ppermute(values_in, axis, pairs)


def wide_bits(size):
    bits = []
    bit = size // 2
    while bit:
        bits.append(bit)
        bit //= 2
    return bits


def bit_of(axis, bit):
    return (lax.axis_index(axis) & bit) != 0


def join(mine, other, is_high, axis):
    low = jnp.where(is_high, other, mine)
    high = jnp.where(is_high, mine, other)
    return jnp.stack([low, high], axis=axis)


def tie(*values_in):
    return lax.optimization_barrier(values_in)


def far_groups():
    bits = wide_bits(lax.axis_size("wide"))[:-1]
    return [bits[i : i + 2] for i in range(0, len(bits), 2)]


def offsets(bits):
    return [
        sum(bit for i, bit in enumerate(reversed(bits)) if (k >> i) & 1)
        for k in range(2 ** len(bits))
    ]


def exchange(values_in, bits):
    return [values_in] + [swap(values_in, "wide", o) for o in offsets(bits)[1:]]


def arrange(parts, bits, axis):
    if not bits:
        return jnp.expand_dims(parts[0], axis)
    half = len(parts) // 2
    low = arrange(parts[:half], bits[1:], axis)
    high = arrange(parts[half:], bits[1:], axis)
    is_high = bit_of("wide", bits[0])
    return jnp.concatenate(
        [jnp.where(is_high, high, low), jnp.where(is_high, low, high)], axis=axis
    )


def arrange_blocks(parts, bits):
    return arrange(parts, bits, 1).reshape((-1,) + parts[0].shape[1:])


def last_bit():
    return wide_bits(lax.axis_size("wide"))[-1]


def gather_narrow(piece):
    far = swap(piece, "narrow", 2)
    return [piece, swap(piece, "narrow", 1), far, swap(far, "narrow", 1)]


def add_low(*parts):
    total = parts[0].astype(f32)
    for part in parts[1:]:
        total = total + part.astype(f32)
    return total.astype(bf16)


def cut(values_in, axis, bits):
    count = 2 ** len(bits)
    size = values_in.shape[0] // count
    at = lax.axis_index(axis)
    places = []
    for o in offsets(bits):
        other = at ^ o
        place = 0
        for bit in bits:
            place = 2 * place + ((other & bit) != 0).astype(jnp.int32)
        places.append(place)
    return [lax.dynamic_slice_in_dim(values_in, p * size, size, 0) for p in places]


def send_cut(parts, bits):
    return [swap(part, "wide", o) for part, o in zip(parts[1:], offsets(bits)[1:])]


def reduce_far(part):
    for bits in far_groups():
        parts = cut(part, "wide", bits)
        part = add_low(parts[0], *send_cut(parts, bits))
    return part


def spread_far(part):
    for bits in reversed(far_groups()):
        part = arrange(exchange(part, bits), bits, 0).reshape((-1,) + part.shape[1:])
    return part


def reduce_last(part):
    parts = cut(part, "wide", [last_bit()])
    return add_low(parts[0], *send_cut(parts, [last_bit()]))


def spread_last(part):
    bits = [last_bit()]
    return arrange(exchange(part, bits), bits, 0).reshape((-1,) + part.shape[1:])


def tree_sum(parts):
    while len(parts) > 1:
        parts = [parts[i] + parts[i + 1] for i in range(0, len(parts), 2)]
    return parts[0]


def reduce_everywhere(values_in):
    for bits in far_groups() + [[last_bit()]]:
        values_in = tree_sum(exchange(values_in, bits))
    return tree_sum([values_in] + [swap(values_in, "narrow", o) for o in (1, 2, 3)])


def body(
    tokens, image_lengths, heads_weight, heads_bias, out_weight, out_bias, up_weight, up_bias,
    down_weight, down_bias, first_gain, first_shift, second_gain, second_shift, mixer_scale,
    feed_scale, cotangent,
):
    micro, row_count, width = tokens.shape
    narrow_size = lax.axis_size("narrow")
    narrow_at = lax.axis_index("narrow")
    own = row_count // narrow_size
    cols = heads_weight.shape[2]
    heads = cols // HEAD_DIM
    rows = micro * own
    halo = round_up(MOST - 1, 16)
    window = min(row_count, round_up(own + 2 * halo, 128))
    lead = round_up((window - own) // 2, 16)
    start = jnp.clip(narrow_at * own - lead, 0, row_count - window)
    off = narrow_at * own - start
    offset = off.reshape(1).astype(jnp.int32)

    hidden = up_weight.shape[1]
    groups = far_groups()

    bias_pieces = gather_narrow(
        jnp.concatenate([heads_bias.reshape(-1), up_bias]).reshape(1, -1)
    )
    qv_biases = [heads_bias[None]]
    qv_biases += [b[:, : 2 * cols].reshape(1, 2, cols) for b in bias_pieces[1:]]
    up_biases = [up_bias.reshape(1, hidden)] + [b[:, 2 * cols :] for b in bias_pieces[1:]]
    heads_blocks = jnp.concatenate(
        [heads_weight[:, 1], heads_weight[:, 2], heads_weight[:, 0], out_weight.T], axis=1
    )[None]
    for bits in groups:
        heads_blocks = arrange_blocks(exchange(heads_blocks, bits), bits)
    feed_blocks = jnp.concatenate([up_weight, down_weight.T], axis=1)[None]
    heads_blocks, feed_blocks = tie(heads_blocks, feed_blocks)
    for bits in groups[:-1]:
        feed_blocks = arrange_blocks(exchange(feed_blocks, bits), bits)
    feed_parts = exchange(feed_blocks, groups[-1])
    last = [last_bit()]
    heads_all = arrange_blocks(exchange(heads_blocks, last), last)
    heads_own = heads_all.reshape(width, -1)

    ends = jnp.cumsum(image_lengths[:, 0], axis=1)
    places = narrow_at * own + jnp.arange(own, dtype=jnp.int32)
    passed = ends[:, :, None] <= places[None, None, :]
    first_key = jnp.max(jnp.where(passed, ends[:, :, None], 0), axis=1) - start
    last_key = jnp.min(jnp.where(passed, row_count, ends[:, :, None]), axis=1) - start
    bounds = jnp.stack([first_key, last_key], axis=1).astype(jnp.int32)
    size = query_chunk(own)
    bounds = bounds.reshape(micro, 2, own // size, size).transpose(0, 2, 1, 3)
    bounds = jnp.tile(bounds, (1, 1, 1, heads))

    place = jnp.stack([narrow_at, start, off]).astype(jnp.int32)
    vectors = jnp.stack(
        [out_bias, down_bias, first_gain, first_shift, second_gain, second_shift, mixer_scale,
         feed_scale]
    )
    own_spec, part_spec, vec_spec = own_rows((own, width)), per_micro((own, width)), full((8, width))
    low_rows = jax.ShapeDtypeStruct((micro, own, width), bf16)
    high_rows = jax.ShapeDtypeStruct((micro, own, width), f32)
    sum_rows = jax.ShapeDtypeStruct((8, width), f32)
    window_normed, feed_grad = rows_call(
        first_norm_kernel, "first_norm", place, [tokens, cotangent, vectors],
        [per_micro((row_count, width)), own_spec, vec_spec],
        [jax.ShapeDtypeStruct((micro, window, width), bf16), low_rows],
        [per_micro((window, width)), part_spec],
    )
    feed_grad = feed_grad.reshape(rows, width)

    def halves(blocks):
        half = blocks.shape[0] // 2
        return blocks[:half], blocks[half:]

    def attend_on(piece, at, before):
        return attend(offset, window_normed, [piece], qv_biases[at], bounds, own, before)

    heads_low, heads_high = halves(heads_all)
    window_normed, heads_low, *biases = tie(window_normed, heads_low, *qv_biases, *up_biases)
    qv_biases, up_biases = biases[:narrow_size], biases[narrow_size:]
    heads_near = swap(heads_own, "narrow", 1)
    far_low = swap(heads_low, "narrow", 2)
    mixed, saved0 = attend_on(heads_own, 0, None)
    mixed, far_low, *feed_parts = tie(mixed, far_low, *feed_parts)
    feed_low, feed_high = halves(arrange_blocks(feed_parts, groups[-1]))
    mixed, feed_low, feed_high, heads_high = tie(mixed, feed_low, feed_high, heads_high)
    far_high = swap(heads_high, "narrow", 2)
    low_other = exchange(feed_low, last)[1]
    mixed, saved1 = attend_on(heads_near, 1, mixed)
    mixed, far_high, low_other = tie(mixed, far_high, low_other)
    heads_far = jnp.concatenate([far_low, far_high], axis=0).reshape(width, -1)
    mixed, heads_far, feed_low, feed_high = tie(mixed, heads_far, feed_low, feed_high)
    heads_cross = swap(heads_far, "narrow", 1)
    high_other = exchange(feed_high, last)[1]
    feed_far_low = swap(feed_low, "narrow", 2)
    mixed, saved2 = attend_on(heads_far, 2, mixed)
    mixed, high_other, feed_far_low = tie(mixed, high_other, feed_far_low)

    def whole_feed(low, high, low_sent, high_sent):
        mine = jnp.concatenate([low, high], axis=0)
        other = jnp.concatenate([low_sent, high_sent], axis=0)
        return arrange_blocks([mine, other], last).reshape(width, -1)

    feed_own = whole_feed(feed_low, feed_high, low_other, high_other)
    mixed, feed_own, feed_high = tie(mixed, feed_own, feed_high)
    feed_near = swap(feed_own, "narrow", 1)
    feed_far_high = swap(feed_high, "narrow", 2)
    mixed, saved3 = attend_on(heads_cross, 3, mixed)
    mixed, feed_far_high = tie(mixed, feed_far_high)
    middle, second_normed = rows_call(
        second_norm_kernel, "second_norm", place, [mixed, tokens, vectors],
        [part_spec, own_spec, vec_spec], [high_rows, low_rows], [part_spec, part_spec],
    )
    second_normed = second_normed.reshape(rows, width)

    def feed_on(pieces, biases, before):
        return feed_part(second_normed, feed_grad, pieces, biases, before)

    second_normed, feed_far_low = tie(second_normed, feed_far_low)
    far_low_other = exchange(feed_far_low, last)[1]
    sums, (part0,), bias0 = feed_on([feed_own], up_biases[:1], None)
    *sums, far_low_other, feed_far_high = tie(*sums, far_low_other, feed_far_high)
    far_high_other = exchange(feed_far_high, last)[1]
    sums, (part1,), bias1 = feed_on([feed_near], up_biases[1:2], sums)
    *sums, far_high_other = tie(*sums, far_high_other)
    feed_far = whole_feed(feed_far_low, feed_far_high, far_low_other, far_high_other)
    *sums, feed_far, part1 = tie(*sums, feed_far, part1)
    feed_cross = swap(feed_far, "narrow", 1)
    given = swap(part1, "narrow", 1)
    sums, (part2,), bias2 = feed_on([feed_far], up_biases[2:3], sums)
    *sums, given = tie(*sums, given)
    near_keep, near_give = cut(add_low(part0, given), "wide", last)
    up_give, down_give = near_give[:, :hidden], near_give[:, hidden:]
    *sums, near_keep, up_give, down_give = tie(*sums, near_keep, up_give, down_give)
    up_sent = swap(up_give, "wide", last[0])
    sums, (part3,), bias3 = feed_on([feed_cross], up_biases[3:], sums)
    feed, second_normed_grad, up_sent, part3, down_give = tie(*sums, up_sent, part3, down_give)
    down_sent = swap(down_give, "wide", last[0])
    given = swap(part3, "narrow", 1)
    up_bias_parts = bias0 + bias1 + bias2 + bias3

    layer_own, middle_grad, mixed_grad, back_sums = rows_call(
        second_back_kernel, "second_back", place,
        [feed.reshape(micro, own, width), second_normed_grad.reshape(micro, own, width), middle,
         mixed, cotangent, vectors],
        [part_spec, part_spec, part_spec, part_spec, own_spec, vec_spec],
        [low_rows, high_rows, low_rows, sum_rows],
        [part_spec, part_spec, part_spec, vec_spec],
    )
    layer_far = swap(layer_own, "narrow", 2)
    layer_parts = [
        layer_own, swap(layer_own, "narrow", 1), layer_far, swap(layer_far, "narrow", 1)
    ]

    def back_on(pieces, saved, grad_in, halo):
        return attend_back(
            offset, window_normed, mixed_grad, pieces, saved, bounds, grad_in, halo
        )

    mixed_grad, down_sent, given = tie(mixed_grad, down_sent, given)
    near = add_low(near_keep, jnp.concatenate([up_sent, down_sent], axis=1))
    far_cut = cut(add_low(part2, given), "wide", last)
    mixed_grad, near, *far_cut = tie(mixed_grad, near, *far_cut)
    far_sent = send_cut(far_cut, last)
    window_grad, (heads3,), sums3, _ = back_on([heads_cross], saved3, None, 0)
    given3 = swap(heads3, "narrow", 1)
    window_grad, *far_sent = tie(window_grad, *far_sent)
    far = add_low(far_cut[0], *far_sent)
    window_grad, far = tie(window_grad, far)
    far_given = swap(far, "narrow", 2)
    window_grad, (heads2,), sums2, _ = back_on([heads_far], saved2, window_grad, 0)
    window_grad, far_given, given3 = tie(window_grad, far_given, given3)
    mine = add_low(near, far_given)
    for bits in groups[:-1]:
        parts = cut(mine, "wide", bits)
        mine = add_low(parts[0], *send_cut(parts, bits))
    mine_cut = cut(mine, "wide", groups[-1])
    heads_sum = add_low(heads2, given3)
    window_grad, heads_sum, *mine_cut = tie(window_grad, heads_sum, *mine_cut)
    mine_sent = send_cut(mine_cut, groups[-1])
    heads_given = swap(heads_sum, "narrow", 2)
    window_grad, (heads1,), sums1, _ = back_on([heads_near], saved1, window_grad, 0)
    given1 = swap(heads1, "narrow", 1)
    window_grad, heads_given, *mine_sent = tie(window_grad, heads_given, *mine_sent)
    mine = add_low(mine_cut[0], *mine_sent)
    window_grad, mine = tie(window_grad, mine)
    mine_all = exchange(mine, groups[-1])
    window_grad, (heads0,), sums0, halos = back_on([heads_own], saved0, window_grad, halo)
    window_grad, *mine_all = tie(window_grad, *mine_all)
    window_grad, *layer_parts = tie(window_grad, *layer_parts)
    y_high, core_high = bit_of("narrow", 2), bit_of("narrow", 1)
    layer_near = join(layer_parts[0], layer_parts[1], core_high, 1)
    layer_far = join(layer_parts[2], layer_parts[3], core_high, 1)
    layer_out = join(layer_near, layer_far, y_high, 1).reshape(micro, row_count, width)
    mine = arrange(mine_all, groups[-1], 0).reshape((-1,) + mine.shape[1:])
    for bits in reversed(groups[:-1]):
        mine = arrange(exchange(mine, bits), bits, 0).reshape((-1,) + mine.shape[1:])
    feed_total = spread_last(mine)
    heads_total = spread_last(
        spread_far(reduce_far(reduce_last(add_low(heads0, given1, heads_given))))
    )
    head_bias_parts = [
        jnp.concatenate([s[0, 2 * cols : 3 * cols], s[0, cols : 2 * cols]])
        for s in [*sums0, *sums1, *sums2, *sums3]
    ]

    from_left = shift(halos[1], "narrow", 1)
    from_right = shift(halos[0], "narrow", -1)
    token_grad, first_sums = rows_call(
        first_back_kernel, "first_back", place,
        [window_grad, from_left, from_right, middle_grad, tokens, vectors],
        [per_micro((window, width)), per_micro((halo, width)), per_micro((halo, width)), part_spec,
         own_spec, vec_spec],
        [low_rows, sum_rows], [part_spec, vec_spec],
    )
    outer = jnp.stack([mixer_scale, feed_scale] + [jnp.ones_like(out_bias)] * 6)
    sums = (back_sums + first_sums) * outer
    group_sums = jnp.stack(
        [jnp.concatenate([head_bias_parts[r], up_bias_parts[r][0]]) for r in range(narrow_size)]
    )
    group_sums = jnp.stack([group_sums[r ^ narrow_at] for r in range(narrow_size)])
    packed = jnp.concatenate([sums.reshape(-1), group_sums.reshape(-1)]).reshape(-1, 128)
    packed = reduce_everywhere(packed).reshape(-1)
    sums = packed[: 8 * width].reshape(8, width)
    group_sums = packed[8 * width :].reshape(narrow_size, -1)
    mine = lax.dynamic_slice_in_dim(group_sums, narrow_at, 1, 0)[0]

    heads_grad = jnp.stack(
        [heads_total[:, 2 * cols : 3 * cols], heads_total[:, :cols], heads_total[:, cols : 2 * cols]],
        axis=1,
    ).astype(f32)
    out_grad = heads_total[:, 3 * cols :].T.astype(f32)
    return (
        layer_out, token_grad, heads_grad, mine[: 2 * cols].reshape(2, cols), out_grad, sums[0],
        feed_total[:, :hidden].astype(f32), mine[2 * cols :],
        feed_total[:, hidden:].T.astype(f32), sums[1], sums[2],
        sums[3], sums[4], sums[5], sums[6], sums[7],
    )


def solution(mesh):
    return jax.shard_map(
        body,
        mesh=mesh,
        in_specs=(
            P(None, "wide", None),
            P(None, "wide", None),
            P("wide", None, "narrow"),
            P(None, "narrow"),
            P("narrow", "wide"),
            P(),
            P("wide", "narrow"),
            P("narrow"),
            P("narrow", "wide"),
            P(),
            P(),
            P(),
            P(),
            P(),
            P(),
            P(),
            P(None, "wide", None),
        ),
        out_specs=(
            P(None, "wide", None),
            P(None, ("wide", "narrow"), None),
            P(None, None, "narrow"),
            P(None, "narrow"),
            P("narrow", None),
            P(),
            P(None, "narrow"),
            P("narrow"),
            P("narrow", None),
            P(),
            P(),
            P(),
            P(),
            P(),
            P(),
            P(),
        ),
        check_vma=False,
    )
```

```python
import math
from functools import partial

import jax
import jax.numpy as jnp
from jax import lax
from jax.experimental import pallas as pl
from jax.experimental.pallas import tpu as pltpu
from jax.sharding import PartitionSpec as P

HEAD_DIM = 64
MOST = 196
epsilon = 1e-06
bf16 = jnp.bfloat16
f32 = jnp.float32
LOG2E = math.log2(math.e)
VMEM_LIMIT = 60 * 1024 * 1024
FEED_CHUNKS = 2
QUERIES = 160


def round_up(value, step):
    return -(-value // step) * step


def nt(left, right):
    return lax.dot_general(left, right, (((1,), (1,)), ((), ())), preferred_element_type=f32)


def tn(left, right):
    return lax.dot_general(left, right, (((0,), (0,)), ((), ())), preferred_element_type=f32)


def nn(left, right):
    return jnp.dot(left, right, preferred_element_type=f32)


def query_chunk(own):
    return QUERIES if own % QUERIES == 0 else own


def key_span(own, win):
    return min(win, query_chunk(own) + 2 * round_up(MOST - 1, 16))


def key_start(off, at, own, win):
    first = jnp.clip(off + at - round_up(MOST - 1, 16), 0, win - key_span(own, win))
    return pl.multiple_of(first, 16)


def params():
    return pltpu.CompilerParams(
        dimension_semantics=("arbitrary",), vmem_limit_bytes=VMEM_LIMIT
    )


def cost(flops, transcendentals, moved):
    return pl.CostEstimate(flops=1024, transcendentals=0, bytes_accessed=1024)


def full(shape):
    return pl.BlockSpec(shape, lambda *a: (0,) * len(shape))


def per_micro(shape):
    return pl.BlockSpec((1,) + shape, lambda m, *a: (m,) + (0,) * len(shape))


def stack_heads(rows, heads):
    lane = lax.broadcasted_iota(jnp.int32, rows.shape, 1) // HEAD_DIM
    zero = jnp.zeros_like(rows)
    return jnp.concatenate([jnp.where(lane == h, rows, zero) for h in range(heads)], axis=0)


def unstack_heads(stacked, heads):
    rows = stacked.shape[0] // heads
    lane = lax.broadcasted_iota(jnp.int32, (rows, stacked.shape[1]), 1) // HEAD_DIM
    out = stacked[:rows]
    for h in range(1, heads):
        out = jnp.where(lane == h, stacked[h * rows : (h + 1) * rows], out)
    return out


def attend_kernel(own, heads, count, first, off_ref, *refs):
    x_ref, b_ref, bnd_ref = refs[:3]
    w_refs = refs[3 : 3 + count]
    rest = refs[3 + count + (0 if first else 1) :]
    mixed_ref = rest[0]
    off = pl.multiple_of(off_ref[0], 16)
    win = x_ref.shape[1]
    cols = heads * HEAD_DIM
    xw = x_ref[0]
    xo = x_ref[0, pl.ds(off, own), :]
    size, span = query_chunk(own), key_span(own, win)
    place = lax.broadcasted_iota(jnp.int32, (span, heads * size), 0)
    mixed = None if first else refs[3 + count][0]
    for i in range(count):
        q_ref, k_ref, v_ref, o_ref, l_ref = rest[1 + 5 * i : 6 + 5 * i]
        w = w_refs[i]
        both = nn(xw, w[:, : 2 * cols])
        k = both[:, :cols].astype(bf16)
        v = (both[:, cols:] + b_ref[i, 1:2]).astype(bf16)
        q = (nn(xo, w[:, 2 * cols : 3 * cols]) + b_ref[i, 0:1]).astype(bf16)
        q_ref[0] = q
        k_ref[0] = k
        v_ref[0] = v
        parts = []
        for c in range(own // size):
            key_at = key_start(off, c * size, own, win)
            kc, vc = k_ref[0, pl.ds(key_at, span), :], v_ref[0, pl.ds(key_at, span), :]
            qs = stack_heads(q[c * size : (c + 1) * size], heads)
            keep = (place >= bnd_ref[0, c, 0:1] - key_at) & (place < bnd_ref[0, c, 1:2] - key_at)
            scores = nt(kc, qs) * (HEAD_DIM**-0.5 * LOG2E)
            scores = jnp.where(keep, scores, -1e30)
            top = jnp.max(scores, axis=0, keepdims=True)
            weights = jnp.exp2(scores - top)
            total = jnp.sum(weights, axis=0, keepdims=True)
            out = tn(vc, weights.astype(bf16)) * (1.0 / total)
            parts.append(unstack_heads(out.T, heads).astype(bf16))
            l_ref[0, c] = top + jnp.log2(total)
        out = jnp.concatenate(parts, axis=0)
        o_ref[0] = out
        part = nt(out, w[:, 3 * cols :])
        mixed = part if mixed is None else mixed + part
    mixed_ref[0] = mixed


def attend(off, x_win, pieces, bias, bounds, own, mixed):
    micro, win, width = x_win.shape
    cols = pieces[0].shape[1] // 4
    heads = cols // HEAD_DIM
    size = query_chunk(own)
    stacked = heads * size
    count = len(pieces)
    first = mixed is None
    shapes = [jax.ShapeDtypeStruct((micro, own, width), f32)]
    specs = [per_micro((own, width))]
    for _ in pieces:
        for rows in (own, win, win, own):
            shapes.append(jax.ShapeDtypeStruct((micro, rows, cols), bf16))
            specs.append(per_micro((rows, cols)))
        shapes.append(jax.ShapeDtypeStruct((micro, own // size, 1, stacked), f32))
        specs.append(per_micro((own // size, 1, stacked)))
    args = [x_win, bias, bounds] + list(pieces)
    in_specs = [per_micro((win, width)), full(bias.shape), per_micro((own // size, 2, stacked))]
    in_specs += [full((width, 4 * cols))] * count
    if not first:
        args.append(mixed)
        in_specs.append(per_micro((own, width)))
    result = pl.pallas_call(
        partial(attend_kernel, own, heads, count, first),
        grid_spec=pltpu.PrefetchScalarGridSpec(
            num_scalar_prefetch=1, grid=(micro,), in_specs=in_specs, out_specs=specs
        ),
        out_shape=shapes,
        compiler_params=params(),
        cost_estimate=cost(
            count * micro * 2 * (win * width * cols * 3 + 8 * stacked * win * HEAD_DIM),
            count * micro * stacked * win,
            micro * win * width * 2 + count * 4 * width * cols * 2,
        ),
        name="attend",
    )(off, *args)
    return result[0], [tuple(result[1 + 5 * i : 6 + 5 * i]) for i in range(count)]


def attend_back_kernel(own, heads, count, first, halo, off_ref, *refs):
    x_ref, mg_ref, bnd_ref = refs[:3]
    w_refs = refs[3 : 3 + count]
    saved = refs[3 + count : 3 + 6 * count]
    at = 3 + 6 * count
    in_ref = None if first else refs[at]
    rest = refs[at + (0 if first else 1) :]
    dn_ref = rest[0]
    halo_refs = rest[1 + 2 * count : 1 + 2 * count + (2 if halo else 0)]
    *acc_refs, dkv_ref = rest[1 + 2 * count + len(halo_refs) :]
    off = pl.multiple_of(off_ref[0], 16)
    win = x_ref.shape[1]
    cols = heads * HEAD_DIM
    scale = HEAD_DIM**-0.5
    step = pl.program_id(0)
    mg = mg_ref[0]
    xt = x_ref[0].T
    xot = x_ref[0, pl.ds(off, own), :].T
    mgt = mg.T
    size, span = query_chunk(own), key_span(own, win)
    place = lax.broadcasted_iota(jnp.int32, (span, heads * size), 0)
    dn = None if first else in_ref[0]
    dn_own = None
    for i in range(count):
        w = w_refs[i]
        q_ref, k_ref, v_ref, o_ref, l_ref = saved[5 * i : 5 * i + 5]
        dw_ref, db_ref = rest[1 + 2 * i : 3 + 2 * i]
        acc_ref = acc_refs[i]
        o = o_ref[0]
        g = nn(mg, w[:, 3 * cols :]).astype(bf16)
        dkv_ref[...] = jnp.zeros_like(dkv_ref)
        parts = []
        for c in range(own // size):
            key_at = key_start(off, c * size, own, win)
            keys = pl.ds(key_at, span)
            kc, vc = k_ref[0, keys, :], v_ref[0, keys, :]
            qs = stack_heads(q_ref[0, c * size : (c + 1) * size, :], heads)
            gs = stack_heads(g[c * size : (c + 1) * size], heads)
            keep = (place >= bnd_ref[0, c, 0:1] - key_at) & (place < bnd_ref[0, c, 1:2] - key_at)
            scores = nt(kc, qs) * (scale * LOG2E) - l_ref[0, c]
            weights = jnp.exp2(jnp.where(keep, scores, -1e30))
            weighed = weights * nt(vc, gs)
            delta = jnp.sum(weighed, axis=0, keepdims=True)
            slope = (weighed - weights * delta).astype(bf16)
            parts.append((unstack_heads(tn(kc, slope).T, heads) * scale).astype(bf16))
            dkv_ref[0, keys, :] += nn(slope, qs)
            dkv_ref[1, keys, :] += nn(weights.astype(bf16), gs)
        dq = jnp.concatenate(parts, axis=0)
        dkv = jnp.concatenate([dkv_ref[0] * scale, dkv_ref[1]], axis=1).astype(bf16)
        part = nt(dkv, w[:, : 2 * cols])
        dn = part if dn is None else dn + part
        part = nt(dq, w[:, 2 * cols : 3 * cols])
        dn_own = part if dn_own is None else dn_own + part
        left = nn(xt, dkv)
        right = jnp.concatenate([nn(xot, dq), nn(mgt, o)], axis=1)
        sums = jnp.concatenate(
            [
                jnp.sum(dkv.astype(f32), axis=0, keepdims=True),
                jnp.sum(jnp.concatenate([dq, dq], axis=1).astype(f32), axis=0, keepdims=True),
            ],
            axis=1,
        )

        @pl.when(step == 0)
        def _():
            acc_ref[:, : 2 * cols] = left
            acc_ref[:, 2 * cols :] = right
            db_ref[...] = sums

        @pl.when(step > 0)
        def _():
            acc_ref[:, : 2 * cols] += left
            acc_ref[:, 2 * cols :] += right
            db_ref[...] += sums

        @pl.when(step == pl.num_programs(0) - 1)
        def _():
            dw_ref[...] = acc_ref[...].astype(bf16)

    dn_ref[0] = dn
    dn_ref[0, pl.ds(off, own), :] += dn_own
    if halo:
        before = pl.multiple_of(jnp.maximum(off - halo, 0), 16)
        after = pl.multiple_of(jnp.minimum(off + own, win - halo), 16)
        halo_refs[0][0] = dn_ref[0, pl.ds(before, halo), :].astype(bf16)
        halo_refs[1][0] = dn_ref[0, pl.ds(after, halo), :].astype(bf16)


def attend_back(off, x_win, mixed_grad, pieces, saved, bounds, grad_in, halo):
    micro, win, width = x_win.shape
    own = mixed_grad.shape[1]
    cols = pieces[0].shape[1] // 4
    heads = cols // HEAD_DIM
    size = query_chunk(own)
    stacked = heads * size
    count = len(pieces)
    first = grad_in is None
    args = [x_win, mixed_grad, bounds] + list(pieces)
    in_specs = [per_micro((win, width)), per_micro((own, width)), per_micro((own // size, 2, stacked))]
    in_specs += [full((width, 4 * cols))] * count
    for one in saved:
        args += list(one)
        in_specs += [per_micro((rows, cols)) for rows in (own, win, win, own)]
        in_specs.append(per_micro((own // size, 1, stacked)))
    if not first:
        args.append(grad_in)
        in_specs.append(per_micro((win, width)))
    shapes = [jax.ShapeDtypeStruct((micro, win, width), f32)]
    specs = [per_micro((win, width))]
    for _ in pieces:
        shapes += [
            jax.ShapeDtypeStruct((width, 4 * cols), bf16),
            jax.ShapeDtypeStruct((1, 4 * cols), f32),
        ]
        specs += [full((width, 4 * cols)), full((1, 4 * cols))]
    for _ in range(2 if halo else 0):
        shapes.append(jax.ShapeDtypeStruct((micro, halo, width), bf16))
        specs.append(per_micro((halo, width)))
    result = pl.pallas_call(
        partial(attend_back_kernel, own, heads, count, first, halo),
        grid_spec=pltpu.PrefetchScalarGridSpec(
            num_scalar_prefetch=1,
            grid=(micro,),
            in_specs=in_specs,
            out_specs=specs,
            scratch_shapes=[pltpu.VMEM((width, 4 * cols), f32)] * count
            + [pltpu.VMEM((2, win, cols), f32)],
        ),
        out_shape=shapes,
        compiler_params=params(),
        cost_estimate=cost(
            count * micro * (40 * stacked * win * HEAD_DIM + 12 * win * width * cols),
            count * micro * stacked * win,
            micro * (10 * win) * width + count * 4 * width * cols * 4,
        ),
        name="attend_back",
    )(off, *args)
    return result[0], result[1 : 1 + 2 * count : 2], result[2 : 2 + 2 * count : 2], result[1 + 2 * count :]


def feed_kernel(chunks, count, first, *refs):
    x_ref, g_ref = refs[:2]
    w_refs = refs[2 : 2 + count]
    b_refs = refs[2 + count : 2 + 2 * count]
    at = 2 + 2 * count
    if not first:
        fi_ref, ni_ref = refs[at : at + 2]
        at = at + 2
    f_ref, n_ref = refs[at : at + 2]
    outs = refs[at + 2 : at + 2 + 2 * count]
    act_ref, ug_ref, xt_ref, gt_ref = refs[at + 2 + 2 * count :]
    rows = x_ref.shape[0]
    step = rows // chunks
    xt_ref[...] = x_ref[...].T
    gt_ref[...] = g_ref[...].T
    for i in range(count):
        w_ref, b_ref = w_refs[i], b_refs[i]
        dw_ref, db_ref = outs[2 * i : 2 * i + 2]
        hidden = b_ref.shape[1]
        total = jnp.zeros((1, hidden), f32)
        for c in range(chunks):
            rows_at = pl.ds(c * step, step)
            upper = nn(x_ref[rows_at, :], w_ref[:, :hidden]) + b_ref[...]
            phi = 0.5 + 0.5 * lax.erf(upper * math.sqrt(0.5))
            active = (upper * phi).astype(bf16)
            bell = jnp.exp2(upper * upper * (-0.5 * LOG2E)) * (1.0 / math.sqrt(2.0 * math.pi))
            slope = phi + upper * bell
            grad = (nn(g_ref[rows_at, :], w_ref[:, hidden:]) * slope).astype(bf16)
            act_ref[rows_at, :] = active
            ug_ref[rows_at, :] = grad
            total = total + jnp.sum(grad.astype(f32), axis=0, keepdims=True)
            feed = nt(active, w_ref[:, hidden:])
            back = nt(grad, w_ref[:, :hidden])
            if i > 0:
                feed = feed + f_ref[rows_at, :]
                back = back + n_ref[rows_at, :]
            elif not first:
                feed = feed + fi_ref[rows_at, :]
                back = back + ni_ref[rows_at, :]
            f_ref[rows_at, :] = feed
            n_ref[rows_at, :] = back
        db_ref[...] = total
        dw_ref[:, :hidden] = nn(xt_ref[...], ug_ref[...]).astype(bf16)
        dw_ref[:, hidden:] = nn(gt_ref[...], act_ref[...]).astype(bf16)


def feed_part(x2, grad, pieces, biases, before):
    rows, width = x2.shape
    hidden = biases[0].shape[1]
    count = len(pieces)
    first = before is None
    args = [x2, grad] + list(pieces) + list(biases)
    aliases = {}
    if not first:
        aliases = {len(args): 0, len(args) + 1: 1}
        args += list(before)
    whole = pl.BlockSpec(memory_space=pltpu.VMEM)
    shapes = [jax.ShapeDtypeStruct((rows, width), f32)] * 2
    for _ in pieces:
        shapes += [
            jax.ShapeDtypeStruct((width, 2 * hidden), bf16),
            jax.ShapeDtypeStruct((1, hidden), f32),
        ]
    result = pl.pallas_call(
        partial(feed_kernel, FEED_CHUNKS, count, first),
        in_specs=[whole] * len(args),
        out_specs=[whole] * len(shapes),
        out_shape=shapes,
        scratch_shapes=[
            pltpu.VMEM((rows, hidden), bf16),
            pltpu.VMEM((rows, hidden), bf16),
            pltpu.VMEM((width, rows), bf16),
            pltpu.VMEM((width, rows), bf16),
        ],
        input_output_aliases=aliases,
        compiler_params=pltpu.CompilerParams(vmem_limit_bytes=VMEM_LIMIT),
        cost_estimate=cost(
            count * 12 * rows * width * hidden,
            count * 2 * rows * hidden,
            16 * rows * width + count * 8 * width * hidden,
        ),
        name="feed_part",
    )(*args)
    return tuple(result[:2]), list(result[2::2]), list(result[3::2])


def norm_parts(values_in):
    center = jnp.mean(values_in, axis=-1, keepdims=True)
    shifted = values_in - center
    inverse = lax.rsqrt(jnp.mean(shifted * shifted, axis=-1, keepdims=True) + epsilon)
    return (shifted * inverse, inverse)


def norm_back(grad_in, unit_rows, inverse, gain_row):
    scaled = grad_in * gain_row
    return inverse * (
        scaled
        - jnp.mean(scaled, axis=-1, keepdims=True)
        - unit_rows * jnp.mean(scaled * unit_rows, axis=-1, keepdims=True)
    )


VECTORS = (
    "out_bias", "down_bias", "first_gain", "first_shift", "second_gain", "second_shift",
    "mixer_scale", "feed_scale",
)


def row(vec_ref, name):
    at = VECTORS.index(name)
    return vec_ref[at : at + 1]


def own_rows(shape):
    return pl.BlockSpec((1,) + shape, lambda m, place: (m, place[0]) + (0,) * (len(shape) - 1))


def rows_call(kernel, name, place, args, specs, shapes, out_specs):
    micro = args[0].shape[0]
    return pl.pallas_call(
        kernel,
        grid_spec=pltpu.PrefetchScalarGridSpec(
            num_scalar_prefetch=1, grid=(micro,), in_specs=specs, out_specs=out_specs
        ),
        out_shape=shapes,
        compiler_params=params(),
        cost_estimate=cost(0, 0, 0),
        name=name,
    )(place, *args)


def first_norm_kernel(place_ref, x_ref, c_ref, vec_ref, n_ref, g_ref):
    start = pl.multiple_of(place_ref[1], 16)
    win = n_ref.shape[1]
    unit = norm_parts(x_ref[0, pl.ds(start, win), :].astype(f32))[0]
    n_ref[0] = (unit * row(vec_ref, "first_gain") + row(vec_ref, "first_shift")).astype(bf16)
    g_ref[0] = (row(vec_ref, "feed_scale") * c_ref[0].astype(f32)).astype(bf16)


def second_norm_kernel(place_ref, mixed_ref, x_ref, vec_ref, m_ref, n_ref):
    branch = mixed_ref[0] + row(vec_ref, "out_bias")
    middle = x_ref[0].astype(f32) + row(vec_ref, "mixer_scale") * branch
    m_ref[0] = middle
    unit = norm_parts(middle)[0]
    n_ref[0] = (unit * row(vec_ref, "second_gain") + row(vec_ref, "second_shift")).astype(bf16)


def column_sums(sum_ref, rows_in):
    total = jnp.concatenate([jnp.sum(r, axis=0, keepdims=True) for r in rows_in], axis=0)

    @pl.when(pl.program_id(0) == 0)
    def _():
        sum_ref[...] = total

    @pl.when(pl.program_id(0) > 0)
    def _():
        sum_ref[...] += total


def second_back_kernel(
    place_ref, feed_ref, back_ref, m_ref, mixed_ref, c_ref, vec_ref, l_ref, mg_ref, low_ref, sum_ref
):
    middle, back, grad = m_ref[0], back_ref[0], c_ref[0].astype(f32)
    feed_scale = row(vec_ref, "feed_scale")
    branch = feed_ref[0] + row(vec_ref, "down_bias")
    l_ref[0] = (middle + feed_scale * branch).astype(bf16)
    unit, inverse = norm_parts(middle)
    middle_grad = grad + norm_back(back, unit, inverse, row(vec_ref, "second_gain"))
    mg_ref[0] = middle_grad
    low_ref[0] = (row(vec_ref, "mixer_scale") * middle_grad).astype(bf16)
    mixer = mixed_ref[0] + row(vec_ref, "out_bias")
    zero = jnp.zeros_like(grad[:8])
    column_sums(
        sum_ref,
        [middle_grad, grad, zero, zero, back * unit, back, middle_grad * mixer, grad * branch],
    )


def first_back_kernel(
    place_ref, win_ref, left_ref, right_ref, mg_ref, x_ref, vec_ref, t_ref, sum_ref
):
    own, halo = mg_ref.shape[1], left_ref.shape[1]
    off = pl.multiple_of(place_ref[2], 16)
    gap = jnp.zeros((own - halo, left_ref.shape[2]), f32)
    grad = win_ref[0, pl.ds(off, own), :]
    grad = grad + jnp.concatenate([left_ref[0].astype(f32), gap], axis=0)
    grad = grad + jnp.concatenate([gap, right_ref[0].astype(f32)], axis=0)
    unit, inverse = norm_parts(x_ref[0].astype(f32))
    t_ref[0] = (
        mg_ref[0] + norm_back(grad, unit, inverse, row(vec_ref, "first_gain"))
    ).astype(bf16)
    zero = jnp.zeros_like(grad[:8])
    column_sums(sum_ref, [zero, zero, grad * unit, grad, zero, zero, zero, zero])


def swap(values_in, axis, bit):
    size = lax.axis_size(axis)
    return lax.ppermute(values_in, axis, [(i, i ^ bit) for i in range(size)])


def shift(values_in, axis, step):
    size = lax.axis_size(axis)
    pairs = [(i, i + step) for i in range(size) if 0 <= i + step < size]
    return lax.ppermute(values_in, axis, pairs)


def wide_bits(size):
    bits = []
    bit = size // 2
    while bit:
        bits.append(bit)
        bit //= 2
    return bits


def bit_of(axis, bit):
    return (lax.axis_index(axis) & bit) != 0


def join(mine, other, is_high, axis):
    low = jnp.where(is_high, other, mine)
    high = jnp.where(is_high, mine, other)
    return jnp.stack([low, high], axis=axis)


def tie(*values_in):
    return lax.optimization_barrier(values_in)


def far_groups():
    bits = wide_bits(lax.axis_size("wide"))[:-1]
    return [bits[i : i + 2] for i in range(0, len(bits), 2)]


def offsets(bits):
    return [
        sum(bit for i, bit in enumerate(reversed(bits)) if (k >> i) & 1)
        for k in range(2 ** len(bits))
    ]


def exchange(values_in, bits):
    return [values_in] + [swap(values_in, "wide", o) for o in offsets(bits)[1:]]


def arrange(parts, bits, axis):
    if not bits:
        return jnp.expand_dims(parts[0], axis)
    half = len(parts) // 2
    low = arrange(parts[:half], bits[1:], axis)
    high = arrange(parts[half:], bits[1:], axis)
    is_high = bit_of("wide", bits[0])
    return jnp.concatenate(
        [jnp.where(is_high, high, low), jnp.where(is_high, low, high)], axis=axis
    )


def arrange_blocks(parts, bits):
    return arrange(parts, bits, 1).reshape((-1,) + parts[0].shape[1:])


def last_bit():
    return wide_bits(lax.axis_size("wide"))[-1]


def gather_narrow(piece):
    far = swap(piece, "narrow", 2)
    return [piece, swap(piece, "narrow", 1), far, swap(far, "narrow", 1)]


def add_low(*parts):
    total = parts[0].astype(f32)
    for part in parts[1:]:
        total = total + part.astype(f32)
    return total.astype(bf16)


def cut(values_in, axis, bits):
    count = 2 ** len(bits)
    size = values_in.shape[0] // count
    at = lax.axis_index(axis)
    places = []
    for o in offsets(bits):
        other = at ^ o
        place = 0
        for bit in bits:
            place = 2 * place + ((other & bit) != 0).astype(jnp.int32)
        places.append(place)
    return [lax.dynamic_slice_in_dim(values_in, p * size, size, 0) for p in places]


def send_cut(parts, bits):
    return [swap(part, "wide", o) for part, o in zip(parts[1:], offsets(bits)[1:])]


def spread_last(part):
    bits = [last_bit()]
    return arrange(exchange(part, bits), bits, 0).reshape((-1,) + part.shape[1:])


def tree_sum(parts):
    while len(parts) > 1:
        parts = [parts[i] + parts[i + 1] for i in range(0, len(parts), 2)]
    return parts[0]


def reduce_wide(values_in):
    for bits in far_groups() + [[last_bit()]]:
        values_in = tree_sum(exchange(values_in, bits))
    return values_in


def reduce_narrow(values_in):
    return tree_sum([values_in] + [swap(values_in, "narrow", o) for o in (1, 2, 3)])


def body(
    tokens, image_lengths, heads_weight, heads_bias, out_weight, out_bias, up_weight, up_bias,
    down_weight, down_bias, first_gain, first_shift, second_gain, second_shift, mixer_scale,
    feed_scale, cotangent,
):
    micro, row_count, width = tokens.shape
    narrow_size = lax.axis_size("narrow")
    narrow_at = lax.axis_index("narrow")
    own = row_count // narrow_size
    cols = heads_weight.shape[2]
    heads = cols // HEAD_DIM
    rows = micro * own
    halo = round_up(MOST - 1, 16)
    window = min(row_count, round_up(own + 2 * halo, 128))
    lead = round_up((window - own) // 2, 16)
    start = jnp.clip(narrow_at * own - lead, 0, row_count - window)
    off = narrow_at * own - start
    offset = off.reshape(1).astype(jnp.int32)

    hidden = up_weight.shape[1]
    groups = far_groups()

    bias_pieces = gather_narrow(
        jnp.concatenate([heads_bias.reshape(-1), up_bias]).reshape(1, -1)
    )
    qv_biases = [heads_bias[None]]
    qv_biases += [b[:, : 2 * cols].reshape(1, 2, cols) for b in bias_pieces[1:]]
    up_biases = [up_bias.reshape(1, hidden)] + [b[:, 2 * cols :] for b in bias_pieces[1:]]
    heads_blocks = jnp.concatenate(
        [heads_weight[:, 1], heads_weight[:, 2], heads_weight[:, 0], out_weight.T], axis=1
    )[None]
    for bits in groups:
        heads_blocks = arrange_blocks(exchange(heads_blocks, bits), bits)
    feed_blocks = jnp.concatenate([up_weight, down_weight.T], axis=1)[None]
    heads_blocks, feed_blocks = tie(heads_blocks, feed_blocks)
    for bits in groups[:-1]:
        feed_blocks = arrange_blocks(exchange(feed_blocks, bits), bits)
    feed_parts = exchange(feed_blocks, groups[-1])
    last = [last_bit()]
    heads_all = arrange_blocks(exchange(heads_blocks, last), last)
    heads_own = heads_all.reshape(width, -1)

    ends = jnp.cumsum(image_lengths[:, 0], axis=1)
    places = narrow_at * own + jnp.arange(own, dtype=jnp.int32)
    passed = ends[:, :, None] <= places[None, None, :]
    first_key = jnp.max(jnp.where(passed, ends[:, :, None], 0), axis=1) - start
    last_key = jnp.min(jnp.where(passed, row_count, ends[:, :, None]), axis=1) - start
    bounds = jnp.stack([first_key, last_key], axis=1).astype(jnp.int32)
    size = query_chunk(own)
    bounds = bounds.reshape(micro, 2, own // size, size).transpose(0, 2, 1, 3)
    bounds = jnp.tile(bounds, (1, 1, 1, heads))

    place = jnp.stack([narrow_at, start, off]).astype(jnp.int32)
    vectors = jnp.stack(
        [out_bias, down_bias, first_gain, first_shift, second_gain, second_shift, mixer_scale,
         feed_scale]
    )
    own_spec, part_spec, vec_spec = own_rows((own, width)), per_micro((own, width)), full((8, width))
    low_rows = jax.ShapeDtypeStruct((micro, own, width), bf16)
    high_rows = jax.ShapeDtypeStruct((micro, own, width), f32)
    sum_rows = jax.ShapeDtypeStruct((8, width), f32)
    window_normed, feed_grad = rows_call(
        first_norm_kernel, "first_norm", place, [tokens, cotangent, vectors],
        [per_micro((row_count, width)), own_spec, vec_spec],
        [jax.ShapeDtypeStruct((micro, window, width), bf16), low_rows],
        [per_micro((window, width)), part_spec],
    )
    feed_grad = feed_grad.reshape(rows, width)

    def halves(blocks):
        half = blocks.shape[0] // 2
        return blocks[:half], blocks[half:]

    def attend_on(piece, at, before):
        return attend(offset, window_normed, [piece], qv_biases[at], bounds, own, before)

    heads_low, heads_high = halves(heads_all)
    window_normed, heads_low, *biases = tie(window_normed, heads_low, *qv_biases, *up_biases)
    qv_biases, up_biases = biases[:narrow_size], biases[narrow_size:]
    heads_near = swap(heads_own, "narrow", 1)
    far_low = swap(heads_low, "narrow", 2)
    mixed, saved0 = attend_on(heads_own, 0, None)
    mixed, far_low, *feed_parts = tie(mixed, far_low, *feed_parts)
    feed_low, feed_high = halves(arrange_blocks(feed_parts, groups[-1]))
    mixed, feed_low, feed_high, heads_high = tie(mixed, feed_low, feed_high, heads_high)
    far_high = swap(heads_high, "narrow", 2)
    low_other = exchange(feed_low, last)[1]
    mixed, saved1 = attend_on(heads_near, 1, mixed)
    mixed, far_high, low_other = tie(mixed, far_high, low_other)
    heads_far = jnp.concatenate([far_low, far_high], axis=0).reshape(width, -1)
    mixed, heads_far, feed_low, feed_high = tie(mixed, heads_far, feed_low, feed_high)
    heads_cross = swap(heads_far, "narrow", 1)
    high_other = exchange(feed_high, last)[1]
    feed_far_low = swap(feed_low, "narrow", 2)
    mixed, saved2 = attend_on(heads_far, 2, mixed)
    mixed, high_other, feed_far_low = tie(mixed, high_other, feed_far_low)

    def whole_feed(low, high, low_sent, high_sent):
        mine = jnp.concatenate([low, high], axis=0)
        other = jnp.concatenate([low_sent, high_sent], axis=0)
        return arrange_blocks([mine, other], last).reshape(width, -1)

    feed_own = whole_feed(feed_low, feed_high, low_other, high_other)
    mixed, feed_own, feed_high = tie(mixed, feed_own, feed_high)
    feed_near = swap(feed_own, "narrow", 1)
    feed_far_high = swap(feed_high, "narrow", 2)
    mixed, saved3 = attend_on(heads_cross, 3, mixed)
    mixed, feed_far_high = tie(mixed, feed_far_high)
    middle, second_normed = rows_call(
        second_norm_kernel, "second_norm", place, [mixed, tokens, vectors],
        [part_spec, own_spec, vec_spec], [high_rows, low_rows], [part_spec, part_spec],
    )
    second_normed = second_normed.reshape(rows, width)

    def feed_on(pieces, biases, before):
        return feed_part(second_normed, feed_grad, pieces, biases, before)

    second_normed, feed_far_low = tie(second_normed, feed_far_low)
    far_low_other = exchange(feed_far_low, last)[1]
    sums, (part0,), bias0 = feed_on([feed_own], up_biases[:1], None)
    *sums, far_low_other, feed_far_high = tie(*sums, far_low_other, feed_far_high)
    far_high_other = exchange(feed_far_high, last)[1]
    sums, (part1,), bias1 = feed_on([feed_near], up_biases[1:2], sums)
    *sums, far_high_other = tie(*sums, far_high_other)
    feed_far = whole_feed(feed_far_low, feed_far_high, far_low_other, far_high_other)
    *sums, feed_far, part1 = tie(*sums, feed_far, part1)
    feed_cross = swap(feed_far, "narrow", 1)
    given = swap(part1, "narrow", 1)
    sums, (part2,), bias2 = feed_on([feed_far], up_biases[2:3], sums)
    *sums, given = tie(*sums, given)
    near_keep, near_give = cut(add_low(part0, given), "wide", last)
    up_give, down_give = near_give[:, :hidden], near_give[:, hidden:]
    *sums, near_keep, up_give, down_give = tie(*sums, near_keep, up_give, down_give)
    up_sent = swap(up_give, "wide", last[0])
    sums, (part3,), bias3 = feed_on([feed_cross], up_biases[3:], sums)
    feed, second_normed_grad, up_sent, part3, down_give = tie(*sums, up_sent, part3, down_give)
    down_sent = swap(down_give, "wide", last[0])
    given = swap(part3, "narrow", 1)
    up_bias_parts = bias0 + bias1 + bias2 + bias3

    layer_own, middle_grad, mixed_grad, back_sums = rows_call(
        second_back_kernel, "second_back", place,
        [feed.reshape(micro, own, width), second_normed_grad.reshape(micro, own, width), middle,
         mixed, cotangent, vectors],
        [part_spec, part_spec, part_spec, part_spec, own_spec, vec_spec],
        [low_rows, high_rows, low_rows, sum_rows],
        [part_spec, part_spec, part_spec, vec_spec],
    )
    def back_on(pieces, saved, grad_in, halo):
        return attend_back(
            offset, window_normed, mixed_grad, pieces, saved, bounds, grad_in, halo
        )

    mixed_grad, down_sent, given = tie(mixed_grad, down_sent, given)
    near = add_low(near_keep, jnp.concatenate([up_sent, down_sent], axis=1))
    far_cut = cut(add_low(part2, given), "wide", last)
    mixed_grad, near, layer_own, *far_cut = tie(mixed_grad, near, layer_own, *far_cut)
    layer_far = swap(layer_own, "narrow", 2)
    far_sent = send_cut(far_cut, last)
    window_grad, (heads3,), sums3, _ = back_on([heads_cross], saved3, None, 0)
    given3 = swap(heads3, "narrow", 1)
    window_grad, layer_far, *far_sent = tie(window_grad, layer_far, *far_sent)
    far = add_low(far_cut[0], *far_sent)
    window_grad, far, layer_far = tie(window_grad, far, layer_far)
    layer_parts = [
        layer_own, swap(layer_own, "narrow", 1), layer_far, swap(layer_far, "narrow", 1)
    ]
    far_given = swap(far, "narrow", 2)
    window_grad, (heads2,), sums2, _ = back_on([heads_far], saved2, window_grad, 0)
    window_grad, far_given, given3, *layer_parts = tie(
        window_grad, far_given, given3, *layer_parts
    )
    mine = add_low(near, far_given)
    for bits in groups[:-1]:
        parts = cut(mine, "wide", bits)
        mine = add_low(parts[0], *send_cut(parts, bits))
    mine_cut = cut(mine, "wide", groups[-1])
    heads_sum = add_low(heads2, given3)
    window_grad, heads_sum, *mine_cut = tie(window_grad, heads_sum, *mine_cut)
    mine_sent = send_cut(mine_cut, groups[-1])
    heads_given = swap(heads_sum, "narrow", 2)
    window_grad, (heads1,), sums1, _ = back_on([heads_near], saved1, window_grad, 0)
    given1 = swap(heads1, "narrow", 1)
    window_grad, heads_given, *mine_sent = tie(window_grad, heads_given, *mine_sent)
    mine = add_low(mine_cut[0], *mine_sent)
    window_grad, mine = tie(window_grad, mine)
    mine_all = exchange(mine, groups[-1])
    window_grad, (heads0,), sums0, halos = back_on([heads_own], saved0, window_grad, halo)
    window_grad, *mine_all = tie(window_grad, *mine_all)
    heads_cut = cut(add_low(heads0, given1, heads_given), "wide", last)
    tied = tie(window_grad, *halos, *heads_cut, *mine_all, *layer_parts)
    window_grad, *halos = tied[:3]
    heads_cut, layer_parts = tied[3:5], tied[-4:]
    heads_sent = send_cut(heads_cut, last)
    from_left = shift(halos[1], "narrow", 1)
    from_right = shift(halos[0], "narrow", -1)
    mine = arrange(tied[5:-4], groups[-1], 0).reshape((-1,) + mine.shape[1:])
    for bits in reversed(groups[:-1]):
        mine = arrange(exchange(mine, bits), bits, 0).reshape((-1,) + mine.shape[1:])
    mine, *heads_sent = tie(mine, *heads_sent)
    mine_sent = exchange(mine, last)[1]
    heads_part = add_low(heads_cut[0], *heads_sent)
    for bits in groups[:-1]:
        parts = cut(heads_part, "wide", bits)
        heads_part = add_low(parts[0], *send_cut(parts, bits))
    heads_cut = cut(heads_part, "wide", groups[-1])
    window_grad, from_left, from_right, *heads_cut = tie(
        window_grad, from_left, from_right, *heads_cut
    )
    heads_sent = send_cut(heads_cut, groups[-1])
    y_high, core_high = bit_of("narrow", 2), bit_of("narrow", 1)
    layer_near = join(layer_parts[0], layer_parts[1], core_high, 1)
    layer_far = join(layer_parts[2], layer_parts[3], core_high, 1)
    layer_out = join(layer_near, layer_far, y_high, 1).reshape(micro, row_count, width)
    head_bias_parts = [
        jnp.concatenate([s[0, 2 * cols : 3 * cols], s[0, cols : 2 * cols]])
        for s in [*sums0, *sums1, *sums2, *sums3]
    ]

    token_grad, first_sums = rows_call(
        first_back_kernel, "first_back", place,
        [window_grad, from_left, from_right, middle_grad, tokens, vectors],
        [per_micro((window, width)), per_micro((halo, width)), per_micro((halo, width)), part_spec,
         own_spec, vec_spec],
        [low_rows, sum_rows], [part_spec, vec_spec],
    )
    outer = jnp.stack([mixer_scale, feed_scale] + [jnp.ones_like(out_bias)] * 6)
    sums = (back_sums + first_sums) * outer
    group_sums = jnp.stack(
        [jnp.concatenate([head_bias_parts[r], up_bias_parts[r][0]]) for r in range(narrow_size)]
    )
    group_sums = jnp.stack([group_sums[r ^ narrow_at] for r in range(narrow_size)])
    packed = jnp.concatenate([sums.reshape(-1), group_sums.reshape(-1)]).reshape(-1, 128)
    packed, mine_sent, *heads_sent = tie(packed, mine_sent, *heads_sent)
    heads_part = add_low(heads_cut[0], *heads_sent)
    packed, heads_part, mine_sent = tie(packed, heads_part, mine_sent)
    heads_all = exchange(heads_part, groups[-1])
    packed = reduce_narrow(packed)
    feed_total = arrange([mine, mine_sent], last, 0).reshape(width, -1)
    packed, *heads_all = tie(packed, *heads_all)
    packed = reduce_wide(packed)
    heads_total = arrange(heads_all, groups[-1], 0).reshape((-1,) + heads_part.shape[1:])
    for bits in reversed(groups[:-1]):
        heads_total = arrange(exchange(heads_total, bits), bits, 0)
        heads_total = heads_total.reshape((-1,) + heads_part.shape[1:])
    heads_total = spread_last(heads_total)
    packed = packed.reshape(-1)
    sums = packed[: 8 * width].reshape(8, width)
    group_sums = packed[8 * width :].reshape(narrow_size, -1)
    mine = lax.dynamic_slice_in_dim(group_sums, narrow_at, 1, 0)[0]

    heads_grad = jnp.stack(
        [heads_total[:, 2 * cols : 3 * cols], heads_total[:, :cols], heads_total[:, cols : 2 * cols]],
        axis=1,
    ).astype(f32)
    out_grad = heads_total[:, 3 * cols :].T.astype(f32)
    return (
        layer_out, token_grad, heads_grad, mine[: 2 * cols].reshape(2, cols), out_grad, sums[0],
        feed_total[:, :hidden].astype(f32), mine[2 * cols :],
        feed_total[:, hidden:].T.astype(f32), sums[1], sums[2],
        sums[3], sums[4], sums[5], sums[6], sums[7],
    )


def solution(mesh):
    return jax.shard_map(
        body,
        mesh=mesh,
        in_specs=(
            P(None, "wide", None),
            P(None, "wide", None),
            P("wide", None, "narrow"),
            P(None, "narrow"),
            P("narrow", "wide"),
            P(),
            P("wide", "narrow"),
            P("narrow"),
            P("narrow", "wide"),
            P(),
            P(),
            P(),
            P(),
            P(),
            P(),
            P(),
            P(None, "wide", None),
        ),
        out_specs=(
            P(None, "wide", None),
            P(None, ("wide", "narrow"), None),
            P(None, None, "narrow"),
            P(None, "narrow"),
            P("narrow", None),
            P(),
            P(None, "narrow"),
            P("narrow"),
            P("narrow", None),
            P(),
            P(),
            P(),
            P(),
            P(),
            P(),
            P(),
        ),
        check_vma=False,
    )
```

```python
import math
from functools import partial

import jax
import jax.numpy as jnp
from jax import lax
from jax.experimental import pallas as pl
from jax.experimental.pallas import tpu as pltpu
from jax.sharding import PartitionSpec as P

HEAD_DIM = 64
MOST = 196
epsilon = 1e-06
bf16 = jnp.bfloat16
f32 = jnp.float32
LOG2E = math.log2(math.e)
VMEM_LIMIT = 60 * 1024 * 1024
FEED_CHUNKS = 2
QUERIES = 160


def round_up(value, step):
    return -(-value // step) * step


def nt(left, right):
    return lax.dot_general(left, right, (((1,), (1,)), ((), ())), preferred_element_type=f32)


def tn(left, right):
    return lax.dot_general(left, right, (((0,), (0,)), ((), ())), preferred_element_type=f32)


def nn(left, right):
    return jnp.dot(left, right, preferred_element_type=f32)


def query_chunk(own):
    return QUERIES if own % QUERIES == 0 else own


def key_span(own, win):
    return min(win, query_chunk(own) + 2 * round_up(MOST - 1, 16))


def key_start(off, at, own, win):
    first = jnp.clip(off + at - round_up(MOST - 1, 16), 0, win - key_span(own, win))
    return pl.multiple_of(first, 16)


def params():
    return pltpu.CompilerParams(
        dimension_semantics=("arbitrary",), vmem_limit_bytes=VMEM_LIMIT
    )


def cost(flops, transcendentals, moved):
    return pl.CostEstimate(flops=1024, transcendentals=0, bytes_accessed=1024)


def full(shape):
    return pl.BlockSpec(shape, lambda *a: (0,) * len(shape))


def per_micro(shape):
    return pl.BlockSpec((1,) + shape, lambda m, *a: (m,) + (0,) * len(shape))


def stack_heads(rows, heads):
    lane = lax.broadcasted_iota(jnp.int32, rows.shape, 1) // HEAD_DIM
    zero = jnp.zeros_like(rows)
    return jnp.concatenate([jnp.where(lane == h, rows, zero) for h in range(heads)], axis=0)


def unstack_heads(stacked, heads):
    rows = stacked.shape[0] // heads
    lane = lax.broadcasted_iota(jnp.int32, (rows, stacked.shape[1]), 1) // HEAD_DIM
    out = stacked[:rows]
    for h in range(1, heads):
        out = jnp.where(lane == h, stacked[h * rows : (h + 1) * rows], out)
    return out


def attend_kernel(own, heads, count, first, off_ref, *refs):
    x_ref, b_ref, bnd_ref = refs[:3]
    w_refs = refs[3 : 3 + count]
    rest = refs[3 + count + (0 if first else 1) :]
    mixed_ref = rest[0]
    off = pl.multiple_of(off_ref[0], 16)
    win = x_ref.shape[1]
    cols = heads * HEAD_DIM
    xw = x_ref[0]
    xo = x_ref[0, pl.ds(off, own), :]
    size, span = query_chunk(own), key_span(own, win)
    place = lax.broadcasted_iota(jnp.int32, (span, heads * size), 0)
    mixed = None if first else refs[3 + count][0]
    for i in range(count):
        q_ref, k_ref, v_ref, o_ref, l_ref = rest[1 + 5 * i : 6 + 5 * i]
        w = w_refs[i]
        both = nn(xw, w[:, : 2 * cols])
        k = both[:, :cols].astype(bf16)
        v = (both[:, cols:] + b_ref[i, 1:2]).astype(bf16)
        q = (nn(xo, w[:, 2 * cols : 3 * cols]) + b_ref[i, 0:1]).astype(bf16)
        q_ref[0] = q
        k_ref[0] = k
        v_ref[0] = v
        parts = []
        for c in range(own // size):
            key_at = key_start(off, c * size, own, win)
            kc, vc = k_ref[0, pl.ds(key_at, span), :], v_ref[0, pl.ds(key_at, span), :]
            qs = stack_heads(q[c * size : (c + 1) * size], heads)
            keep = (place >= bnd_ref[0, c, 0:1] - key_at) & (place < bnd_ref[0, c, 1:2] - key_at)
            scores = nt(kc, qs) * (HEAD_DIM**-0.5 * LOG2E)
            scores = jnp.where(keep, scores, -1e30)
            top = jnp.max(scores, axis=0, keepdims=True)
            weights = jnp.exp2(scores - top)
            total = jnp.sum(weights, axis=0, keepdims=True)
            out = tn(vc, weights.astype(bf16)) * (1.0 / total)
            parts.append(unstack_heads(out.T, heads).astype(bf16))
            l_ref[0, c] = top + jnp.log2(total)
        out = jnp.concatenate(parts, axis=0)
        o_ref[0] = out
        part = nt(out, w[:, 3 * cols :])
        mixed = part if mixed is None else mixed + part
    mixed_ref[0] = mixed


def attend(off, x_win, pieces, bias, bounds, own, mixed):
    micro, win, width = x_win.shape
    cols = pieces[0].shape[1] // 4
    heads = cols // HEAD_DIM
    size = query_chunk(own)
    stacked = heads * size
    count = len(pieces)
    first = mixed is None
    shapes = [jax.ShapeDtypeStruct((micro, own, width), f32)]
    specs = [per_micro((own, width))]
    for _ in pieces:
        for rows in (own, win, win, own):
            shapes.append(jax.ShapeDtypeStruct((micro, rows, cols), bf16))
            specs.append(per_micro((rows, cols)))
        shapes.append(jax.ShapeDtypeStruct((micro, own // size, 1, stacked), f32))
        specs.append(per_micro((own // size, 1, stacked)))
    args = [x_win, bias, bounds] + list(pieces)
    in_specs = [per_micro((win, width)), full(bias.shape), per_micro((own // size, 2, stacked))]
    in_specs += [full((width, 4 * cols))] * count
    if not first:
        args.append(mixed)
        in_specs.append(per_micro((own, width)))
    result = pl.pallas_call(
        partial(attend_kernel, own, heads, count, first),
        grid_spec=pltpu.PrefetchScalarGridSpec(
            num_scalar_prefetch=1, grid=(micro,), in_specs=in_specs, out_specs=specs
        ),
        out_shape=shapes,
        compiler_params=params(),
        cost_estimate=cost(
            count * micro * 2 * (win * width * cols * 3 + 8 * stacked * win * HEAD_DIM),
            count * micro * stacked * win,
            micro * win * width * 2 + count * 4 * width * cols * 2,
        ),
        name="attend",
    )(off, *args)
    return result[0], [tuple(result[1 + 5 * i : 6 + 5 * i]) for i in range(count)]


def attend_back_kernel(own, heads, count, first, halo, off_ref, *refs):
    x_ref, mg_ref, bnd_ref = refs[:3]
    w_refs = refs[3 : 3 + count]
    saved = refs[3 + count : 3 + 6 * count]
    at = 3 + 6 * count
    in_ref = None if first else refs[at]
    rest = refs[at + (0 if first else 1) :]
    dn_ref = rest[0]
    halo_refs = rest[1 + 2 * count : 1 + 2 * count + (2 if halo else 0)]
    *acc_refs, dkv_ref = rest[1 + 2 * count + len(halo_refs) :]
    off = pl.multiple_of(off_ref[0], 16)
    win = x_ref.shape[1]
    cols = heads * HEAD_DIM
    scale = HEAD_DIM**-0.5
    step = pl.program_id(0)
    mg = mg_ref[0]
    xt = x_ref[0].T
    xot = x_ref[0, pl.ds(off, own), :].T
    mgt = mg.T
    size, span = query_chunk(own), key_span(own, win)
    place = lax.broadcasted_iota(jnp.int32, (span, heads * size), 0)
    dn = None if first else in_ref[0]
    dn_own = None
    for i in range(count):
        w = w_refs[i]
        q_ref, k_ref, v_ref, o_ref, l_ref = saved[5 * i : 5 * i + 5]
        dw_ref, db_ref = rest[1 + 2 * i : 3 + 2 * i]
        acc_ref = acc_refs[i]
        o = o_ref[0]
        g = nn(mg, w[:, 3 * cols :]).astype(bf16)
        dkv_ref[...] = jnp.zeros_like(dkv_ref)
        parts = []
        for c in range(own // size):
            key_at = key_start(off, c * size, own, win)
            keys = pl.ds(key_at, span)
            kc, vc = k_ref[0, keys, :], v_ref[0, keys, :]
            qs = stack_heads(q_ref[0, c * size : (c + 1) * size, :], heads)
            gs = stack_heads(g[c * size : (c + 1) * size], heads)
            keep = (place >= bnd_ref[0, c, 0:1] - key_at) & (place < bnd_ref[0, c, 1:2] - key_at)
            scores = nt(kc, qs) * (scale * LOG2E) - l_ref[0, c]
            weights = jnp.exp2(jnp.where(keep, scores, -1e30))
            weighed = weights * nt(vc, gs)
            delta = jnp.sum(weighed, axis=0, keepdims=True)
            slope = (weighed - weights * delta).astype(bf16)
            parts.append((unstack_heads(tn(kc, slope).T, heads) * scale).astype(bf16))
            dkv_ref[0, keys, :] += nn(slope, qs)
            dkv_ref[1, keys, :] += nn(weights.astype(bf16), gs)
        dq = jnp.concatenate(parts, axis=0)
        dkv = jnp.concatenate([dkv_ref[0] * scale, dkv_ref[1]], axis=1).astype(bf16)
        part = nt(dkv, w[:, : 2 * cols])
        dn = part if dn is None else dn + part
        part = nt(dq, w[:, 2 * cols : 3 * cols])
        dn_own = part if dn_own is None else dn_own + part
        left = nn(xt, dkv)
        right = jnp.concatenate([nn(xot, dq), nn(mgt, o)], axis=1)
        sums = jnp.concatenate(
            [
                jnp.sum(dkv.astype(f32), axis=0, keepdims=True),
                jnp.sum(jnp.concatenate([dq, dq], axis=1).astype(f32), axis=0, keepdims=True),
            ],
            axis=1,
        )

        @pl.when(step == 0)
        def _():
            acc_ref[:, : 2 * cols] = left
            acc_ref[:, 2 * cols :] = right
            db_ref[...] = sums

        @pl.when(step > 0)
        def _():
            acc_ref[:, : 2 * cols] += left
            acc_ref[:, 2 * cols :] += right
            db_ref[...] += sums

        @pl.when(step == pl.num_programs(0) - 1)
        def _():
            dw_ref[...] = acc_ref[...].astype(bf16)

    dn_ref[0] = dn
    dn_ref[0, pl.ds(off, own), :] += dn_own
    if halo:
        before = pl.multiple_of(jnp.maximum(off - halo, 0), 16)
        after = pl.multiple_of(jnp.minimum(off + own, win - halo), 16)
        halo_refs[0][0] = dn_ref[0, pl.ds(before, halo), :].astype(bf16)
        halo_refs[1][0] = dn_ref[0, pl.ds(after, halo), :].astype(bf16)


def attend_back(off, x_win, mixed_grad, pieces, saved, bounds, grad_in, halo):
    micro, win, width = x_win.shape
    own = mixed_grad.shape[1]
    cols = pieces[0].shape[1] // 4
    heads = cols // HEAD_DIM
    size = query_chunk(own)
    stacked = heads * size
    count = len(pieces)
    first = grad_in is None
    args = [x_win, mixed_grad, bounds] + list(pieces)
    in_specs = [per_micro((win, width)), per_micro((own, width)), per_micro((own // size, 2, stacked))]
    in_specs += [full((width, 4 * cols))] * count
    for one in saved:
        args += list(one)
        in_specs += [per_micro((rows, cols)) for rows in (own, win, win, own)]
        in_specs.append(per_micro((own // size, 1, stacked)))
    if not first:
        args.append(grad_in)
        in_specs.append(per_micro((win, width)))
    shapes = [jax.ShapeDtypeStruct((micro, win, width), f32)]
    specs = [per_micro((win, width))]
    for _ in pieces:
        shapes += [
            jax.ShapeDtypeStruct((width, 4 * cols), bf16),
            jax.ShapeDtypeStruct((1, 4 * cols), f32),
        ]
        specs += [full((width, 4 * cols)), full((1, 4 * cols))]
    for _ in range(2 if halo else 0):
        shapes.append(jax.ShapeDtypeStruct((micro, halo, width), bf16))
        specs.append(per_micro((halo, width)))
    result = pl.pallas_call(
        partial(attend_back_kernel, own, heads, count, first, halo),
        grid_spec=pltpu.PrefetchScalarGridSpec(
            num_scalar_prefetch=1,
            grid=(micro,),
            in_specs=in_specs,
            out_specs=specs,
            scratch_shapes=[pltpu.VMEM((width, 4 * cols), f32)] * count
            + [pltpu.VMEM((2, win, cols), f32)],
        ),
        out_shape=shapes,
        compiler_params=params(),
        cost_estimate=cost(
            count * micro * (40 * stacked * win * HEAD_DIM + 12 * win * width * cols),
            count * micro * stacked * win,
            micro * (10 * win) * width + count * 4 * width * cols * 4,
        ),
        name="attend_back",
    )(off, *args)
    return result[0], result[1 : 1 + 2 * count : 2], result[2 : 2 + 2 * count : 2], result[1 + 2 * count :]


def feed_kernel(chunks, count, first, *refs):
    x_ref, g_ref = refs[:2]
    w_refs = refs[2 : 2 + count]
    b_refs = refs[2 + count : 2 + 2 * count]
    at = 2 + 2 * count
    if not first:
        fi_ref, ni_ref = refs[at : at + 2]
        at = at + 2
    f_ref, n_ref = refs[at : at + 2]
    outs = refs[at + 2 : at + 2 + 2 * count]
    act_ref, ug_ref, xt_ref, gt_ref = refs[at + 2 + 2 * count :]
    rows = x_ref.shape[0]
    step = rows // chunks
    xt_ref[...] = x_ref[...].T
    gt_ref[...] = g_ref[...].T
    for i in range(count):
        w_ref, b_ref = w_refs[i], b_refs[i]
        dw_ref, db_ref = outs[2 * i : 2 * i + 2]
        hidden = b_ref.shape[1]
        total = jnp.zeros((1, hidden), f32)
        for c in range(chunks):
            rows_at = pl.ds(c * step, step)
            upper = nn(x_ref[rows_at, :], w_ref[:, :hidden]) + b_ref[...]
            phi = 0.5 + 0.5 * lax.erf(upper * math.sqrt(0.5))
            active = (upper * phi).astype(bf16)
            bell = jnp.exp2(upper * upper * (-0.5 * LOG2E)) * (1.0 / math.sqrt(2.0 * math.pi))
            slope = phi + upper * bell
            grad = (nn(g_ref[rows_at, :], w_ref[:, hidden:]) * slope).astype(bf16)
            act_ref[rows_at, :] = active
            ug_ref[rows_at, :] = grad
            total = total + jnp.sum(grad.astype(f32), axis=0, keepdims=True)
            feed = nt(active, w_ref[:, hidden:])
            back = nt(grad, w_ref[:, :hidden])
            if i > 0:
                feed = feed + f_ref[rows_at, :]
                back = back + n_ref[rows_at, :]
            elif not first:
                feed = feed + fi_ref[rows_at, :]
                back = back + ni_ref[rows_at, :]
            f_ref[rows_at, :] = feed
            n_ref[rows_at, :] = back
        db_ref[...] = total
        dw_ref[:, :hidden] = nn(xt_ref[...], ug_ref[...]).astype(bf16)
        dw_ref[:, hidden:] = nn(gt_ref[...], act_ref[...]).astype(bf16)


def feed_part(x2, grad, pieces, biases, before):
    rows, width = x2.shape
    hidden = biases[0].shape[1]
    count = len(pieces)
    first = before is None
    args = [x2, grad] + list(pieces) + list(biases)
    aliases = {}
    if not first:
        aliases = {len(args): 0, len(args) + 1: 1}
        args += list(before)
    whole = pl.BlockSpec(memory_space=pltpu.VMEM)
    shapes = [jax.ShapeDtypeStruct((rows, width), f32)] * 2
    for _ in pieces:
        shapes += [
            jax.ShapeDtypeStruct((width, 2 * hidden), bf16),
            jax.ShapeDtypeStruct((1, hidden), f32),
        ]
    result = pl.pallas_call(
        partial(feed_kernel, FEED_CHUNKS, count, first),
        in_specs=[whole] * len(args),
        out_specs=[whole] * len(shapes),
        out_shape=shapes,
        scratch_shapes=[
            pltpu.VMEM((rows, hidden), bf16),
            pltpu.VMEM((rows, hidden), bf16),
            pltpu.VMEM((width, rows), bf16),
            pltpu.VMEM((width, rows), bf16),
        ],
        input_output_aliases=aliases,
        compiler_params=pltpu.CompilerParams(vmem_limit_bytes=VMEM_LIMIT),
        cost_estimate=cost(
            count * 12 * rows * width * hidden,
            count * 2 * rows * hidden,
            16 * rows * width + count * 8 * width * hidden,
        ),
        name="feed_part",
    )(*args)
    return tuple(result[:2]), list(result[2::2]), list(result[3::2])


def norm_parts(values_in):
    center = jnp.mean(values_in, axis=-1, keepdims=True)
    shifted = values_in - center
    inverse = lax.rsqrt(jnp.mean(shifted * shifted, axis=-1, keepdims=True) + epsilon)
    return (shifted * inverse, inverse)


def norm_back(grad_in, unit_rows, inverse, gain_row):
    scaled = grad_in * gain_row
    return inverse * (
        scaled
        - jnp.mean(scaled, axis=-1, keepdims=True)
        - unit_rows * jnp.mean(scaled * unit_rows, axis=-1, keepdims=True)
    )


VECTORS = (
    "out_bias", "down_bias", "first_gain", "first_shift", "second_gain", "second_shift",
    "mixer_scale", "feed_scale",
)


def row(vec_ref, name):
    at = VECTORS.index(name)
    return vec_ref[at : at + 1]


def own_rows(shape):
    return pl.BlockSpec((1,) + shape, lambda m, place: (m, place[0]) + (0,) * (len(shape) - 1))


def rows_call(kernel, name, place, args, specs, shapes, out_specs):
    micro = args[0].shape[0]
    return pl.pallas_call(
        kernel,
        grid_spec=pltpu.PrefetchScalarGridSpec(
            num_scalar_prefetch=1, grid=(micro,), in_specs=specs, out_specs=out_specs
        ),
        out_shape=shapes,
        compiler_params=params(),
        cost_estimate=cost(0, 0, 0),
        name=name,
    )(place, *args)


def first_norm_kernel(place_ref, x_ref, c_ref, vec_ref, n_ref, g_ref):
    start = pl.multiple_of(place_ref[1], 16)
    win = n_ref.shape[1]
    unit = norm_parts(x_ref[0, pl.ds(start, win), :].astype(f32))[0]
    n_ref[0] = (unit * row(vec_ref, "first_gain") + row(vec_ref, "first_shift")).astype(bf16)
    g_ref[0] = (row(vec_ref, "feed_scale") * c_ref[0].astype(f32)).astype(bf16)


def second_norm_kernel(place_ref, mixed_ref, x_ref, vec_ref, m_ref, n_ref):
    branch = mixed_ref[0] + row(vec_ref, "out_bias")
    middle = x_ref[0].astype(f32) + row(vec_ref, "mixer_scale") * branch
    m_ref[0] = middle
    unit = norm_parts(middle)[0]
    n_ref[0] = (unit * row(vec_ref, "second_gain") + row(vec_ref, "second_shift")).astype(bf16)


def column_sums(sum_ref, rows_in):
    total = jnp.concatenate([jnp.sum(r, axis=0, keepdims=True) for r in rows_in], axis=0)

    @pl.when(pl.program_id(0) == 0)
    def _():
        sum_ref[...] = total

    @pl.when(pl.program_id(0) > 0)
    def _():
        sum_ref[...] += total


def second_back_kernel(
    place_ref, feed_ref, back_ref, m_ref, mixed_ref, c_ref, vec_ref, l_ref, mg_ref, low_ref, sum_ref
):
    middle, back, grad = m_ref[0], back_ref[0], c_ref[0].astype(f32)
    feed_scale = row(vec_ref, "feed_scale")
    branch = feed_ref[0] + row(vec_ref, "down_bias")
    l_ref[0] = (middle + feed_scale * branch).astype(bf16)
    unit, inverse = norm_parts(middle)
    middle_grad = grad + norm_back(back, unit, inverse, row(vec_ref, "second_gain"))
    mg_ref[0] = middle_grad
    low_ref[0] = (row(vec_ref, "mixer_scale") * middle_grad).astype(bf16)
    mixer = mixed_ref[0] + row(vec_ref, "out_bias")
    zero = jnp.zeros_like(grad[:8])
    column_sums(
        sum_ref,
        [middle_grad, grad, zero, zero, back * unit, back, middle_grad * mixer, grad * branch],
    )


def first_back_kernel(
    place_ref, win_ref, left_ref, right_ref, mg_ref, x_ref, vec_ref, t_ref, sum_ref
):
    own, halo = mg_ref.shape[1], left_ref.shape[1]
    off = pl.multiple_of(place_ref[2], 16)
    gap = jnp.zeros((own - halo, left_ref.shape[2]), f32)
    grad = win_ref[0, pl.ds(off, own), :]
    grad = grad + jnp.concatenate([left_ref[0].astype(f32), gap], axis=0)
    grad = grad + jnp.concatenate([gap, right_ref[0].astype(f32)], axis=0)
    unit, inverse = norm_parts(x_ref[0].astype(f32))
    t_ref[0] = (
        mg_ref[0] + norm_back(grad, unit, inverse, row(vec_ref, "first_gain"))
    ).astype(bf16)
    zero = jnp.zeros_like(grad[:8])
    column_sums(sum_ref, [zero, zero, grad * unit, grad, zero, zero, zero, zero])


def swap(values_in, axis, bit):
    size = lax.axis_size(axis)
    return lax.ppermute(values_in, axis, [(i, i ^ bit) for i in range(size)])


def shift(values_in, axis, step):
    size = lax.axis_size(axis)
    pairs = [(i, i + step) for i in range(size) if 0 <= i + step < size]
    return lax.ppermute(values_in, axis, pairs)


def wide_bits(size):
    bits = []
    bit = size // 2
    while bit:
        bits.append(bit)
        bit //= 2
    return bits


def bit_of(axis, bit):
    return (lax.axis_index(axis) & bit) != 0


def join(mine, other, is_high, axis):
    low = jnp.where(is_high, other, mine)
    high = jnp.where(is_high, mine, other)
    return jnp.stack([low, high], axis=axis)


def tie(*values_in):
    return lax.optimization_barrier(values_in)


def far_groups():
    bits = wide_bits(lax.axis_size("wide"))[:-1]
    return [bits[i : i + 2] for i in range(0, len(bits), 2)]


def offsets(bits):
    return [
        sum(bit for i, bit in enumerate(reversed(bits)) if (k >> i) & 1)
        for k in range(2 ** len(bits))
    ]


def exchange(values_in, bits):
    return [values_in] + [swap(values_in, "wide", o) for o in offsets(bits)[1:]]


def arrange(parts, bits, axis):
    if not bits:
        return jnp.expand_dims(parts[0], axis)
    half = len(parts) // 2
    low = arrange(parts[:half], bits[1:], axis)
    high = arrange(parts[half:], bits[1:], axis)
    is_high = bit_of("wide", bits[0])
    return jnp.concatenate(
        [jnp.where(is_high, high, low), jnp.where(is_high, low, high)], axis=axis
    )


def arrange_blocks(parts, bits):
    return arrange(parts, bits, 1).reshape((-1,) + parts[0].shape[1:])


def last_bit():
    return wide_bits(lax.axis_size("wide"))[-1]


def gather_narrow(piece):
    far = swap(piece, "narrow", 2)
    return [piece, swap(piece, "narrow", 1), far, swap(far, "narrow", 1)]


def add_low(*parts):
    total = parts[0].astype(f32)
    for part in parts[1:]:
        total = total + part.astype(f32)
    return total.astype(bf16)


def cut(values_in, axis, bits):
    count = 2 ** len(bits)
    size = values_in.shape[0] // count
    at = lax.axis_index(axis)
    places = []
    for o in offsets(bits):
        other = at ^ o
        place = 0
        for bit in bits:
            place = 2 * place + ((other & bit) != 0).astype(jnp.int32)
        places.append(place)
    return [lax.dynamic_slice_in_dim(values_in, p * size, size, 0) for p in places]


def send_cut(parts, bits):
    return [swap(part, "wide", o) for part, o in zip(parts[1:], offsets(bits)[1:])]


def spread_last(part):
    bits = [last_bit()]
    return arrange(exchange(part, bits), bits, 0).reshape((-1,) + part.shape[1:])


def tree_sum(parts):
    while len(parts) > 1:
        parts = [parts[i] + parts[i + 1] for i in range(0, len(parts), 2)]
    return parts[0]


def reduce_wide(values_in):
    for bits in far_groups() + [[last_bit()]]:
        values_in = tree_sum(exchange(values_in, bits))
    return values_in


def reduce_narrow(values_in):
    return tree_sum([values_in] + [swap(values_in, "narrow", o) for o in (1, 2, 3)])


def body(
    tokens, image_lengths, heads_weight, heads_bias, out_weight, out_bias, up_weight, up_bias,
    down_weight, down_bias, first_gain, first_shift, second_gain, second_shift, mixer_scale,
    feed_scale, cotangent,
):
    micro, row_count, width = tokens.shape
    narrow_size = lax.axis_size("narrow")
    narrow_at = lax.axis_index("narrow")
    own = row_count // narrow_size
    cols = heads_weight.shape[2]
    heads = cols // HEAD_DIM
    rows = micro * own
    halo = round_up(MOST - 1, 16)
    window = min(row_count, round_up(own + 2 * halo, 128))
    lead = round_up((window - own) // 2, 16)
    start = jnp.clip(narrow_at * own - lead, 0, row_count - window)
    off = narrow_at * own - start
    offset = off.reshape(1).astype(jnp.int32)

    hidden = up_weight.shape[1]
    groups = far_groups()

    bias_pieces = gather_narrow(
        jnp.concatenate([heads_bias.reshape(-1), up_bias]).reshape(1, -1)
    )
    qv_biases = [heads_bias[None]]
    qv_biases += [b[:, : 2 * cols].reshape(1, 2, cols) for b in bias_pieces[1:]]
    up_biases = [up_bias.reshape(1, hidden)] + [b[:, 2 * cols :] for b in bias_pieces[1:]]
    heads_blocks = jnp.concatenate(
        [heads_weight[:, 1], heads_weight[:, 2], heads_weight[:, 0], out_weight.T], axis=1
    )[None]
    for bits in groups:
        heads_blocks = arrange_blocks(exchange(heads_blocks, bits), bits)
    feed_blocks = jnp.concatenate([up_weight, down_weight.T], axis=1)[None]
    heads_blocks, feed_blocks, *biases = tie(heads_blocks, feed_blocks, *qv_biases, *up_biases)
    qv_biases, up_biases = biases[:narrow_size], biases[narrow_size:]
    for bits in groups[:-1]:
        feed_blocks = arrange_blocks(exchange(feed_blocks, bits), bits)
    feed_parts = exchange(feed_blocks, groups[-1])
    last = [last_bit()]
    heads_all = arrange_blocks(exchange(heads_blocks, last), last)
    heads_own = heads_all.reshape(width, -1)

    ends = jnp.cumsum(image_lengths[:, 0], axis=1)
    places = narrow_at * own + jnp.arange(own, dtype=jnp.int32)
    passed = ends[:, :, None] <= places[None, None, :]
    first_key = jnp.max(jnp.where(passed, ends[:, :, None], 0), axis=1) - start
    last_key = jnp.min(jnp.where(passed, row_count, ends[:, :, None]), axis=1) - start
    bounds = jnp.stack([first_key, last_key], axis=1).astype(jnp.int32)
    size = query_chunk(own)
    bounds = bounds.reshape(micro, 2, own // size, size).transpose(0, 2, 1, 3)
    bounds = jnp.tile(bounds, (1, 1, 1, heads))

    place = jnp.stack([narrow_at, start, off]).astype(jnp.int32)
    vectors = jnp.stack(
        [out_bias, down_bias, first_gain, first_shift, second_gain, second_shift, mixer_scale,
         feed_scale]
    )
    own_spec, part_spec, vec_spec = own_rows((own, width)), per_micro((own, width)), full((8, width))
    low_rows = jax.ShapeDtypeStruct((micro, own, width), bf16)
    high_rows = jax.ShapeDtypeStruct((micro, own, width), f32)
    sum_rows = jax.ShapeDtypeStruct((8, width), f32)
    window_normed, feed_grad = rows_call(
        first_norm_kernel, "first_norm", place, [tokens, cotangent, vectors],
        [per_micro((row_count, width)), own_spec, vec_spec],
        [jax.ShapeDtypeStruct((micro, window, width), bf16), low_rows],
        [per_micro((window, width)), part_spec],
    )
    feed_grad = feed_grad.reshape(rows, width)

    def halves(blocks):
        half = blocks.shape[0] // 2
        return blocks[:half], blocks[half:]

    def attend_on(piece, at, before):
        return attend(offset, window_normed, [piece], qv_biases[at], bounds, own, before)

    heads_low, heads_high = halves(heads_all)
    window_normed, heads_low = tie(window_normed, heads_low)
    heads_near = swap(heads_own, "narrow", 1)
    far_low = swap(heads_low, "narrow", 2)
    mixed, saved0 = attend_on(heads_own, 0, None)
    mixed, far_low, *feed_parts = tie(mixed, far_low, *feed_parts)
    feed_low, feed_high = halves(arrange_blocks(feed_parts, groups[-1]))
    mixed, feed_low, feed_high, heads_high = tie(mixed, feed_low, feed_high, heads_high)
    far_high = swap(heads_high, "narrow", 2)
    low_other = exchange(feed_low, last)[1]
    mixed, saved1 = attend_on(heads_near, 1, mixed)
    mixed, far_high, low_other = tie(mixed, far_high, low_other)
    heads_far = jnp.concatenate([far_low, far_high], axis=0).reshape(width, -1)
    mixed, heads_far, feed_low, feed_high = tie(mixed, heads_far, feed_low, feed_high)
    heads_cross = swap(heads_far, "narrow", 1)
    high_other = exchange(feed_high, last)[1]
    feed_far_low = swap(feed_low, "narrow", 2)
    mixed, saved2 = attend_on(heads_far, 2, mixed)
    mixed, high_other, feed_far_low = tie(mixed, high_other, feed_far_low)

    def whole_feed(low, high, low_sent, high_sent):
        mine = jnp.concatenate([low, high], axis=0)
        other = jnp.concatenate([low_sent, high_sent], axis=0)
        return arrange_blocks([mine, other], last).reshape(width, -1)

    feed_own = whole_feed(feed_low, feed_high, low_other, high_other)
    mixed, feed_own, feed_high = tie(mixed, feed_own, feed_high)
    feed_near = swap(feed_own, "narrow", 1)
    feed_far_high = swap(feed_high, "narrow", 2)
    mixed, saved3 = attend_on(heads_cross, 3, mixed)
    mixed, feed_far_high = tie(mixed, feed_far_high)
    middle, second_normed = rows_call(
        second_norm_kernel, "second_norm", place, [mixed, tokens, vectors],
        [part_spec, own_spec, vec_spec], [high_rows, low_rows], [part_spec, part_spec],
    )
    second_normed = second_normed.reshape(rows, width)

    def feed_on(pieces, biases, before):
        return feed_part(second_normed, feed_grad, pieces, biases, before)

    second_normed, feed_far_low = tie(second_normed, feed_far_low)
    far_low_other = exchange(feed_far_low, last)[1]
    sums, (part0,), bias0 = feed_on([feed_own], up_biases[:1], None)
    *sums, far_low_other, feed_far_high = tie(*sums, far_low_other, feed_far_high)
    far_high_other = exchange(feed_far_high, last)[1]
    sums, (part1,), bias1 = feed_on([feed_near], up_biases[1:2], sums)
    *sums, far_high_other = tie(*sums, far_high_other)
    feed_far = whole_feed(feed_far_low, feed_far_high, far_low_other, far_high_other)
    *sums, feed_far, part1 = tie(*sums, feed_far, part1)
    feed_cross = swap(feed_far, "narrow", 1)
    given = swap(part1, "narrow", 1)
    sums, (part2,), bias2 = feed_on([feed_far], up_biases[2:3], sums)
    *sums, given = tie(*sums, given)
    near_keep, near_give = cut(add_low(part0, given), "wide", last)
    up_give, down_give = near_give[:, :hidden], near_give[:, hidden:]
    *sums, near_keep, up_give, down_give = tie(*sums, near_keep, up_give, down_give)
    up_sent = swap(up_give, "wide", last[0])
    sums, (part3,), bias3 = feed_on([feed_cross], up_biases[3:], sums)
    feed, second_normed_grad, up_sent, part3, down_give = tie(*sums, up_sent, part3, down_give)
    down_sent = swap(down_give, "wide", last[0])
    given = swap(part3, "narrow", 1)
    up_bias_parts = bias0 + bias1 + bias2 + bias3

    layer_own, middle_grad, mixed_grad, back_sums = rows_call(
        second_back_kernel, "second_back", place,
        [feed.reshape(micro, own, width), second_normed_grad.reshape(micro, own, width), middle,
         mixed, cotangent, vectors],
        [part_spec, part_spec, part_spec, part_spec, own_spec, vec_spec],
        [low_rows, high_rows, low_rows, sum_rows],
        [part_spec, part_spec, part_spec, vec_spec],
    )
    def back_on(pieces, saved, grad_in, halo):
        return attend_back(
            offset, window_normed, mixed_grad, pieces, saved, bounds, grad_in, halo
        )

    mixed_grad, down_sent, given = tie(mixed_grad, down_sent, given)
    near = add_low(near_keep, jnp.concatenate([up_sent, down_sent], axis=1))
    far_cut = cut(add_low(part2, given), "wide", last)
    mixed_grad, near, layer_own, *far_cut = tie(mixed_grad, near, layer_own, *far_cut)
    layer_far = swap(layer_own, "narrow", 2)
    far_sent = send_cut(far_cut, last)
    window_grad, (heads3,), sums3, _ = back_on([heads_cross], saved3, None, 0)
    given3 = swap(heads3, "narrow", 1)
    window_grad, layer_far, *far_sent = tie(window_grad, layer_far, *far_sent)
    far = add_low(far_cut[0], *far_sent)
    window_grad, far, layer_far = tie(window_grad, far, layer_far)
    layer_parts = [
        layer_own, swap(layer_own, "narrow", 1), layer_far, swap(layer_far, "narrow", 1)
    ]
    far_given = swap(far, "narrow", 2)
    window_grad, (heads2,), sums2, _ = back_on([heads_far], saved2, window_grad, 0)
    window_grad, far_given, given3, *layer_parts = tie(
        window_grad, far_given, given3, *layer_parts
    )
    mine = add_low(near, far_given)
    for bits in groups[:-1]:
        parts = cut(mine, "wide", bits)
        mine = add_low(parts[0], *send_cut(parts, bits))
    mine_cut = cut(mine, "wide", groups[-1])
    heads_sum = add_low(heads2, given3)
    window_grad, heads_sum, *mine_cut = tie(window_grad, heads_sum, *mine_cut)
    mine_sent = send_cut(mine_cut, groups[-1])
    heads_given = swap(heads_sum, "narrow", 2)
    window_grad, (heads1,), sums1, _ = back_on([heads_near], saved1, window_grad, 0)
    given1 = swap(heads1, "narrow", 1)
    window_grad, heads_given, *mine_sent = tie(window_grad, heads_given, *mine_sent)
    mine = add_low(mine_cut[0], *mine_sent)
    window_grad, mine = tie(window_grad, mine)
    mine_all = exchange(mine, groups[-1])
    window_grad, (heads0,), sums0, halos = back_on([heads_own], saved0, window_grad, halo)
    window_grad, *mine_all = tie(window_grad, *mine_all)
    heads_cut = cut(add_low(heads0, given1, heads_given), "wide", last)
    tied = tie(window_grad, *halos, *heads_cut, *mine_all, *layer_parts)
    window_grad, *halos = tied[:3]
    heads_cut, layer_parts = tied[3:5], tied[-4:]
    heads_sent = send_cut(heads_cut, last)
    from_left = shift(halos[1], "narrow", 1)
    from_right = shift(halos[0], "narrow", -1)
    mine = arrange(tied[5:-4], groups[-1], 0).reshape((-1,) + mine.shape[1:])
    for bits in reversed(groups[:-1]):
        mine = arrange(exchange(mine, bits), bits, 0).reshape((-1,) + mine.shape[1:])
    mine, *heads_sent = tie(mine, *heads_sent)
    mine_sent = exchange(mine, last)[1]
    heads_part = add_low(heads_cut[0], *heads_sent)
    for bits in groups[:-1]:
        parts = cut(heads_part, "wide", bits)
        heads_part = add_low(parts[0], *send_cut(parts, bits))
    heads_cut = cut(heads_part, "wide", groups[-1])
    window_grad, from_left, from_right, *heads_cut = tie(
        window_grad, from_left, from_right, *heads_cut
    )
    heads_sent = send_cut(heads_cut, groups[-1])
    y_high, core_high = bit_of("narrow", 2), bit_of("narrow", 1)
    layer_near = join(layer_parts[0], layer_parts[1], core_high, 1)
    layer_far = join(layer_parts[2], layer_parts[3], core_high, 1)
    layer_out = join(layer_near, layer_far, y_high, 1).reshape(micro, row_count, width)
    head_bias_parts = [
        jnp.concatenate([s[0, 2 * cols : 3 * cols], s[0, cols : 2 * cols]])
        for s in [*sums0, *sums1, *sums2, *sums3]
    ]

    token_grad, first_sums = rows_call(
        first_back_kernel, "first_back", place,
        [window_grad, from_left, from_right, middle_grad, tokens, vectors],
        [per_micro((window, width)), per_micro((halo, width)), per_micro((halo, width)), part_spec,
         own_spec, vec_spec],
        [low_rows, sum_rows], [part_spec, vec_spec],
    )
    outer = jnp.stack([mixer_scale, feed_scale] + [jnp.ones_like(out_bias)] * 6)
    sums = (back_sums + first_sums) * outer
    group_sums = jnp.stack(
        [jnp.concatenate([head_bias_parts[r], up_bias_parts[r][0]]) for r in range(narrow_size)]
    )
    group_sums = jnp.stack([group_sums[r ^ narrow_at] for r in range(narrow_size)])
    packed = jnp.concatenate([sums.reshape(-1), group_sums.reshape(-1)]).reshape(-1, 128)
    packed, mine_sent, *heads_sent = tie(packed, mine_sent, *heads_sent)
    heads_part = add_low(heads_cut[0], *heads_sent)
    packed, heads_part, mine_sent = tie(packed, heads_part, mine_sent)
    heads_all = exchange(heads_part, groups[-1])
    packed = reduce_narrow(packed)
    feed_total = arrange([mine, mine_sent], last, 0).reshape(width, -1)
    packed, *heads_all = tie(packed, *heads_all)
    packed = reduce_wide(packed)
    heads_total = arrange(heads_all, groups[-1], 0).reshape((-1,) + heads_part.shape[1:])
    for bits in reversed(groups[:-1]):
        heads_total = arrange(exchange(heads_total, bits), bits, 0)
        heads_total = heads_total.reshape((-1,) + heads_part.shape[1:])
    heads_total = spread_last(heads_total)
    packed = packed.reshape(-1)
    sums = packed[: 8 * width].reshape(8, width)
    group_sums = packed[8 * width :].reshape(narrow_size, -1)
    mine = lax.dynamic_slice_in_dim(group_sums, narrow_at, 1, 0)[0]

    heads_grad = jnp.stack(
        [heads_total[:, 2 * cols : 3 * cols], heads_total[:, :cols], heads_total[:, cols : 2 * cols]],
        axis=1,
    ).astype(f32)
    out_grad = heads_total[:, 3 * cols :].T.astype(f32)
    return (
        layer_out, token_grad, heads_grad, mine[: 2 * cols].reshape(2, cols), out_grad, sums[0],
        feed_total[:, :hidden].astype(f32), mine[2 * cols :],
        feed_total[:, hidden:].T.astype(f32), sums[1], sums[2],
        sums[3], sums[4], sums[5], sums[6], sums[7],
    )


def solution(mesh):
    return jax.shard_map(
        body,
        mesh=mesh,
        in_specs=(
            P(None, "wide", None),
            P(None, "wide", None),
            P("wide", None, "narrow"),
            P(None, "narrow"),
            P("narrow", "wide"),
            P(),
            P("wide", "narrow"),
            P("narrow"),
            P("narrow", "wide"),
            P(),
            P(),
            P(),
            P(),
            P(),
            P(),
            P(),
            P(None, "wide", None),
        ),
        out_specs=(
            P(None, "wide", None),
            P(None, ("wide", "narrow"), None),
            P(None, None, "narrow"),
            P(None, "narrow"),
            P("narrow", None),
            P(),
            P(None, "narrow"),
            P("narrow"),
            P("narrow", None),
            P(),
            P(),
            P(),
            P(),
            P(),
            P(),
            P(),
        ),
        check_vma=False,
    )
```

```python
import math
from functools import partial

import jax
import jax.numpy as jnp
from jax import lax
from jax.experimental import pallas as pl
from jax.experimental.pallas import tpu as pltpu
from jax.sharding import PartitionSpec as P

HEAD_DIM = 64
MOST = 196
epsilon = 1e-06
bf16 = jnp.bfloat16
f32 = jnp.float32
LOG2E = math.log2(math.e)
VMEM_LIMIT = 60 * 1024 * 1024
FEED_CHUNKS = 2
QUERIES = 160


def round_up(value, step):
    return -(-value // step) * step


def nt(left, right):
    return lax.dot_general(left, right, (((1,), (1,)), ((), ())), preferred_element_type=f32)


def tn(left, right):
    return lax.dot_general(left, right, (((0,), (0,)), ((), ())), preferred_element_type=f32)


def nn(left, right):
    return jnp.dot(left, right, preferred_element_type=f32)


def query_chunk(own):
    return QUERIES if own % QUERIES == 0 else own


def key_span(own, win):
    return min(win, query_chunk(own) + 2 * round_up(MOST - 1, 16))


def key_start(off, at, own, win):
    first = jnp.clip(off + at - round_up(MOST - 1, 16), 0, win - key_span(own, win))
    return pl.multiple_of(first, 16)


def params():
    return pltpu.CompilerParams(
        dimension_semantics=("arbitrary",), vmem_limit_bytes=VMEM_LIMIT
    )


def cost(flops, transcendentals, moved):
    return pl.CostEstimate(flops=1024, transcendentals=0, bytes_accessed=1024)


def full(shape):
    return pl.BlockSpec(shape, lambda *a: (0,) * len(shape))


def per_micro(shape):
    return pl.BlockSpec((1,) + shape, lambda m, *a: (m,) + (0,) * len(shape))


def stack_heads(rows, heads):
    lane = lax.broadcasted_iota(jnp.int32, rows.shape, 1) // HEAD_DIM
    zero = jnp.zeros_like(rows)
    return jnp.concatenate([jnp.where(lane == h, rows, zero) for h in range(heads)], axis=0)


def unstack_heads(stacked, heads):
    rows = stacked.shape[0] // heads
    lane = lax.broadcasted_iota(jnp.int32, (rows, stacked.shape[1]), 1) // HEAD_DIM
    out = stacked[:rows]
    for h in range(1, heads):
        out = jnp.where(lane == h, stacked[h * rows : (h + 1) * rows], out)
    return out


def attend_kernel(own, heads, count, first, off_ref, *refs):
    x_ref, b_ref, bnd_ref = refs[:3]
    w_refs = refs[3 : 3 + count]
    rest = refs[3 + count + (0 if first else 1) :]
    mixed_ref = rest[0]
    off = pl.multiple_of(off_ref[0], 16)
    win = x_ref.shape[1]
    cols = heads * HEAD_DIM
    xw = x_ref[0]
    xo = x_ref[0, pl.ds(off, own), :]
    size, span = query_chunk(own), key_span(own, win)
    place = lax.broadcasted_iota(jnp.int32, (span, heads * size), 0)
    mixed = None if first else refs[3 + count][0]
    for i in range(count):
        q_ref, k_ref, v_ref, o_ref, l_ref = rest[1 + 5 * i : 6 + 5 * i]
        w = w_refs[i]
        both = nn(xw, w[:, : 2 * cols])
        k = both[:, :cols].astype(bf16)
        v = (both[:, cols:] + b_ref[i, 1:2]).astype(bf16)
        q = (nn(xo, w[:, 2 * cols : 3 * cols]) + b_ref[i, 0:1]).astype(bf16)
        q_ref[0] = q
        k_ref[0] = k
        v_ref[0] = v
        parts = []
        for c in range(own // size):
            key_at = key_start(off, c * size, own, win)
            kc, vc = k_ref[0, pl.ds(key_at, span), :], v_ref[0, pl.ds(key_at, span), :]
            qs = stack_heads(q[c * size : (c + 1) * size], heads)
            keep = (place >= bnd_ref[0, c, 0:1] - key_at) & (place < bnd_ref[0, c, 1:2] - key_at)
            scores = nt(kc, qs) * (HEAD_DIM**-0.5 * LOG2E)
            scores = jnp.where(keep, scores, -1e30)
            top = jnp.max(scores, axis=0, keepdims=True)
            weights = jnp.exp2(scores - top)
            total = jnp.sum(weights, axis=0, keepdims=True)
            out = tn(vc, weights.astype(bf16)) * (1.0 / total)
            parts.append(unstack_heads(out.T, heads).astype(bf16))
            l_ref[0, c] = top + jnp.log2(total)
        out = jnp.concatenate(parts, axis=0)
        o_ref[0] = out
        part = nt(out, w[:, 3 * cols :])
        mixed = part if mixed is None else mixed + part
    mixed_ref[0] = mixed


def attend(off, x_win, pieces, bias, bounds, own, mixed):
    micro, win, width = x_win.shape
    cols = pieces[0].shape[1] // 4
    heads = cols // HEAD_DIM
    size = query_chunk(own)
    stacked = heads * size
    count = len(pieces)
    first = mixed is None
    shapes = [jax.ShapeDtypeStruct((micro, own, width), f32)]
    specs = [per_micro((own, width))]
    for _ in pieces:
        for rows in (own, win, win, own):
            shapes.append(jax.ShapeDtypeStruct((micro, rows, cols), bf16))
            specs.append(per_micro((rows, cols)))
        shapes.append(jax.ShapeDtypeStruct((micro, own // size, 1, stacked), f32))
        specs.append(per_micro((own // size, 1, stacked)))
    args = [x_win, bias, bounds] + list(pieces)
    in_specs = [per_micro((win, width)), full(bias.shape), per_micro((own // size, 2, stacked))]
    in_specs += [full((width, 4 * cols))] * count
    if not first:
        args.append(mixed)
        in_specs.append(per_micro((own, width)))
    result = pl.pallas_call(
        partial(attend_kernel, own, heads, count, first),
        grid_spec=pltpu.PrefetchScalarGridSpec(
            num_scalar_prefetch=1, grid=(micro,), in_specs=in_specs, out_specs=specs
        ),
        out_shape=shapes,
        compiler_params=params(),
        cost_estimate=cost(
            count * micro * 2 * (win * width * cols * 3 + 8 * stacked * win * HEAD_DIM),
            count * micro * stacked * win,
            micro * win * width * 2 + count * 4 * width * cols * 2,
        ),
        name="attend",
    )(off, *args)
    return result[0], [tuple(result[1 + 5 * i : 6 + 5 * i]) for i in range(count)]


def attend_back_kernel(own, heads, count, first, halo, off_ref, *refs):
    x_ref, mg_ref, bnd_ref = refs[:3]
    w_refs = refs[3 : 3 + count]
    saved = refs[3 + count : 3 + 6 * count]
    at = 3 + 6 * count
    in_ref = None if first else refs[at]
    rest = refs[at + (0 if first else 1) :]
    dn_ref = rest[0]
    halo_refs = rest[1 + 2 * count : 1 + 2 * count + (2 if halo else 0)]
    *acc_refs, dkv_ref = rest[1 + 2 * count + len(halo_refs) :]
    off = pl.multiple_of(off_ref[0], 16)
    win = x_ref.shape[1]
    cols = heads * HEAD_DIM
    scale = HEAD_DIM**-0.5
    step = pl.program_id(0)
    mg = mg_ref[0]
    xt = x_ref[0].T
    xot = x_ref[0, pl.ds(off, own), :].T
    mgt = mg.T
    size, span = query_chunk(own), key_span(own, win)
    place = lax.broadcasted_iota(jnp.int32, (span, heads * size), 0)
    dn = None if first else in_ref[0]
    dn_own = None
    for i in range(count):
        w = w_refs[i]
        q_ref, k_ref, v_ref, o_ref, l_ref = saved[5 * i : 5 * i + 5]
        dw_ref, db_ref = rest[1 + 2 * i : 3 + 2 * i]
        acc_ref = acc_refs[i]
        o = o_ref[0]
        g = nn(mg, w[:, 3 * cols :]).astype(bf16)
        dkv_ref[...] = jnp.zeros_like(dkv_ref)
        parts = []
        for c in range(own // size):
            key_at = key_start(off, c * size, own, win)
            keys = pl.ds(key_at, span)
            kc, vc = k_ref[0, keys, :], v_ref[0, keys, :]
            qs = stack_heads(q_ref[0, c * size : (c + 1) * size, :], heads)
            gs = stack_heads(g[c * size : (c + 1) * size], heads)
            keep = (place >= bnd_ref[0, c, 0:1] - key_at) & (place < bnd_ref[0, c, 1:2] - key_at)
            scores = nt(kc, qs) * (scale * LOG2E) - l_ref[0, c]
            weights = jnp.exp2(jnp.where(keep, scores, -1e30))
            weighed = weights * nt(vc, gs)
            delta = jnp.sum(weighed, axis=0, keepdims=True)
            slope = (weighed - weights * delta).astype(bf16)
            parts.append((unstack_heads(tn(kc, slope).T, heads) * scale).astype(bf16))
            dkv_ref[0, keys, :] += nn(slope, qs)
            dkv_ref[1, keys, :] += nn(weights.astype(bf16), gs)
        dq = jnp.concatenate(parts, axis=0)
        dkv = jnp.concatenate([dkv_ref[0] * scale, dkv_ref[1]], axis=1).astype(bf16)
        part = nt(dkv, w[:, : 2 * cols])
        dn = part if dn is None else dn + part
        part = nt(dq, w[:, 2 * cols : 3 * cols])
        dn_own = part if dn_own is None else dn_own + part
        left = nn(xt, dkv)
        right = jnp.concatenate([nn(xot, dq), nn(mgt, o)], axis=1)
        sums = jnp.concatenate(
            [
                jnp.sum(dkv.astype(f32), axis=0, keepdims=True),
                jnp.sum(jnp.concatenate([dq, dq], axis=1).astype(f32), axis=0, keepdims=True),
            ],
            axis=1,
        )

        @pl.when(step == 0)
        def _():
            acc_ref[:, : 2 * cols] = left
            acc_ref[:, 2 * cols :] = right
            db_ref[...] = sums

        @pl.when(step > 0)
        def _():
            acc_ref[:, : 2 * cols] += left
            acc_ref[:, 2 * cols :] += right
            db_ref[...] += sums

        @pl.when(step == pl.num_programs(0) - 1)
        def _():
            dw_ref[...] = acc_ref[...].astype(bf16)

    dn_ref[0] = dn
    dn_ref[0, pl.ds(off, own), :] += dn_own
    if halo:
        before = pl.multiple_of(jnp.maximum(off - halo, 0), 16)
        after = pl.multiple_of(jnp.minimum(off + own, win - halo), 16)
        halo_refs[0][0] = dn_ref[0, pl.ds(before, halo), :].astype(bf16)
        halo_refs[1][0] = dn_ref[0, pl.ds(after, halo), :].astype(bf16)


def attend_back(off, x_win, mixed_grad, pieces, saved, bounds, grad_in, halo):
    micro, win, width = x_win.shape
    own = mixed_grad.shape[1]
    cols = pieces[0].shape[1] // 4
    heads = cols // HEAD_DIM
    size = query_chunk(own)
    stacked = heads * size
    count = len(pieces)
    first = grad_in is None
    args = [x_win, mixed_grad, bounds] + list(pieces)
    in_specs = [per_micro((win, width)), per_micro((own, width)), per_micro((own // size, 2, stacked))]
    in_specs += [full((width, 4 * cols))] * count
    for one in saved:
        args += list(one)
        in_specs += [per_micro((rows, cols)) for rows in (own, win, win, own)]
        in_specs.append(per_micro((own // size, 1, stacked)))
    if not first:
        args.append(grad_in)
        in_specs.append(per_micro((win, width)))
    shapes = [jax.ShapeDtypeStruct((micro, win, width), f32)]
    specs = [per_micro((win, width))]
    for _ in pieces:
        shapes += [
            jax.ShapeDtypeStruct((width, 4 * cols), bf16),
            jax.ShapeDtypeStruct((1, 4 * cols), f32),
        ]
        specs += [full((width, 4 * cols)), full((1, 4 * cols))]
    for _ in range(2 if halo else 0):
        shapes.append(jax.ShapeDtypeStruct((micro, halo, width), bf16))
        specs.append(per_micro((halo, width)))
    result = pl.pallas_call(
        partial(attend_back_kernel, own, heads, count, first, halo),
        grid_spec=pltpu.PrefetchScalarGridSpec(
            num_scalar_prefetch=1,
            grid=(micro,),
            in_specs=in_specs,
            out_specs=specs,
            scratch_shapes=[pltpu.VMEM((width, 4 * cols), f32)] * count
            + [pltpu.VMEM((2, win, cols), f32)],
        ),
        out_shape=shapes,
        compiler_params=params(),
        cost_estimate=cost(
            count * micro * (40 * stacked * win * HEAD_DIM + 12 * win * width * cols),
            count * micro * stacked * win,
            micro * (10 * win) * width + count * 4 * width * cols * 4,
        ),
        name="attend_back",
    )(off, *args)
    return result[0], result[1 : 1 + 2 * count : 2], result[2 : 2 + 2 * count : 2], result[1 + 2 * count :]


def feed_kernel(chunks, count, first, *refs):
    x_ref, g_ref = refs[:2]
    w_refs = refs[2 : 2 + count]
    b_refs = refs[2 + count : 2 + 2 * count]
    at = 2 + 2 * count
    if not first:
        fi_ref, ni_ref = refs[at : at + 2]
        at = at + 2
    f_ref, n_ref = refs[at : at + 2]
    outs = refs[at + 2 : at + 2 + 2 * count]
    act_ref, ug_ref, xt_ref, gt_ref = refs[at + 2 + 2 * count :]
    rows = x_ref.shape[0]
    step = rows // chunks
    xt_ref[...] = x_ref[...].T
    gt_ref[...] = g_ref[...].T
    for i in range(count):
        w_ref, b_ref = w_refs[i], b_refs[i]
        dw_ref, db_ref = outs[2 * i : 2 * i + 2]
        hidden = b_ref.shape[1]
        total = jnp.zeros((1, hidden), f32)
        for c in range(chunks):
            rows_at = pl.ds(c * step, step)
            upper = nn(x_ref[rows_at, :], w_ref[:, :hidden]) + b_ref[...]
            phi = 0.5 + 0.5 * lax.erf(upper * math.sqrt(0.5))
            active = (upper * phi).astype(bf16)
            bell = jnp.exp2(upper * upper * (-0.5 * LOG2E)) * (1.0 / math.sqrt(2.0 * math.pi))
            slope = phi + upper * bell
            grad = (nn(g_ref[rows_at, :], w_ref[:, hidden:]) * slope).astype(bf16)
            act_ref[rows_at, :] = active
            ug_ref[rows_at, :] = grad
            total = total + jnp.sum(grad.astype(f32), axis=0, keepdims=True)
            feed = nt(active, w_ref[:, hidden:])
            back = nt(grad, w_ref[:, :hidden])
            if i > 0:
                feed = feed + f_ref[rows_at, :]
                back = back + n_ref[rows_at, :]
            elif not first:
                feed = feed + fi_ref[rows_at, :]
                back = back + ni_ref[rows_at, :]
            f_ref[rows_at, :] = feed
            n_ref[rows_at, :] = back
        db_ref[...] = total
        dw_ref[:, :hidden] = nn(xt_ref[...], ug_ref[...]).astype(bf16)
        dw_ref[:, hidden:] = nn(gt_ref[...], act_ref[...]).astype(bf16)


def feed_part(x2, grad, pieces, biases, before):
    rows, width = x2.shape
    hidden = biases[0].shape[1]
    count = len(pieces)
    first = before is None
    args = [x2, grad] + list(pieces) + list(biases)
    aliases = {}
    if not first:
        aliases = {len(args): 0, len(args) + 1: 1}
        args += list(before)
    whole = pl.BlockSpec(memory_space=pltpu.VMEM)
    shapes = [jax.ShapeDtypeStruct((rows, width), f32)] * 2
    for _ in pieces:
        shapes += [
            jax.ShapeDtypeStruct((width, 2 * hidden), bf16),
            jax.ShapeDtypeStruct((1, hidden), f32),
        ]
    result = pl.pallas_call(
        partial(feed_kernel, FEED_CHUNKS, count, first),
        in_specs=[whole] * len(args),
        out_specs=[whole] * len(shapes),
        out_shape=shapes,
        scratch_shapes=[
            pltpu.VMEM((rows, hidden), bf16),
            pltpu.VMEM((rows, hidden), bf16),
            pltpu.VMEM((width, rows), bf16),
            pltpu.VMEM((width, rows), bf16),
        ],
        input_output_aliases=aliases,
        compiler_params=pltpu.CompilerParams(vmem_limit_bytes=VMEM_LIMIT),
        cost_estimate=cost(
            count * 12 * rows * width * hidden,
            count * 2 * rows * hidden,
            16 * rows * width + count * 8 * width * hidden,
        ),
        name="feed_part",
    )(*args)
    return tuple(result[:2]), list(result[2::2]), list(result[3::2])


def norm_parts(values_in):
    center = jnp.mean(values_in, axis=-1, keepdims=True)
    shifted = values_in - center
    inverse = lax.rsqrt(jnp.mean(shifted * shifted, axis=-1, keepdims=True) + epsilon)
    return (shifted * inverse, inverse)


def norm_back(grad_in, unit_rows, inverse, gain_row):
    scaled = grad_in * gain_row
    return inverse * (
        scaled
        - jnp.mean(scaled, axis=-1, keepdims=True)
        - unit_rows * jnp.mean(scaled * unit_rows, axis=-1, keepdims=True)
    )


VECTORS = (
    "out_bias", "down_bias", "first_gain", "first_shift", "second_gain", "second_shift",
    "mixer_scale", "feed_scale",
)


def row(vec_ref, name):
    at = VECTORS.index(name)
    return vec_ref[at : at + 1]


def own_rows(shape):
    return pl.BlockSpec((1,) + shape, lambda m, place: (m, place[0]) + (0,) * (len(shape) - 1))


def rows_call(kernel, name, place, args, specs, shapes, out_specs):
    micro = args[0].shape[0]
    return pl.pallas_call(
        kernel,
        grid_spec=pltpu.PrefetchScalarGridSpec(
            num_scalar_prefetch=1, grid=(micro,), in_specs=specs, out_specs=out_specs
        ),
        out_shape=shapes,
        compiler_params=params(),
        cost_estimate=cost(0, 0, 0),
        name=name,
    )(place, *args)


def first_norm_kernel(place_ref, x_ref, c_ref, vec_ref, n_ref, g_ref):
    start = pl.multiple_of(place_ref[1], 16)
    win = n_ref.shape[1]
    unit = norm_parts(x_ref[0, pl.ds(start, win), :].astype(f32))[0]
    n_ref[0] = (unit * row(vec_ref, "first_gain") + row(vec_ref, "first_shift")).astype(bf16)
    g_ref[0] = (row(vec_ref, "feed_scale") * c_ref[0].astype(f32)).astype(bf16)


def second_norm_kernel(place_ref, mixed_ref, x_ref, vec_ref, m_ref, n_ref):
    branch = mixed_ref[0] + row(vec_ref, "out_bias")
    middle = x_ref[0].astype(f32) + row(vec_ref, "mixer_scale") * branch
    m_ref[0] = middle
    unit = norm_parts(middle)[0]
    n_ref[0] = (unit * row(vec_ref, "second_gain") + row(vec_ref, "second_shift")).astype(bf16)


def column_sums(sum_ref, rows_in):
    total = jnp.concatenate([jnp.sum(r, axis=0, keepdims=True) for r in rows_in], axis=0)

    @pl.when(pl.program_id(0) == 0)
    def _():
        sum_ref[...] = total

    @pl.when(pl.program_id(0) > 0)
    def _():
        sum_ref[...] += total


def second_back_kernel(
    place_ref, feed_ref, back_ref, m_ref, mixed_ref, c_ref, vec_ref, l_ref, mg_ref, low_ref, sum_ref
):
    middle, back, grad = m_ref[0], back_ref[0], c_ref[0].astype(f32)
    feed_scale = row(vec_ref, "feed_scale")
    branch = feed_ref[0] + row(vec_ref, "down_bias")
    l_ref[0] = (middle + feed_scale * branch).astype(bf16)
    unit, inverse = norm_parts(middle)
    middle_grad = grad + norm_back(back, unit, inverse, row(vec_ref, "second_gain"))
    mg_ref[0] = middle_grad
    low_ref[0] = (row(vec_ref, "mixer_scale") * middle_grad).astype(bf16)
    mixer = mixed_ref[0] + row(vec_ref, "out_bias")
    zero = jnp.zeros_like(grad[:8])
    column_sums(
        sum_ref,
        [middle_grad, grad, zero, zero, back * unit, back, middle_grad * mixer, grad * branch],
    )


def first_back_kernel(
    place_ref, win_ref, left_ref, right_ref, mg_ref, x_ref, vec_ref, t_ref, sum_ref
):
    own, halo = mg_ref.shape[1], left_ref.shape[1]
    off = pl.multiple_of(place_ref[2], 16)
    gap = jnp.zeros((own - halo, left_ref.shape[2]), f32)
    grad = win_ref[0, pl.ds(off, own), :]
    grad = grad + jnp.concatenate([left_ref[0].astype(f32), gap], axis=0)
    grad = grad + jnp.concatenate([gap, right_ref[0].astype(f32)], axis=0)
    unit, inverse = norm_parts(x_ref[0].astype(f32))
    t_ref[0] = (
        mg_ref[0] + norm_back(grad, unit, inverse, row(vec_ref, "first_gain"))
    ).astype(bf16)
    zero = jnp.zeros_like(grad[:8])
    column_sums(sum_ref, [zero, zero, grad * unit, grad, zero, zero, zero, zero])


def swap(values_in, axis, bit):
    size = lax.axis_size(axis)
    return lax.ppermute(values_in, axis, [(i, i ^ bit) for i in range(size)])


def shift(values_in, axis, step):
    size = lax.axis_size(axis)
    pairs = [(i, i + step) for i in range(size) if 0 <= i + step < size]
    return lax.ppermute(values_in, axis, pairs)


def wide_bits(size):
    bits = []
    bit = size // 2
    while bit:
        bits.append(bit)
        bit //= 2
    return bits


def bit_of(axis, bit):
    return (lax.axis_index(axis) & bit) != 0


def join(mine, other, is_high, axis):
    low = jnp.where(is_high, other, mine)
    high = jnp.where(is_high, mine, other)
    return jnp.stack([low, high], axis=axis)


def tie(*values_in):
    return lax.optimization_barrier(values_in)


def far_groups():
    bits = wide_bits(lax.axis_size("wide"))[:-1]
    return [bits[i : i + 2] for i in range(0, len(bits), 2)]


def offsets(bits):
    return [
        sum(bit for i, bit in enumerate(reversed(bits)) if (k >> i) & 1)
        for k in range(2 ** len(bits))
    ]


def exchange(values_in, bits):
    return [values_in] + [swap(values_in, "wide", o) for o in offsets(bits)[1:]]


def arrange(parts, bits, axis):
    if not bits:
        return jnp.expand_dims(parts[0], axis)
    half = len(parts) // 2
    low = arrange(parts[:half], bits[1:], axis)
    high = arrange(parts[half:], bits[1:], axis)
    is_high = bit_of("wide", bits[0])
    return jnp.concatenate(
        [jnp.where(is_high, high, low), jnp.where(is_high, low, high)], axis=axis
    )


def arrange_blocks(parts, bits):
    return arrange(parts, bits, 1).reshape((-1,) + parts[0].shape[1:])


def last_bit():
    return wide_bits(lax.axis_size("wide"))[-1]


def gather_narrow(piece):
    far = swap(piece, "narrow", 2)
    return [piece, swap(piece, "narrow", 1), far, swap(far, "narrow", 1)]


def add_low(*parts):
    total = parts[0].astype(f32)
    for part in parts[1:]:
        total = total + part.astype(f32)
    return total.astype(bf16)


def cut(values_in, axis, bits):
    count = 2 ** len(bits)
    size = values_in.shape[0] // count
    at = lax.axis_index(axis)
    places = []
    for o in offsets(bits):
        other = at ^ o
        place = 0
        for bit in bits:
            place = 2 * place + ((other & bit) != 0).astype(jnp.int32)
        places.append(place)
    return [lax.dynamic_slice_in_dim(values_in, p * size, size, 0) for p in places]


def send_cut(parts, bits):
    return [swap(part, "wide", o) for part, o in zip(parts[1:], offsets(bits)[1:])]


def spread_last(part):
    bits = [last_bit()]
    return arrange(exchange(part, bits), bits, 0).reshape((-1,) + part.shape[1:])


def tree_sum(parts):
    while len(parts) > 1:
        parts = [parts[i] + parts[i + 1] for i in range(0, len(parts), 2)]
    return parts[0]


def reduce_wide(values_in):
    for bits in far_groups() + [[last_bit()]]:
        values_in = tree_sum(exchange(values_in, bits))
    return values_in


def reduce_narrow(values_in):
    return tree_sum([values_in] + [swap(values_in, "narrow", o) for o in (1, 2, 3)])


def body(
    tokens, image_lengths, heads_weight, heads_bias, out_weight, out_bias, up_weight, up_bias,
    down_weight, down_bias, first_gain, first_shift, second_gain, second_shift, mixer_scale,
    feed_scale, cotangent,
):
    micro, row_count, width = tokens.shape
    narrow_size = lax.axis_size("narrow")
    narrow_at = lax.axis_index("narrow")
    own = row_count // narrow_size
    cols = heads_weight.shape[2]
    heads = cols // HEAD_DIM
    rows = micro * own
    halo = round_up(MOST - 1, 16)
    window = min(row_count, round_up(own + 2 * halo, 128))
    lead = round_up((window - own) // 2, 16)
    start = jnp.clip(narrow_at * own - lead, 0, row_count - window)
    off = narrow_at * own - start
    offset = off.reshape(1).astype(jnp.int32)

    hidden = up_weight.shape[1]
    groups = far_groups()

    bias_pieces = gather_narrow(
        jnp.concatenate([heads_bias.reshape(-1), up_bias]).reshape(1, -1)
    )
    qv_biases = [heads_bias[None]]
    qv_biases += [b[:, : 2 * cols].reshape(1, 2, cols) for b in bias_pieces[1:]]
    up_biases = [up_bias.reshape(1, hidden)] + [b[:, 2 * cols :] for b in bias_pieces[1:]]
    heads_blocks = jnp.concatenate(
        [heads_weight[:, 1], heads_weight[:, 2], heads_weight[:, 0], out_weight.T], axis=1
    )[None]
    for bits in groups:
        heads_blocks = arrange_blocks(exchange(heads_blocks, bits), bits)
    feed_blocks = jnp.concatenate([up_weight, down_weight.T], axis=1)[None]
    heads_blocks, feed_blocks, *biases = tie(heads_blocks, feed_blocks, *qv_biases, *up_biases)
    qv_biases, up_biases = biases[:narrow_size], biases[narrow_size:]
    for bits in groups[:-1]:
        feed_blocks = arrange_blocks(exchange(feed_blocks, bits), bits)
    feed_parts = exchange(feed_blocks, groups[-1])
    last = [last_bit()]
    heads_all = arrange_blocks(exchange(heads_blocks, last), last)
    heads_own = heads_all.reshape(width, -1)

    ends = jnp.cumsum(image_lengths[:, 0], axis=1)
    places = narrow_at * own + jnp.arange(own, dtype=jnp.int32)
    passed = ends[:, :, None] <= places[None, None, :]
    first_key = jnp.max(jnp.where(passed, ends[:, :, None], 0), axis=1) - start
    last_key = jnp.min(jnp.where(passed, row_count, ends[:, :, None]), axis=1) - start
    bounds = jnp.stack([first_key, last_key], axis=1).astype(jnp.int32)
    size = query_chunk(own)
    bounds = bounds.reshape(micro, 2, own // size, size).transpose(0, 2, 1, 3)
    bounds = jnp.tile(bounds, (1, 1, 1, heads))

    place = jnp.stack([narrow_at, start, off]).astype(jnp.int32)
    vectors = jnp.stack(
        [out_bias, down_bias, first_gain, first_shift, second_gain, second_shift, mixer_scale,
         feed_scale]
    )
    own_spec, part_spec, vec_spec = own_rows((own, width)), per_micro((own, width)), full((8, width))
    low_rows = jax.ShapeDtypeStruct((micro, own, width), bf16)
    high_rows = jax.ShapeDtypeStruct((micro, own, width), f32)
    sum_rows = jax.ShapeDtypeStruct((8, width), f32)
    window_normed, feed_grad = rows_call(
        first_norm_kernel, "first_norm", place, [tokens, cotangent, vectors],
        [per_micro((row_count, width)), own_spec, vec_spec],
        [jax.ShapeDtypeStruct((micro, window, width), bf16), low_rows],
        [per_micro((window, width)), part_spec],
    )
    feed_grad = feed_grad.reshape(rows, width)

    def halves(blocks):
        half = blocks.shape[0] // 2
        return blocks[:half], blocks[half:]

    def attend_on(piece, at, before):
        return attend(offset, window_normed, [piece], qv_biases[at], bounds, own, before)

    heads_low, heads_high = halves(heads_all)
    window_normed, heads_low = tie(window_normed, heads_low)
    heads_near = swap(heads_own, "narrow", 1)
    far_low = swap(heads_low, "narrow", 2)
    mixed, saved0 = attend_on(heads_own, 0, None)
    mixed, far_low, *feed_parts = tie(mixed, far_low, *feed_parts)
    feed_low, feed_high = halves(arrange_blocks(feed_parts, groups[-1]))
    mixed, feed_low, feed_high, heads_high = tie(mixed, feed_low, feed_high, heads_high)
    far_high = swap(heads_high, "narrow", 2)
    low_other = exchange(feed_low, last)[1]
    mixed, saved1 = attend_on(heads_near, 1, mixed)
    mixed, far_high, low_other = tie(mixed, far_high, low_other)
    heads_far = jnp.concatenate([far_low, far_high], axis=0).reshape(width, -1)
    mixed, heads_far, feed_low, feed_high = tie(mixed, heads_far, feed_low, feed_high)
    heads_cross = swap(heads_far, "narrow", 1)
    high_other = exchange(feed_high, last)[1]
    feed_far_low = swap(feed_low, "narrow", 2)
    mixed, saved2 = attend_on(heads_far, 2, mixed)
    mixed, high_other, feed_far_low = tie(mixed, high_other, feed_far_low)

    def whole_feed(low, high, low_sent, high_sent):
        mine = jnp.concatenate([low, high], axis=0)
        other = jnp.concatenate([low_sent, high_sent], axis=0)
        return arrange_blocks([mine, other], last).reshape(width, -1)

    feed_own = whole_feed(feed_low, feed_high, low_other, high_other)
    mixed, feed_own, feed_high = tie(mixed, feed_own, feed_high)
    feed_near = swap(feed_own, "narrow", 1)
    feed_far_high = swap(feed_high, "narrow", 2)
    mixed, saved3 = attend_on(heads_cross, 3, mixed)
    mixed, feed_far_high = tie(mixed, feed_far_high)
    middle, second_normed = rows_call(
        second_norm_kernel, "second_norm", place, [mixed, tokens, vectors],
        [part_spec, own_spec, vec_spec], [high_rows, low_rows], [part_spec, part_spec],
    )
    second_normed = second_normed.reshape(rows, width)

    def feed_on(pieces, biases, before):
        return feed_part(second_normed, feed_grad, pieces, biases, before)

    second_normed, feed_far_low = tie(second_normed, feed_far_low)
    far_low_other = exchange(feed_far_low, last)[1]
    sums, (part0,), bias0 = feed_on([feed_own], up_biases[:1], None)
    *sums, far_low_other, feed_far_high = tie(*sums, far_low_other, feed_far_high)
    far_high_other = exchange(feed_far_high, last)[1]
    sums, (part1,), bias1 = feed_on([feed_near], up_biases[1:2], sums)
    *sums, far_high_other = tie(*sums, far_high_other)
    feed_far = whole_feed(feed_far_low, feed_far_high, far_low_other, far_high_other)
    *sums, feed_far, part1 = tie(*sums, feed_far, part1)
    feed_cross = swap(feed_far, "narrow", 1)
    given = swap(part1, "narrow", 1)
    sums, (part2,), bias2 = feed_on([feed_far], up_biases[2:3], sums)
    *sums, given = tie(*sums, given)
    near_keep, near_give = cut(add_low(part0, given), "wide", last)
    up_give, down_give = near_give[:, :hidden], near_give[:, hidden:]
    *sums, near_keep, up_give, down_give = tie(*sums, near_keep, up_give, down_give)
    up_sent = swap(up_give, "wide", last[0])
    sums, (part3,), bias3 = feed_on([feed_cross], up_biases[3:], sums)
    feed, second_normed_grad, up_sent, part3, down_give = tie(*sums, up_sent, part3, down_give)
    down_sent = swap(down_give, "wide", last[0])
    given = swap(part3, "narrow", 1)
    up_bias_parts = bias0 + bias1 + bias2 + bias3

    layer_own, middle_grad, mixed_grad, back_sums = rows_call(
        second_back_kernel, "second_back", place,
        [feed.reshape(micro, own, width), second_normed_grad.reshape(micro, own, width), middle,
         mixed, cotangent, vectors],
        [part_spec, part_spec, part_spec, part_spec, own_spec, vec_spec],
        [low_rows, high_rows, low_rows, sum_rows],
        [part_spec, part_spec, part_spec, vec_spec],
    )
    def back_on(pieces, saved, grad_in, halo):
        return attend_back(
            offset, window_normed, mixed_grad, pieces, saved, bounds, grad_in, halo
        )

    mixed_grad, down_sent, given = tie(mixed_grad, down_sent, given)
    near = add_low(near_keep, jnp.concatenate([up_sent, down_sent], axis=1))
    far_cut = cut(add_low(part2, given), "wide", last)
    mixed_grad, near, layer_own, *far_cut = tie(mixed_grad, near, layer_own, *far_cut)
    layer_far, layer_last = swap(layer_own[:-1], "narrow", 2), layer_own[-1:]
    far_sent = send_cut(far_cut, last)
    window_grad, (heads3,), sums3, _ = back_on([heads_cross], saved3, None, 0)
    given3 = swap(heads3, "narrow", 1)
    window_grad, layer_far, *far_sent = tie(window_grad, layer_far, *far_sent)
    far = add_low(far_cut[0], *far_sent)
    window_grad, far, layer_far = tie(window_grad, far, layer_far)
    layer_parts = [
        layer_own, swap(layer_own, "narrow", 1), layer_far, swap(layer_far, "narrow", 1)
    ]
    far_given = swap(far, "narrow", 2)
    window_grad, (heads2,), sums2, _ = back_on([heads_far], saved2, window_grad, 0)
    window_grad, far_given, given3, *layer_parts = tie(
        window_grad, far_given, given3, *layer_parts
    )
    mine = add_low(near, far_given)
    for bits in groups[:-1]:
        parts = cut(mine, "wide", bits)
        mine = add_low(parts[0], *send_cut(parts, bits))
    mine_cut = cut(mine, "wide", groups[-1])
    heads_sum = add_low(heads2, given3)
    window_grad, heads_sum, *mine_cut = tie(window_grad, heads_sum, *mine_cut)
    mine_sent = send_cut(mine_cut, groups[-1])
    heads_given = swap(heads_sum, "narrow", 2)
    window_grad, (heads1,), sums1, _ = back_on([heads_near], saved1, window_grad, 0)
    given1 = swap(heads1, "narrow", 1)
    window_grad, heads_given, *mine_sent = tie(window_grad, heads_given, *mine_sent)
    mine = add_low(mine_cut[0], *mine_sent)
    window_grad, mine, layer_last = tie(window_grad, mine, layer_last)
    mine_all = exchange(mine, groups[-1])
    layer_last = swap(layer_last, "narrow", 2)
    window_grad, (heads0,), sums0, halos = back_on([heads_own], saved0, window_grad, halo)
    window_grad, layer_last, *mine_all = tie(window_grad, layer_last, *mine_all)
    layer_last = [layer_last, swap(layer_last, "narrow", 1)]
    heads_cut = cut(add_low(heads0, given1, heads_given), "wide", last)
    tied = tie(window_grad, *halos, *heads_cut, *mine_all, *layer_parts)
    window_grad, *halos = tied[:3]
    heads_cut, layer_parts = tied[3:5], tied[-4:]
    heads_sent = send_cut(heads_cut, last)
    from_left = shift(halos[1], "narrow", 1)
    from_right = shift(halos[0], "narrow", -1)
    mine = arrange(tied[5:-4], groups[-1], 0).reshape((-1,) + mine.shape[1:])
    for bits in reversed(groups[:-1]):
        mine = arrange(exchange(mine, bits), bits, 0).reshape((-1,) + mine.shape[1:])
    mine, *heads_sent = tie(mine, *heads_sent)
    mine_sent = exchange(mine, last)[1]
    heads_part = add_low(heads_cut[0], *heads_sent)
    for bits in groups[:-1]:
        parts = cut(heads_part, "wide", bits)
        heads_part = add_low(parts[0], *send_cut(parts, bits))
    heads_cut = cut(heads_part, "wide", groups[-1])
    window_grad, from_left, from_right, *heads_cut = tie(
        window_grad, from_left, from_right, *heads_cut
    )
    heads_sent = send_cut(heads_cut, groups[-1])
    y_high, core_high = bit_of("narrow", 2), bit_of("narrow", 1)
    layer_near = join(layer_parts[0], layer_parts[1], core_high, 1)
    layer_far = [
        jnp.concatenate(pair, axis=0) for pair in zip(layer_parts[2:], layer_last)
    ]
    layer_far = join(*layer_far, core_high, 1)
    layer_out = join(layer_near, layer_far, y_high, 1).reshape(micro, row_count, width)
    head_bias_parts = [
        jnp.concatenate([s[0, 2 * cols : 3 * cols], s[0, cols : 2 * cols]])
        for s in [*sums0, *sums1, *sums2, *sums3]
    ]

    token_grad, first_sums = rows_call(
        first_back_kernel, "first_back", place,
        [window_grad, from_left, from_right, middle_grad, tokens, vectors],
        [per_micro((window, width)), per_micro((halo, width)), per_micro((halo, width)), part_spec,
         own_spec, vec_spec],
        [low_rows, sum_rows], [part_spec, vec_spec],
    )
    outer = jnp.stack([mixer_scale, feed_scale] + [jnp.ones_like(out_bias)] * 6)
    sums = (back_sums + first_sums) * outer
    group_sums = jnp.stack(
        [jnp.concatenate([head_bias_parts[r], up_bias_parts[r][0]]) for r in range(narrow_size)]
    )
    group_sums = jnp.stack([group_sums[r ^ narrow_at] for r in range(narrow_size)])
    packed = jnp.concatenate([sums.reshape(-1), group_sums.reshape(-1)]).reshape(-1, 128)
    packed, mine_sent, *heads_sent = tie(packed, mine_sent, *heads_sent)
    heads_part = add_low(heads_cut[0], *heads_sent)
    packed, heads_part, mine_sent = tie(packed, heads_part, mine_sent)
    heads_all = exchange(heads_part, groups[-1])
    packed = reduce_narrow(packed)
    feed_total = arrange([mine, mine_sent], last, 0).reshape(width, -1)
    packed, *heads_all = tie(packed, *heads_all)
    packed = reduce_wide(packed)
    heads_total = arrange(heads_all, groups[-1], 0).reshape((-1,) + heads_part.shape[1:])
    for bits in reversed(groups[:-1]):
        heads_total = arrange(exchange(heads_total, bits), bits, 0)
        heads_total = heads_total.reshape((-1,) + heads_part.shape[1:])
    heads_total = spread_last(heads_total)
    packed = packed.reshape(-1)
    sums = packed[: 8 * width].reshape(8, width)
    group_sums = packed[8 * width :].reshape(narrow_size, -1)
    mine = lax.dynamic_slice_in_dim(group_sums, narrow_at, 1, 0)[0]

    heads_grad = jnp.stack(
        [heads_total[:, 2 * cols : 3 * cols], heads_total[:, :cols], heads_total[:, cols : 2 * cols]],
        axis=1,
    ).astype(f32)
    out_grad = heads_total[:, 3 * cols :].T.astype(f32)
    return (
        layer_out, token_grad, heads_grad, mine[: 2 * cols].reshape(2, cols), out_grad, sums[0],
        feed_total[:, :hidden].astype(f32), mine[2 * cols :],
        feed_total[:, hidden:].T.astype(f32), sums[1], sums[2],
        sums[3], sums[4], sums[5], sums[6], sums[7],
    )


def solution(mesh):
    return jax.shard_map(
        body,
        mesh=mesh,
        in_specs=(
            P(None, "wide", None),
            P(None, "wide", None),
            P("wide", None, "narrow"),
            P(None, "narrow"),
            P("narrow", "wide"),
            P(),
            P("wide", "narrow"),
            P("narrow"),
            P("narrow", "wide"),
            P(),
            P(),
            P(),
            P(),
            P(),
            P(),
            P(),
            P(None, "wide", None),
        ),
        out_specs=(
            P(None, "wide", None),
            P(None, ("wide", "narrow"), None),
            P(None, None, "narrow"),
            P(None, "narrow"),
            P("narrow", None),
            P(),
            P(None, "narrow"),
            P("narrow"),
            P("narrow", None),
            P(),
            P(),
            P(),
            P(),
            P(),
            P(),
            P(),
        ),
        check_vma=False,
    )
```
